32 devices in a mesh: seq: 4 (over y, x), sample: 2 (over core), head: 4 (over z).
Axes of the slice: x: 2, y: 2, z: 4, core: 2. Of those that a mesh axis runs over, the one named last changes fastest.
Arguments:
- block_in: bfloat16 [4, 2048, 1024], P('sample', 'seq'), may hold values from -6 to 6
- out_cotangent: bfloat16 [4, 2048, 1024], P('sample', 'seq'), may hold values from -6 to 6
- norm_gain: float32 [1024], replicated, may hold values from 0.25 to 1.75
- gate_proj: bfloat16 [1024, 2048], P(None, 'head'), may hold values from -0.296875 to 0.296875
- value_proj: bfloat16 [1024, 2048], P(None, 'head'), may hold values from -0.1875 to 0.1875
- state_proj: bfloat16 [2, 1024, 128], P(None, None, 'head'), may hold values from -0.1875 to 0.1875
- step_proj: bfloat16 [1024, 32], P(None, 'head'), may hold values from -0.1875 to 0.1875
- conv_value: float32 [4, 2048], P(None, 'head'), may hold values from -0.6 to 0.6
- conv_state: float32 [4, 2, 128], P(None, None, 'head'), may hold values from -0.6 to 0.6
- conv_value_bias: float32 [2048], P('head'), may hold values from -0.5 to 0.5
- conv_state_bias: float32 [2, 128], P(None, 'head'), may hold values from -0.5 to 0.5
- step_bias: float32 [32], P('head'), may hold values from -4.5 to -3
- decay_log: float32 [32], P('head'), may hold values from -10 to 1
- skip_gain: float32 [32], P('head'), may hold values from 0.5 to 1.5
- gated_gain: float32 [2048], P('head'), may hold values from 0.25 to 1.75
- out_proj: bfloat16 [2048, 1024], P('head'), may hold values from -0.125 to 0.125
Outputs:
- block_out: bfloat16 [4, 2048, 1024], P('sample', 'seq')
- input_grad: float32 [4, 2048, 1024], P('sample', 'seq')
- norm_gain_grad: float32 [1024], replicated
- gate_proj_grad: float32 [1024, 2048], P(None, 'head')
- value_proj_grad: float32 [1024, 2048], P(None, 'head')
- state_proj_grad: float32 [2, 1024, 128], P(None, None, 'head')
- step_proj_grad: float32 [1024, 32], P(None, 'head')
- conv_value_grad: float32 [4, 2048], P(None, 'head')
- conv_state_grad: float32 [4, 2, 128], P(None, None, 'head')
- conv_value_bias_grad: float32 [2048], P('head')
- conv_state_bias_grad: float32 [2, 128], P(None, 'head')
- step_bias_grad: float32 [32], P('head')
- decay_log_grad: float32 [32], P('head')
- skip_gain_grad: float32 [32], P('head')
- gated_gain_grad: float32 [2048], P('head')
- out_proj_grad: float32 [2048, 1024], P('head')
The draws below stay inside these ranges and needn't reach their ends.
All inputs are finite; a program needn't handle non-finite values.
Results may differ from the reference program's by a relative error of at most 0.0055.
The reference program's roundings to bfloat16 on the way count: a program that leaves them out, or rounds other values in their place, can miss the bound.
Values may be sent and summed in bfloat16 or wider, within the bound.
A program may use at most 192 MiB of HBM per device.

```python
import jax
import jax.numpy as jnp
from jax import lax

D = 1024
H = 32
P_SIZE = 64
N = 128
CONV = 4
GROUP = 256
DI = 2048
LENGTH = 2048
BATCH = 4


clip_edge = 0.296875


def draw_gate_proj(key, part):
    columns = lax.broadcasted_iota(jnp.float32, (D, DI), 1) / DI
    entries = jnp.clip(jax.random.normal(jax.random.fold_in(key, 13), (D, DI), jnp.float32), -5.0, 5.0)
    return jnp.clip(entries * (1.0 + 2.0 * columns) * D ** (-0.5), -clip_edge, clip_edge).astype(jnp.bfloat16)


def draw_decay_log(key, part):
    picks = jax.random.uniform(jax.random.fold_in(key, 21), (H,), jnp.float32)
    fast_rates = jax.random.uniform(jax.random.fold_in(key, 22), (H,), jnp.float32, 0.5, 1.5)
    slow_rates = jax.random.uniform(jax.random.fold_in(key, 23), (H,), jnp.float32, 5.0, 40.0) / LENGTH
    return jnp.log(jnp.where(picks < 0.5, fast_rates, slow_rates))


def block_levels(rng, dims, shards, least, largest):
    level, own = 1.0, jax.random.fold_in(rng, 6)
    for dim, blocks in shards:
        heights = jnp.exp(jax.random.uniform(jax.random.fold_in(own, dim), (blocks,), jnp.float32, least / len(shards), largest / len(shards)))
        level = level * jnp.repeat(heights, dims[dim] // blocks).reshape([-1 if axis == dim else 1 for axis in range(len(dims))])
    return level


def gaussian(stream_key, dims, scale, reach, pieces=(), held_as=jnp.bfloat16):
    values = jax.random.normal(stream_key, dims, jnp.float32) * scale
    if len(pieces) > 0:
        values = block_levels(stream_key, dims, pieces, -0.22, 0.18) * values
    return jnp.clip(values, min=-reach, max=reach).astype(held_as)


def setup_inputs(seed: int = 0) -> dict:
    key_list = jax.random.split(jax.random.key(seed), 17)
    return {
        "block_in": gaussian(key_list[0], (BATCH, LENGTH, D), 1.0, 6.0, ((0, 2), (1, 4))),
        "out_cotangent": gaussian(key_list[1], (BATCH, LENGTH, D), 1.0, 6.0, ((0, 2), (1, 4))),
        "norm_gain": jnp.clip(1.0 + 0.15 * jax.random.normal(key_list[2], (D,), jnp.float32), 0.25, 1.75),
        "gate_proj": draw_gate_proj(jax.random.fold_in(key_list[16], 71), 0),
        "value_proj": gaussian(key_list[4], (D, DI), D ** -0.5, 0.1875, ((1, 4),)),
        "state_proj": gaussian(key_list[5], (2, D, N), D ** -0.5, 0.1875, ((2, 4),)),
        "step_proj": gaussian(key_list[6], (D, H), D ** -0.5, 0.1875, ((1, 4),)),
        "conv_value": jnp.clip(jax.random.uniform(key_list[7], (CONV, DI), jnp.float32, -0.6, 0.6) * block_levels(key_list[7], (CONV, DI), ((1, 4),), -0.4, 0.0), -0.6, 0.6),
        "conv_state": jnp.clip(jax.random.uniform(key_list[8], (CONV, 2, N), jnp.float32, -0.6, 0.6) * block_levels(key_list[8], (CONV, 2, N), ((2, 4),), -0.4, 0.0), -0.6, 0.6),
        "conv_value_bias": jnp.clip(jax.random.uniform(key_list[9], (DI,), jnp.float32, -0.5, 0.5) * block_levels(key_list[9], (DI,), ((0, 4),), -0.4, 0.0), -0.5, 0.5),
        "conv_state_bias": jnp.clip(jax.random.uniform(key_list[10], (2, N), jnp.float32, -0.5, 0.5) * block_levels(key_list[10], (2, N), ((1, 4),), -0.4, 0.0), -0.5, 0.5),
        "step_bias": jnp.clip(-4.5 + 1.5 * jax.random.uniform(key_list[11], (H,), jnp.float32) ** block_levels(key_list[11], (H,), ((0, 4),), -0.2, 0.2), -4.5, -3.0),
        "decay_log": draw_decay_log(jax.random.fold_in(key_list[16], 71), 0),
        "skip_gain": jnp.clip(0.5 + 1.0 * jax.random.uniform(key_list[13], (H,), jnp.float32) ** block_levels(key_list[13], (H,), ((0, 4),), -0.2, 0.2), 0.5, 1.5),
        "gated_gain": jnp.clip(1.0 + 0.15 * jax.random.normal(key_list[14], (DI,), jnp.float32), 0.25, 1.75),
        "out_proj": gaussian(key_list[15], (DI, D), DI ** -0.5, 0.125, ((0, 4),)),
    }


highest = lax.Precision.HIGHEST

def group_pass(values, input_vectors, readout, step_sizes, decay_rates, skip_gain, initial):
    total_length, local_heads, head_width = values.shape
    block_count = total_length // GROUP
    state_width = input_vectors.shape[-1]
    value_blocks = values.reshape(block_count, GROUP, local_heads, head_width)
    input_blocks = input_vectors.reshape(block_count, GROUP, state_width)
    readout_blocks = readout.reshape(block_count, GROUP, state_width)
    step_blocks = step_sizes.reshape(block_count, GROUP, local_heads)
    row_index = lax.broadcasted_iota(jnp.int32, (GROUP, GROUP), 0)
    column_index = lax.broadcasted_iota(jnp.int32, (GROUP, GROUP), 1)
    causal = (row_index >= column_index)[:, :, None]

    def advance(carried_state, block_item):
        block_values, block_inputs, block_readout, block_steps = block_item
        cumulative = jnp.cumsum(block_steps * decay_rates[None, :], axis=0)
        log_gaps = jnp.where(causal, cumulative[:, None, :] - cumulative[None, :, :], 0.0)
        decay_weights = jnp.where(causal, jnp.exp(log_gaps), 0.0)
        scores = jnp.dot(block_readout, block_inputs.T, precision=highest)
        mixing = scores[:, :, None] * decay_weights * block_steps[None, :, :]
        within = jnp.einsum('tsh,shp->thp', mixing, block_values, precision=highest)
        carried = jnp.exp(cumulative)[:, :, None] * jnp.einsum('tn,hpn->thp', block_readout, carried_state, precision=highest)
        outputs = within + carried + skip_gain[None, :, None] * block_values
        tail_weight = jnp.exp(cumulative[-1:, :] - cumulative) * block_steps
        next_state = jnp.exp(cumulative[-1])[:, None, None] * carried_state + jnp.einsum('sh,sn,shp->hpn', tail_weight, block_inputs, block_values, precision=highest)
        return (next_state, (outputs, cumulative))
    final_state, (outputs, cumulatives) = lax.scan(advance, initial, (value_blocks, input_blocks, readout_blocks, step_blocks))
    return (outputs.reshape(total_length, local_heads, head_width), final_state, cumulatives)

def mixer(values, input_vectors, readout, step_raw, step_bias, decay_log, skip_gain, initial):
    step_sizes = jax.nn.softplus(step_raw + step_bias[None, :])
    decay_rates = -jnp.exp(decay_log)
    outputs, final_state, cumulatives = group_pass(values, input_vectors, readout, step_sizes, decay_rates, skip_gain, initial)
    return (outputs, final_state)

def silu_slope(inputs):
    sigmoid_values = jax.nn.sigmoid(inputs)
    return sigmoid_values * (1.0 + inputs * (1.0 - sigmoid_values))

def reference(block_in, out_cotangent, norm_gain, gate_proj, value_proj, state_proj, step_proj, conv_value, conv_state, conv_value_bias, conv_state_bias, step_bias, decay_log, skip_gain, gated_gain, out_proj):
    conv_taps = conv_value.shape[0]
    channels = DI + 2 * N
    conv_weight = jnp.concatenate([conv_value, conv_state.reshape(conv_taps, 2 * N)], axis=1)
    conv_bias = jnp.concatenate([conv_value_bias, conv_state_bias.reshape(2 * N)])

    def one_sequence(totals, sequence_pair):
        seq_in, seq_cotangent = sequence_pair
        flat_in = seq_in.astype(jnp.float32)
        inv_rms = lax.rsqrt(lax.optimization_barrier(jnp.mean(flat_in * flat_in, axis=1, keepdims=True)) + 1e-05)
        normed = (flat_in * inv_rms * norm_gain[None, :]).astype(jnp.bfloat16)
        gate_pre = jnp.dot(normed, gate_proj, preferred_element_type=jnp.float32).astype(jnp.bfloat16)
        value_pre = jnp.dot(normed, value_proj, preferred_element_type=jnp.float32).astype(jnp.bfloat16)
        state_pre = jnp.stack([jnp.dot(normed, state_proj[0], preferred_element_type=jnp.float32), jnp.dot(normed, state_proj[1], preferred_element_type=jnp.float32)], axis=1).astype(jnp.bfloat16)
        step_raw = jnp.dot(normed, step_proj, preferred_element_type=jnp.float32)
        conv_in = jnp.concatenate([value_pre, state_pre.reshape(LENGTH, 2 * N)], axis=1)
        padded = jnp.concatenate([jnp.zeros((conv_taps - 1, channels), jnp.bfloat16), conv_in], axis=0).astype(jnp.float32)
        pre_act = jnp.zeros((LENGTH, channels), jnp.float32) + conv_bias[None, :]
        for tap_index in range(conv_taps):
            pre_act = pre_act + conv_weight[tap_index][None, :] * padded[tap_index:tap_index + LENGTH]
        activated = jax.nn.silu(pre_act).astype(jnp.bfloat16)
        values = activated[:, :DI].astype(jnp.float32).reshape(LENGTH, H, P_SIZE)
        input_vectors = activated[:, DI:DI + N].astype(jnp.float32)
        readout = activated[:, DI + N:].astype(jnp.float32)
        initial = jnp.zeros((H, P_SIZE, N), jnp.float32)
        primal, pullback = jax.vjp(mixer, values, input_vectors, readout, step_raw, step_bias, decay_log, skip_gain, initial)
        mixed = primal[0].reshape(LENGTH, DI)
        gate_value = gate_pre.astype(jnp.float32)
        gate_act = jax.nn.silu(gate_value)
        gated = mixed * gate_act
        gated_rms = lax.rsqrt(lax.optimization_barrier(jnp.mean(gated * gated, axis=1, keepdims=True)) + 1e-05)
        gated_norm = (gated * gated_rms * gated_gain[None, :]).astype(jnp.bfloat16)
        block_out = (flat_in + jnp.dot(gated_norm, out_proj, preferred_element_type=jnp.float32)).astype(jnp.bfloat16)
        d_norm_out = jnp.dot(seq_cotangent, out_proj.T, preferred_element_type=jnp.float32)
        out_proj_grad = jnp.dot(gated_norm.T, seq_cotangent, preferred_element_type=jnp.float32)
        gated_gain_grad = lax.optimization_barrier(jnp.sum(d_norm_out * gated * gated_rms, axis=0))
        scaled = d_norm_out * gated_gain[None, :]
        d_gated = gated_rms * scaled - gated * gated_rms ** 3 * lax.optimization_barrier(jnp.mean(scaled * gated, axis=1, keepdims=True))
        d_mixed = d_gated * gate_act
        d_gate = (d_gated * mixed * silu_slope(gate_value)).astype(jnp.bfloat16)
        d_values, d_inputs, d_readout, d_step_raw, step_bias_grad, decay_grad, skip_grad, unused = pullback((d_mixed.reshape(LENGTH, H, P_SIZE), jnp.zeros_like(primal[1])))
        d_pre = jnp.concatenate([d_values.reshape(LENGTH, DI), d_inputs, d_readout], axis=1) * silu_slope(pre_act)
        d_extended = jnp.concatenate([d_pre, jnp.zeros((conv_taps - 1, channels), jnp.float32)], axis=0)
        d_conv_in = jnp.zeros((LENGTH, channels), jnp.float32)
        conv_terms = []
        for tap_index in range(conv_taps):
            offset = conv_taps - 1 - tap_index
            d_conv_in = d_conv_in + conv_weight[tap_index][None, :] * d_extended[offset:offset + LENGTH]
            conv_terms.append(lax.optimization_barrier(jnp.sum(d_pre * padded[tap_index:tap_index + LENGTH], axis=0)))
        conv_grad = jnp.stack(conv_terms)
        conv_bias_grad = lax.optimization_barrier(jnp.sum(d_pre, axis=0))
        d_conv_in = d_conv_in.astype(jnp.bfloat16)
        d_value_pre = d_conv_in[:, :DI]
        d_state_pre = d_conv_in[:, DI:].reshape(LENGTH, 2, N)
        d_step = d_step_raw.astype(jnp.bfloat16)
        normed_rows = normed.T
        gate_grad = jnp.dot(normed_rows, d_gate, preferred_element_type=jnp.float32)
        value_grad = jnp.dot(normed_rows, d_value_pre, preferred_element_type=jnp.float32)
        state_grad = jnp.stack([jnp.dot(normed_rows, d_state_pre[:, 0], preferred_element_type=jnp.float32), jnp.dot(normed_rows, d_state_pre[:, 1], preferred_element_type=jnp.float32)])
        step_grad = jnp.dot(normed_rows, d_step, preferred_element_type=jnp.float32)
        d_normed = jnp.dot(d_gate, gate_proj.T, preferred_element_type=jnp.float32)
        d_normed = d_normed + jnp.dot(d_value_pre, value_proj.T, preferred_element_type=jnp.float32)
        d_normed = d_normed + jnp.dot(d_state_pre[:, 0], state_proj[0].T, preferred_element_type=jnp.float32)
        d_normed = d_normed + jnp.dot(d_state_pre[:, 1], state_proj[1].T, preferred_element_type=jnp.float32)
        d_normed = d_normed + jnp.dot(d_step, step_proj.T, preferred_element_type=jnp.float32)
        norm_grad = lax.optimization_barrier(jnp.sum(d_normed * flat_in * inv_rms, axis=0))
        scaled_in = d_normed * norm_gain[None, :]
        input_grad = seq_cotangent.astype(jnp.float32) + inv_rms * scaled_in - flat_in * inv_rms ** 3 * lax.optimization_barrier(jnp.mean(scaled_in * flat_in, axis=1, keepdims=True))
        grads = (norm_grad, gate_grad, value_grad, state_grad, step_grad, conv_grad[:, :DI], conv_grad[:, DI:].reshape(conv_taps, 2, N), conv_bias_grad[:DI], conv_bias_grad[DI:].reshape(2, N), step_bias_grad, decay_grad, skip_grad, gated_gain_grad, out_proj_grad)
        totals = jax.tree.map(lambda earlier_sum, new_term: earlier_sum + new_term, totals, grads)
        return (totals, (block_out, input_grad))
    shapes = (norm_gain, gate_proj, value_proj, state_proj, step_proj, conv_value, conv_state, conv_value_bias, conv_state_bias, step_bias, decay_log, skip_gain, gated_gain, out_proj)
    zero_totals = jax.tree.map(lambda weight: jnp.zeros(weight.shape, jnp.float32), shapes)
    totals, (block_outs, input_grads) = lax.scan(one_sequence, zero_totals, (block_in, out_cotangent))
    return (block_outs, input_grads, totals[0], totals[1], totals[2], totals[3], totals[4], totals[5], totals[6], totals[7], totals[8], totals[9], totals[10], totals[11], totals[12], totals[13])
```

```python
import functools

import jax
import jax.numpy as jnp
from jax import lax
from jax.experimental import pallas as pl
from jax.experimental.pallas import tpu as pltpu
from jax.sharding import PartitionSpec as P

f32, bf16 = jnp.float32, jnp.bfloat16
HI = lax.Precision.HIGHEST
MESH = pl.DeviceIdType.MESH
Q = 128
TILE = 32
HALO = 16
EPS = 1e-05
NN, NT, TN = ((1,), (0,)), ((1,), (1,)), ((0,), (0,))


def mm(a, b, dims=NN, precision=None):
    return lax.dot_general(
        a, b, (dims, ((), ())), preferred_element_type=f32, precision=precision
    )


def mm2(a, b, dims=NN):
    high = b.astype(bf16)
    return mm(a, high, dims) + mm(a, (b - high.astype(f32)).astype(bf16), dims)


def at(i, n):
    return pl.ds(pl.multiple_of(i * n, n), n)


def loop(count, body):
    def step(i, carry):
        body(i)
        return carry

    lax.fori_loop(0, count, step, 0)


def iota(shape, axis):
    return lax.broadcasted_iota(jnp.int32, shape, axis)


def lane_heads(heads, width):
    shift = (width // heads).bit_length() - 1
    return ((iota((Q, width), 1) >> shift) == iota((Q, width), 0)).astype(f32)


def triangle(keep):
    return jnp.where(keep(iota((Q, Q), 0), iota((Q, Q), 1)), 1.0, 0.0)


def fold8(v):
    return jnp.sum(v.reshape(v.shape[0] // 8, 8, v.shape[1]), axis=0)


def row_of(v, e):
    return mm(jnp.broadcast_to(v, (8, Q)), e, precision=HI)[0:1]


def normalize(v, gain):
    inv = lax.rsqrt(jnp.mean(v * v, axis=1, keepdims=True) + EPS)
    return (v * inv * gain).astype(bf16), inv


def remote(src, dst, send, recv, **place):
    return pltpu.make_async_remote_copy(
        src_ref=src, dst_ref=dst, send_sem=send, recv_sem=recv, device_id=place, device_id_type=MESH
    )


class Fold:
    def __init__(self, part, near, far, sems, tiles):
        self.part, self.near, self.far, self.tiles = part, near, far, tiles
        self.a, self.b, self.c, self.d = sems
        self.rows = part.shape[0] // tiles
        place = lax.axis_index("head")
        self.inner = (place == 1) | (place == 2)
        self.beside = jnp.where(place < 2, 1 - place, 5 - place)
        self.across = 3 - place

    def outward(self, i, src):
        r = at(i, self.rows)
        return remote(src.at[r], self.near.at[r], self.a.at[i], self.b.at[i], head=self.beside)

    def middle(self, i):
        r = at(i, self.rows)
        return remote(self.part.at[r], self.far.at[r], self.c.at[i], self.d.at[i], head=self.across)

    def begin(self, first, count):
        @pl.when(jnp.logical_not(self.inner))
        def _():
            loop(count, lambda i: self.outward(first + i, self.part).start())

    def add(self, dst, u, v, i):
        def tile(j):
            r = at(i * (self.rows // TILE) + j, TILE)
            dst[r, :] = (u[r, :].astype(f32) + v[r, :].astype(f32)).astype(bf16)

        loop(self.rows // TILE, tile)

    def one(self, i):
        @pl.when(self.inner)
        def _():
            self.outward(i, self.near).wait_recv()
            self.add(self.part, self.part, self.near, i)
            self.middle(i).start()

    def two(self, i):
        @pl.when(self.inner)
        def _():
            self.middle(i).wait_recv()
            self.add(self.near, self.part, self.far, i)
            self.outward(i, self.near).start()

    def end(self):
        @pl.when(self.inner)
        def _():
            def done(i):
                self.middle(i).wait_send()
                self.outward(i, self.near).wait_send()

            loop(self.tiles, done)

        @pl.when(jnp.logical_not(self.inner))
        def _():
            def done(i):
                self.outward(i, self.part).wait_send()
                self.outward(i, self.near).wait_recv()

            loop(self.tiles, done)


class Relay:
    def __init__(self, blocks, slots, send, recv, count, way):
        self.blocks, self.slots, self.send, self.recv = blocks, slots, send, recv
        self.count, self.way = count, way
        self.place = lax.axis_index("seq")

    def copies(self, d, source):
        to = self.place + self.way * d
        return [
            remote(b, s.at[source], self.send.at[j, d - 1], self.recv.at[j, d - 1], seq=to)
            for j, (b, s) in enumerate(zip(self.blocks, self.slots))
        ]

    def reaches(self, d):
        return self.place + d < self.count if self.way > 0 else self.place >= d

    def hears(self, d):
        return self.place >= d if self.way > 0 else self.place + d < self.count

    def start(self):
        for d in range(1, self.count):

            @pl.when(self.reaches(d))
            def _():
                for c in self.copies(d, self.place):
                    c.start()

    def gather(self, state, e):
        state[...] = jnp.zeros_like(state)
        for d in range(self.count - 1, 0, -1):

            @pl.when(self.hears(d))
            def _():
                source = self.place - self.way * d
                for c in self.copies(d, source):
                    c.wait_recv()
                for s in range(state.shape[0]):
                    decay = mm(jnp.exp(self.slots[1][source, s]), e[...], precision=HI)[0:1]
                    state[s] = state[s] * decay + self.slots[0][source, s].astype(f32)

    def finish(self):
        for d in range(1, self.count):

            @pl.when(self.reaches(d))
            def _():
                for c in self.copies(d, self.place):
                    c.wait_send()


def block(
    dims,
    x_in, cot_in, gain, wg_in, wv_in, spt, stp, wo_in, cst, cwv, hp, sk, gg,
    outs, dnorm, grads, state_out, small_out,
    xb, cot, wg, wv, wst, wo, cwt, cw, xh,
    nt, inv, gate, pad, slope, act, dt, sg, cum, cum_t, dt_t, entry, ys, dy, gn, dg, later,
    dcs, e, st, work, off, tt, stats, stats_t, stats_in,
    fin, tot, slots, slots_t, chained,
    part1, far1, part2, far2,
    gr, gr_in, gr_pieces, gr_sum, sg_in, sg_pieces, sg_line, sg_sum,
    acc, hsums, sums, nsums, smallz, smallz_in, small, small_two, small_in, nx, edge8,
    load, halo_sem, wt_s, wt_r, f_s, f_r, b_s, b_r, st_s, st_r, nx_s, nx_r,
    z1, z2, ga_s, ga_r, gb_s, gb_r, gc_s, gc_r, gd_s, gd_r,
    sa_s, sa_r, sb_s, sb_r, sz_s, sz_r, sc_s, sc_r, sd_s, sd_r, m1_s, m1_r, m2_s, m2_r,
):
    S, L, seqs, lines, tiles = dims
    T, D = xb.shape
    C = wg.shape[1]
    W = C + 2 * Q
    NC = L // Q
    own = spt.shape[0] // 2
    full = C * lines
    ps, pc, ph = lax.axis_index("seq"), lax.axis_index("sample"), lax.axis_index("head")
    other = 1 - pc
    group = 2 * seqs
    DC = D // C
    mine = ps * 2 + pc
    near1, near2 = outs, dnorm
    nb = part1

    def peer(i):
        p = lax.rem(mine + i, group)
        return {"seq": p // 2, "sample": lax.rem(p, 2)}

    def line(i):
        return lax.rem(ph + i, lines)

    def ring(i):
        return lax.rem(ps + i, seqs)

    moves = [
        pltpu.make_async_copy(x_in, xb, load.at[0]),
        pltpu.make_async_copy(wg_in, wg, load.at[1]),
        pltpu.make_async_copy(wv_in, wv, load.at[2]),
        pltpu.make_async_copy(stp, wst.at[pl.ds(2 * Q, Q)], load.at[3]),
        pltpu.make_async_copy(spt.at[pl.ds(0, own)], wst.at[at(ph, own)], load.at[4]),
        pltpu.make_async_copy(
            spt.at[pl.ds(own, own)], wst.at[pl.ds(pl.multiple_of(Q + ph * own, own), own)], load.at[5]
        ),
        pltpu.make_async_copy(cst.at[pl.ds(0, own)], cwt.at[at(ph, own)], load.at[6]),
        pltpu.make_async_copy(
            cst.at[pl.ds(own, own)], cwt.at[pl.ds(pl.multiple_of(Q + ph * own, own), own)], load.at[7]
        ),
        pltpu.make_async_copy(cot_in, cot, load.at[8]),
        pltpu.make_async_copy(wo_in, wo, load.at[9]),
    ]
    for m in moves:
        m.start()
    barrier = pltpu.get_barrier_semaphore()
    for i in range(1, group):
        pl.semaphore_signal(barrier, inc=1, device_id=peer(i), device_id_type=MESH)
    for i in range(1, lines):
        pl.semaphore_signal(barrier, inc=1, device_id={"head": line(i)}, device_id_type=MESH)
    pl.semaphore_wait(barrier, group - 1 + lines - 1)

    def halo(s):
        return remote(
            x_in.at[pl.ds(s * L + L - HALO, HALO)], xh.at[pl.ds(s * HALO, HALO)],
            halo_sem.at[0, s], halo_sem.at[1, s], seq=ps + 1,
        )

    @pl.when(ps < seqs - 1)
    def _():
        for s in range(S):
            halo(s).start()

    @pl.when(ps == 0)
    def _():
        xh[...] = jnp.zeros_like(xh)

    def weights(i):
        to = line(i)
        low = at(ph, own)
        high = pl.ds(pl.multiple_of(Q + ph * own, own), own)
        parts = [
            (spt.at[pl.ds(0, own)], wst.at[low]),
            (spt.at[pl.ds(own, own)], wst.at[high]),
            (cst.at[pl.ds(0, own)], cwt.at[low]),
            (cst.at[pl.ds(own, own)], cwt.at[high]),
        ]
        return [
            remote(a, b, wt_s.at[j, i - 1], wt_r.at[j, i - 1], head=to)
            for j, (a, b) in enumerate(parts)
        ]

    for i in range(1, lines):
        for c in weights(i):
            c.start()

    e[...] = lane_heads(C // 64, C)
    moves[0].wait()

    def norm_rows(r):
        n, i = normalize(xb[at(r, TILE), :].astype(f32), gain[...])
        nb[at(r, TILE), :] = n
        inv[at(r, TILE), :] = jnp.broadcast_to(i, (TILE, Q))

    loop(T // TILE, norm_rows)
    moves[1].wait()
    moves[2].wait()

    def project(s):
        n = nb[at(s, L), :]
        gate[at(s, L), :] = mm(n, wg[...]).astype(bf16)
        pad[s, HALO:, 0:C] = mm(n, wv[...]).astype(bf16)

    loop(S, project)

    def turn(i):
        nt[:, at(i, 256)] = nb[at(i, 256), :].T

    loop(T // 256, turn)
    for m in moves[3:8]:
        m.wait()
    for i in range(1, lines):
        for c in weights(i):
            c.wait_recv()

    @pl.when(ps > 0)
    def _():
        for s in range(S):
            halo(s).wait_recv()

    def project_state(s):
        both = mm(nb[at(s, L), :], wst[...], NT)
        pad[s, HALO:, C:] = both[:, 0 : 2 * Q].astype(bf16)
        sg[at(s, L), :] = both[:, 2 * Q :]
        edge, unused = normalize(xh[at(s, HALO), :].astype(f32), gain[...])
        pad[s, 0:HALO, 0:C] = mm(edge, wv[...]).astype(bf16)
        pad[s, 0:HALO, C:] = mm(edge, wst[0 : 2 * Q, :], NT).astype(bf16)

    loop(S, project_state)
    cw[:, 0:C] = cwv[...]
    cw[:, C : C + Q] = cwt[0:Q, :].T[0:8]
    cw[:, C + Q :] = cwt[Q:, :].T[0:8]

    for s in range(S):

        def conv_rows(r):
            for lo in range(0, W, 256):
                lanes = slice(lo, lo + 256)
                w = pad[s, pl.ds(pl.multiple_of(r * TILE, TILE), TILE + HALO), lanes].astype(f32)
                v = cw[4:5, lanes] + cw[0:1, lanes] * w[13 : 13 + TILE]
                for k in range(1, 4):
                    v = v + cw[k : k + 1, lanes] * w[13 + k : 13 + k + TILE]
                g = jax.nn.sigmoid(v)
                rows = at(r + s * (L // TILE), TILE)
                act[rows, lanes] = (v * g).astype(bf16)
                slope[rows, lanes] = g * (1.0 + v * (1.0 - g))

        loop(L // TILE, conv_rows)

    def steps(c):
        z = sg[at(c, Q), :] + hp[0:1, :]
        d = jax.nn.softplus(z)
        dt[at(c, Q), :] = d
        sg[at(c, Q), :] = jax.nn.sigmoid(z)
        run = mm(triangle(lambda i, j: i >= j), d * hp[1:2, :], precision=HI)
        cum[at(c, Q), :] = run
        cum_t[:, at(c, Q)] = run.T[0:8]
        dt_t[:, at(c, Q)] = d.T[0:8]

    loop(T // Q, steps)
    for s in range(S):
        st[...] = jnp.zeros_like(st)
        tot[s] = jnp.zeros((8, Q), f32)

        def chunk(k):
            c = s * NC + k
            run = cum[at(c, Q), :]
            last = run[Q - 1 : Q, :]
            tail = mm(jnp.exp(last - run) * dt[at(c, Q), :], e[...], precision=HI)
            xt = act[at(c, Q), 0:C].astype(f32) * tail
            entry[c] = st[...]
            st[...] = st[...] * row_of(jnp.exp(last), e[...]) + mm2(
                act[at(c, Q), C : C + Q], xt, TN
            )
            tot[s] += jnp.broadcast_to(last, (8, Q))

        loop(NC, chunk)
        fin[s] = st[...].astype(bf16)
    relay = Relay((fin, tot), (slots, slots_t), f_s, f_r, seqs, 1)
    relay.start()

    def weights_of(h, here, causal):
        gap = cum[here, h : h + 1] - cum_t[h : h + 1, here]
        return jnp.exp(jnp.where(causal, gap, -1e30)) * dt_t[h : h + 1, here]

    def within(c):
        here = at(c, Q)
        scores = mm(act[here, C + Q :], act[here, C : C + Q], NT)
        causal = iota((Q, Q), 0) >= iota((Q, Q), 1)
        upper = iota((Q, Q), 1) >= 64
        for p in range(C // Q):
            xp = act[here, p * Q : (p + 1) * Q]
            y = jnp.zeros((Q, Q), f32)
            for o in range(2):
                m = (scores * weights_of(2 * p + o, here, causal)).astype(bf16)
                y = y + mm(m, jnp.where(upper == bool(o), xp, jnp.zeros_like(xp)))
            ys[here, p * Q : (p + 1) * Q] = y

    loop(T // Q, within)
    moves[8].wait()
    moves[9].wait()

    def cotangent(i):
        dy[at(i, 512), :] = mm(cot[at(i, 512), :], wo[...], NT)

    loop(T // 512, cotangent)
    relay.gather(chained, e)

    for s in range(S):
        off[...] = jnp.zeros_like(off)

        def across(k):
            c = s * NC + k
            here = at(c, Q)
            si = entry[c] + row_of(jnp.exp(off[0:1, :]), e[...]) * chained[s]
            entry[c] = si
            run = cum[here, :]
            work[0] = mm(jnp.exp(run), e[...], precision=HI) * mm2(
                act[here, C + Q :], si
            )
            off[...] += jnp.broadcast_to(run[Q - 1 : Q, :], (8, Q))

            def tile(r):
                rows = at(c * (Q // TILE) + r, TILE)
                y = ys[rows, :] + work[0, at(r, TILE), :]
                ys[rows, :] = y
                m = y + sk[...] * act[rows, 0:C].astype(f32)
                g = gate[rows, :].astype(f32)
                gated = m * (g * jax.nn.sigmoid(g))
                a = jnp.sum(gated * gated, axis=1, keepdims=True)
                b = jnp.sum(dy[rows, :] * gg[...] * gated, axis=1, keepdims=True)
                lane = iota((TILE, Q), 1)
                stats[at(r, TILE), :] = jnp.where(lane == 0, a, jnp.where(lane == 1, b, 0.0))

            loop(Q // TILE, tile)
            stats_t[:, here] = stats[...].T[0:8]

        loop(NC, across)

    def stat(i):
        return remote(stats_t, stats_in.at[i - 1], st_s.at[i - 1], st_r.at[i - 1], head=line(i))

    for i in range(1, lines):
        stat(i).start()
    relay.finish()
    sums[...] = jnp.zeros_like(sums)
    for i in range(1, lines):
        stat(i).wait_recv()

    fold1 = Fold(part1, near1, far1, [z1.at[j] for j in range(4)], tiles)
    for s in range(S):

        def gate_back(k):
            c = s * NC + k
            here = at(c, Q)
            t = stats_t[:, here]
            for i in range(1, lines):
                t = t + stats_in[i - 1, :, here]
            t = t.T
            rms = lax.rsqrt(t[:, 0:1] / full + EPS)
            tt[:, 0:1] = rms
            tt[:, 1:2] = rms * rms * rms * (t[:, 1:2] / full)

            def tile(r):
                rows = at(c * (Q // TILE) + r, TILE)
                near = at(r, TILE)
                rm, co = tt[near, 0:1], tt[near, 1:2]
                x = act[rows, 0:C].astype(f32)
                m = ys[rows, :] + sk[...] * x
                g = gate[rows, :].astype(f32)
                sig = jax.nn.sigmoid(g)
                ga = g * sig
                gated = m * ga
                scaled_rows = gated * rm
                gn[rows, :] = (scaled_rows * gg[...]).astype(bf16)
                d = dy[rows, :]
                dgd = rm * (d * gg[...]) - gated * co
                dmix = dgd * ga
                dg[rows, :] = (dgd * m * (sig * (1.0 + g * (1.0 - sig)))).astype(bf16)
                dy[rows, :] = dmix
                sums[0:8, :] += fold8(d * scaled_rows)
                sums[8:16, :] += fold8(dmix * x)

            loop(Q // TILE, tile)

        loop(NC, gate_back)
        part1[s * L : (s + 1) * L, :] = mm(gn[s * L : (s + 1) * L, :], wo[...]).astype(bf16)
        fold1.begin(s * (tiles // S), tiles // S)

    def spread_dy(c):
        return mm(jnp.exp(cum[at(c, Q), :]), e[...], precision=HI) * dy[at(c, Q), :]

    for s in range(S):
        st[...] = jnp.zeros_like(st)

        def back(k):
            c = s * NC + NC - 1 - k
            last = cum[pl.ds(pl.multiple_of(c * Q + Q - 8, 8), 8), :][7:8]
            later[c] = st[...]
            st[...] = st[...] * row_of(jnp.exp(last), e[...]) + mm2(
                act[at(c, Q), C + Q :], spread_dy(c), TN
            )

        loop(NC, back)
        fin[s] = st[...].astype(bf16)
    relay2 = Relay((fin, tot), (slots, slots_t), b_s, b_r, seqs, -1)
    relay2.start()

    def outer(i):
        half = mm(gn[...], cot[:, at(i, 512)], TN)
        gr[0, at(i, 512), :] = half.astype(bf16)

    loop(D // 512, outer)

    def outer2(i):
        gr[1, at(i, 512), :] = mm(nt[at(i, 512), :], dg[...]).astype(bf16)

    loop(D // 512, outer2)
    HG = D // 2
    PR = HG // seqs

    def pair(k):
        return remote(gr.at[k, at(other, HG)], gr_in.at[k], ga_s.at[k], ga_r.at[k], sample=other)

    pair(0).start()
    pair(1).start()
    relay2.gather(chained, e)
    half = tiles // S

    hsums[...] = jnp.zeros_like(hsums)
    for s in range(S):
        off[...] = jnp.zeros_like(off)

        def state_back(k):
            kk = NC - 1 - k
            c = s * NC + kk
            here = at(c, Q)
            run = cum[here, :]
            last = run[Q - 1 : Q, :]
            ds = later[c] + row_of(jnp.exp(off[0:1, :]), e[...]) * chained[s]
            off[...] += jnp.broadcast_to(last, (8, Q))
            upper = iota((Q, Q), 1) >= 64
            causal = iota((Q, Q), 0) >= iota((Q, Q), 1)
            b, r = act[here, C : C + Q], act[here, C + Q :]
            scores = mm(r, b, NT)
            dsc = jnp.zeros((Q, Q), f32)
            for p in range(C // Q):
                lanes = slice(p * Q, (p + 1) * Q)
                xp = act[here, lanes]
                dyp = dy[here, lanes].astype(bf16)
                dyl = (dy[here, lanes] - dyp.astype(f32)).astype(bf16)
                dx = jnp.zeros((Q, Q), f32)
                for o in range(2):
                    keep = upper == bool(o)
                    dym = jnp.where(keep, dyp, jnp.zeros_like(dyp))
                    dyn = jnp.where(keep, dyl, jnp.zeros_like(dyl))
                    w = weights_of(2 * p + o, here, causal)
                    dsc = dsc + (mm(dym, xp, NT) + mm(dyn, xp, NT)) * w
                    dx = dx + mm((scores * w).astype(bf16), dym, TN)
                work[0, :, lanes] = dx
            d = dt[here, :]
            work[2] = mm(jnp.exp(last - run) * d, e[...], precision=HI)
            work[1] = work[2] * mm2(b, ds)
            bf, rf = b.astype(f32), r.astype(f32)
            d_read = mm(dsc, bf, precision=HI) + mm(spread_dy(c), entry[c], NT, HI)
            d_in = mm(dsc, rf, TN, HI) + mm(act[here, 0:C].astype(f32) * work[2], ds, NT, HI)
            slope[here, C : C + Q] = d_in * slope[here, C : C + Q]
            slope[here, C + Q :] = d_read * slope[here, C + Q :]

            def tile(i):
                rows = at(c * (Q // TILE) + i, TILE)
                near = at(i, TILE)
                x = act[rows, 0:C].astype(f32)
                g = dy[rows, :]
                a, o = work[0, near, :], work[1, near, :]
                work[3, near, :] = g.astype(bf16).astype(f32) * ys[rows, :] - x * a
                work[4, near, :] = x * o
                both = a + o
                work[5, near, :] = x * both
                slope[rows, 0:C] = (both + sk[...] * g) * slope[rows, 0:C]

            loop(Q // TILE, tile)
            ha = mm(work[3], e[...], NT, HI)
            hb = mm(work[4], e[...], NT, HI)
            hc = mm(work[5], e[...], NT, HI)
            crossing = mm(fold8(entry[c] * ds), e[...], NT, HI)
            crossing = jnp.sum(crossing, axis=0, keepdims=True) * jnp.exp(last)
            dlog = (
                mm(triangle(lambda i, j: i <= j), ha, precision=HI)
                + mm(triangle(lambda i, j: i > j), hb, precision=HI)
                + crossing
            )
            g = sg[here, :]
            ratio = jnp.where(d > 1e-30, g / jnp.maximum(d, 1e-30), 1.0)
            rate = hp[1:2, :]
            draw = rate * dlog * g + hc * ratio
            dcs[here, 2 * Q :] = draw.astype(bf16)
            hsums[0:8, :] += fold8(draw)
            hsums[8:16, :] += fold8(rate * dlog * d)
            if s == 0:
                for j in range(half // NC):
                    fold1.one(k * (half // NC) + j)
            else:
                for j in range(half // NC):
                    fold1.one(half + k * (half // NC) + j)
                    fold1.two(k * (half // NC) + j)

        loop(NC, state_back)
        edge8[s] = slope[s * L : s * L + 8, :]

        def next_rows(s):
            return remote(edge8.at[s], nx.at[s], nx_s.at[s], nx_r.at[s], seq=ps - 1)

        @pl.when(ps > 0)
        def _():
            next_rows(s).start()

    def settle(k):
        pair(k).wait_recv()

        def tile(i):
            r = pl.ds(pl.multiple_of(pc * HG + i * TILE, TILE), TILE)
            v = gr[k, r, :].astype(f32) + gr_in[k, at(i, TILE), :].astype(f32)
            gr[k, r, :] = v.astype(bf16)

        loop(HG // TILE, tile)

    def piece(k, i):
        r = pl.ds(pl.multiple_of(pc * HG + ring(i) * PR, PR), PR)
        return remote(gr.at[k, r], gr_pieces.at[k, i - 1], gb_s.at[k, i - 1], gb_r.at[k, i - 1], seq=ring(i))

    for k in range(2):
        settle(k)
        for i in range(1, seqs):
            piece(k, i).start()

    @pl.when(ps == seqs - 1)
    def _():
        nx[...] = jnp.zeros_like(nx)

    @pl.when(ps < seqs - 1)
    def _():
        for s in range(S):
            next_rows(s).wait_recv()

    acc[...] = jnp.zeros_like(acc)
    LT = L // TILE
    for s in range(S):

        def conv_back(r, last):
            for lo in range(0, W, 256):
                lanes = slice(lo, lo + 256)
                if last:
                    w = jnp.concatenate([slope[(s + 1) * L - TILE : (s + 1) * L, lanes], nx[s, :, lanes]], axis=0)
                else:
                    w = slope[pl.ds(pl.multiple_of(s * L + r * TILE, TILE), TILE + 8), lanes]
                u = pad[s, pl.ds(pl.multiple_of(r * TILE, TILE), TILE + HALO), lanes].astype(f32)
                d = w[0:TILE]
                v = cw[3:4, lanes] * d
                for k in range(3):
                    v = v + cw[k : k + 1, lanes] * w[3 - k : 3 - k + TILE]
                rows = at(r + s * LT, TILE)
                if lo < C:
                    gate[rows, lanes] = v.astype(bf16)
                else:
                    dcs[rows, lo - C : lo - C + 256] = v.astype(bf16)
                for k in range(4):
                    acc[8 * k : 8 * k + 8, lanes] += fold8(d * u[13 + k : 13 + k + TILE])
                acc[32:40, lanes] += fold8(d)

        loop(LT - 1, lambda r: conv_back(r, False))
        conv_back(LT - 1, True)
        for j in range(half // 2):
            fold1.two(half + s * (half // 2) + j)

    nsums[...] = jnp.zeros_like(nsums)
    fold2 = Fold(part2, near2, far2, [z2.at[j] for j in range(4)], tiles)

    def into(s):
        rows = at(s, 256)
        v = (
            mm(dg[rows, :], wg[...], NT)
            + mm(gate[rows, :], wv[...], NT)
            + mm(dcs[rows, :], wst[...])
        )
        part2[rows, :] = v.astype(bf16)
        nsums[...] += fold8(v * xb[rows, :].astype(f32) * inv[rows, 0:1])
        per = tiles * 256 // T
        fold2.begin(s * per, per)

    loop(T // 256, into)

    def outer3(i):
        gr[2, at(i, 512), :] = mm(nt[at(i, 512), :], gate[...]).astype(bf16)

    loop(D // 512, outer3)
    pair(2).start()
    for k in range(D // Q):
        t = mm(nt[k * Q : (k + 1) * Q, :], dcs[...])
        for j in range(2):
            later[j * DC + k * Q // C, :, k * Q % C : k * Q % C + Q] = t[:, j * Q : (j + 1) * Q].T
        row = 8 + 8 * (k * Q // C)
        small[row : row + 8, k * Q % C : k * Q % C + Q] = t[:, 2 * Q :].T[0:8]

    SR = Q // seqs
    keep_state = at(pc, DC)

    def state_pair():
        return remote(later.at[at(other, DC)], sg_in, sa_s, sa_r, sample=other)

    state_pair().start()
    for k in range(5):
        row = jnp.sum(acc[8 * k : 8 * k + 8, :], axis=0, keepdims=True)
        small[k : k + 1, :] = row[:, 0:C]
        smallz[k : k + 1, 0 : 2 * Q] = row[:, C:]
        smallz[k : k + 1, 2 * Q :] = jnp.zeros((1, C - 2 * Q), f32)
    small[5:6, :] = jnp.sum(sums[0:8, :], axis=0, keepdims=True)
    small[6:7, :] = jnp.sum(sums[8:16, :], axis=0, keepdims=True)
    small[7:8, :] = jnp.zeros((1, C), f32)
    small[7:8, 0:Q] = jnp.sum(hsums[0:8, :], axis=0, keepdims=True)
    small[7:8, Q : 2 * Q] = jnp.sum(hsums[8:16, :], axis=0, keepdims=True)
    ngrad = jnp.sum(nsums[...], axis=0, keepdims=True)
    for j in range(D // C):
        smallz[5 + j : 6 + j, :] = ngrad[:, j * C : (j + 1) * C]
    smallz[7:8, :] = jnp.zeros((1, C), f32)

    def to_line(i):
        return remote(smallz, smallz_in.at[i - 1], m1_s.at[i - 1], m1_r.at[i - 1], head=line(i))

    for i in range(1, lines):
        to_line(i).start()
    loop(4, lambda i: fold2.one(i))
    settle(2)
    for i in range(1, seqs):
        piece(2, i).start()
    state_pair().wait_recv()
    later[keep_state] = later[keep_state] + sg_in[...]

    def state_piece(i):
        return remote(later.at[keep_state, at(ring(i), SR)], sg_pieces.at[i - 1], sb_s.at[i - 1], sb_r.at[i - 1], seq=ring(i))

    for i in range(1, seqs):
        state_piece(i).start()
    loop(4, lambda i: fold2.one(4 + i))
    total = smallz[...]
    for i in range(1, lines):
        to_line(i).wait_recv()
        total = total + smallz_in[i - 1]
    small[24:32, :] = total

    def to_core():
        return remote(small, small_two.at[0], m2_s.at[seqs - 1], m2_r.at[seqs - 1], sample=other)

    def to_peer(i):
        return remote(small_two.at[1], small_in.at[i - 1], m2_s.at[i - 1], m2_r.at[i - 1], seq=ring(i))

    to_core().start()
    loop(4, lambda i: fold2.two(0 + i))

    to_core().wait_recv()
    small_two[1] = small[...] + small_two[0]
    for i in range(1, seqs):
        to_peer(i).start()

    for k in range(3):
        for i in range(1, seqs):
            piece(k, i).wait_recv()

        def tile(j):
            r = at(j, TILE)
            v = gr[k, pl.ds(pl.multiple_of(pc * HG + ps * PR + j * TILE, TILE), TILE), :].astype(f32)
            for i in range(1, seqs):
                v = v + gr_pieces[k, i - 1, r, :].astype(f32)
            gr_sum[k, r, :] = v.astype(bf16)
            grads[k, pl.ds(pl.multiple_of(pc * HG + ps * PR + j * TILE, TILE), TILE), :] = v.astype(bf16)

        loop(PR // TILE, tile)

    def spread(k, i):
        r = pl.ds(pl.multiple_of(pc * HG + ps * PR, PR), PR)
        return remote(gr_sum.at[k], grads.at[k, r], gc_s.at[k, i - 1], gc_r.at[k, i - 1], seq=ring(i))

    def hand(k, i):
        q = lax.rem(ps + seqs - i, seqs)
        r = pl.ds(pl.multiple_of(pc * HG + q * PR, PR), PR)
        src = gr_sum.at[k] if i == 0 else grads.at[k, r]
        return remote(src, grads.at[k, r], gd_s.at[k, i], gd_r.at[k, i], sample=other)

    for k in range(3):
        for i in range(1, seqs):
            spread(k, i).start()
        hand(k, 0).start()
    loop(4, lambda i: fold2.one(8 + i))
    loop(4, lambda i: fold2.two(4 + i))

    for i in range(1, seqs):
        state_piece(i).wait_recv()
    v = later[keep_state, at(ps, SR), :]
    for i in range(1, seqs):
        v = v + sg_pieces[i - 1]
    sg_sum[0] = v
    owner = (ps * SR) // own

    def to_owner(i):
        return remote(sg_sum.at[0], sg_line.at[i - 1], sz_s.at[i - 1], sz_r.at[i - 1], head=line(i))

    for i in range(1, lines):

        @pl.when(line(i) == owner)
        def _():
            to_owner(i).start()

    loop(4, lambda i: fold2.one(12 + i))
    loop(4, lambda i: fold2.two(8 + i))
    span = max(own // SR, 1)

    def place_row(q, core):
        return pl.ds(pl.multiple_of(core * own + lax.rem(q * SR, own), SR), SR)

    def state_out_to(i):
        return remote(sg_sum.at[1], state_out.at[:, place_row(ps, pc)], sc_s.at[i - 1], sc_r.at[i - 1], seq=ring(i))

    def state_hand(j, src):
        q = ph * span + j
        return remote(src, state_out.at[:, place_row(q, pc)], sd_s.at[j], sd_r.at[j], sample=other)

    @pl.when(ph == owner)
    def _():
        t = sg_sum[0]
        for i in range(1, lines):
            to_owner(i).wait_recv()
            t = t + sg_line[i - 1]
        sg_sum[1] = t
        state_out[:, place_row(ps, pc), :] = t
        for i in range(1, seqs):
            state_out_to(i).start()

    for j in range(span):
        q = ph * span + j

        @pl.when(q == ps)
        def _():
            state_hand(j, sg_sum.at[1]).start()

        for i in range(1, seqs):

            @pl.when(ring(seqs - i) == q)
            def _():
                remote(
                    sg_sum.at[1], state_out.at[:, place_row(q, pc)], sc_s.at[i - 1], sc_r.at[i - 1], seq=ring(i)
                ).wait_recv()
                state_hand(j, state_out.at[:, place_row(q, pc)]).start()

    for k in range(3):
        for i in range(1, seqs):
            q = lax.rem(ps + seqs - i, seqs)
            r = pl.ds(pl.multiple_of(pc * HG + q * PR, PR), PR)
            remote(gr_sum.at[k], grads.at[k, r], gc_s.at[k, i - 1], gc_r.at[k, i - 1], seq=ring(i)).wait_recv()
            hand(k, i).start()
    loop(4, lambda i: fold2.two(12 + i))
    total = small_two[1]
    for i in range(1, seqs):
        to_peer(i).wait_recv()
        total = total + small_in[i - 1]
    small_out[...] = total

    fold1.end()
    fold2.end()
    relay2.finish()
    for i in range(1, lines):
        for c in weights(i):
            c.wait_send()
        stat(i).wait_send()
        to_line(i).wait_send()

        @pl.when(line(i) == owner)
        def _():
            to_owner(i).wait_send()

    @pl.when(ps < seqs - 1)
    def _():
        for s in range(S):
            halo(s).wait_send()

    @pl.when(ps > 0)
    def _():
        for s in range(S):
            next_rows(s).wait_send()

    for k in range(3):
        pair(k).wait_send()
        for i in range(1, seqs):
            piece(k, i).wait_send()
            spread(k, i).wait_send()
        for i in range(seqs):
            q = lax.rem(ps + seqs - i, seqs)
            r = pl.ds(pl.multiple_of(other * HG + q * PR, PR), PR)
            remote(gr_sum.at[k], grads.at[k, r], gd_s.at[k, i], gd_r.at[k, i], sample=other).wait()
    state_pair().wait_send()
    for i in range(1, seqs):
        state_piece(i).wait_send()

        @pl.when(ph == owner)
        def _():
            state_out_to(i).wait_send()

    for j in range(span):
        q = ph * span + j
        remote(sg_sum.at[1], state_out.at[:, place_row(q, other)], sd_s.at[j], sd_r.at[j], sample=other).wait()
    to_core().wait_send()
    for i in range(1, seqs):
        to_peer(i).wait_send()


def finish(x, cot, gain, dn, outs, gr, block_out, input_grad, gate_grad, value_grad, out_grad):
    def tile(i):
        r = at(i, TILE)
        v = x[r, :].astype(f32)
        block_out[r, :] = (v + outs[r, :].astype(f32)).astype(bf16)
        s = dn[r, :].astype(f32) * gain[...]
        i1 = lax.rsqrt(jnp.mean(v * v, axis=1, keepdims=True) + EPS)
        m = jnp.mean(s * v, axis=1, keepdims=True)
        input_grad[r, :] = cot[r, :].astype(f32) + i1 * s - v * (i1 * i1 * i1 * m)

    loop(x.shape[0] // TILE, tile)
    half = gr.shape[1] // 2
    out_grad[:, 0:half] = gr[0, 0:half, :].astype(f32)
    out_grad[:, half:] = gr[0, half:, :].astype(f32)
    gate_grad[...] = gr[1].astype(f32)
    value_grad[...] = gr[2].astype(f32)


def per_device(
    block_in, out_cotangent, norm_gain, gate_proj, value_proj, state_proj, step_proj,
    conv_value, conv_state, conv_value_bias, conv_state_bias, step_bias, decay_log,
    skip_gain, gated_gain, out_proj,
):
    S, L, D = block_in.shape
    T = S * L
    heads = step_proj.shape[1]
    C = gate_proj.shape[1]
    own = state_proj.shape[2]
    W = C + 2 * Q
    NCH = T // Q
    seqs, lines = lax.axis_size("seq"), lax.axis_size("head")
    tiles = 16
    H = D // 2
    PR = H // seqs
    SR = Q // seqs
    x = block_in.reshape(T, D)
    cot = out_cotangent.reshape(T, D)
    spt = state_proj.transpose(0, 2, 1).reshape(2 * own, D)
    stp = jnp.pad(step_proj.T, ((0, Q - heads), (0, 0)))
    taps = jnp.concatenate([conv_state, conv_state_bias[None]], axis=0)
    cst = jnp.pad(taps.transpose(1, 2, 0).reshape(2 * own, 5), ((0, 0), (0, Q - 5)))
    cwv = jnp.pad(jnp.concatenate([conv_value, conv_value_bias[None]], axis=0), ((0, 3), (0, 0)))
    hp = jnp.pad(jnp.stack([step_bias, -jnp.exp(decay_log)]), ((0, 6), (0, Q - heads)))
    sk = jnp.repeat(skip_gain, C // heads)[None]
    gg = gated_gain[None]
    gain = norm_gain[None]
    vm = pl.BlockSpec(memory_space=pltpu.VMEM)
    hbm = pl.BlockSpec(memory_space=pl.ANY)
    dma = pltpu.SemaphoreType.DMA
    n1, l1 = seqs - 1, lines - 1
    V = pltpu.VMEM
    scratch = [
        V((T, D), bf16), V((T, D), bf16), V((D, C), bf16), V((D, C), bf16), V((3 * Q, D), bf16),
        V((C, D), bf16), V((2 * Q, Q), f32), V((8, W), f32), V((S * HALO, D), bf16),
        V((D, T), bf16), V((T, Q), f32), V((T, C), bf16), V((S, HALO + L, W), bf16), V((T, W), f32),
        V((T, W), bf16), V((T, Q), f32), V((T, Q), f32), V((T, Q), f32), V((8, T), f32), V((8, T), f32),
        V((NCH, Q, C), f32), V((T, C), f32), V((T, C), f32), V((T, C), bf16), V((T, C), bf16),
        V((NCH, Q, C), f32),
        V((T, 3 * Q), bf16), V((Q, C), f32), V((Q, C), f32), V((6, Q, C), f32),
        V((8, Q), f32), V((Q, Q), f32), V((Q, Q), f32), V((8, T), f32), V((l1, 8, T), f32),
        V((S, Q, C), bf16), V((S, 8, Q), f32), V((seqs, S, Q, C), bf16), V((seqs, S, 8, Q), f32),
        V((S, Q, C), f32),
        V((T, D), bf16), V((T, D), bf16), V((T, D), bf16), V((T, D), bf16),
        V((3, D, C), bf16), V((3, H, C), bf16), V((3, n1, PR, C), bf16), V((3, PR, C), bf16),
        V((D // C, Q, C), f32), V((n1, D // C, SR, C), f32), V((l1, D // C, SR, C), f32),
        V((2, D // C, SR, C), f32),
        V((40, W), f32), V((16, Q), f32), V((16, C), f32), V((8, D), f32), V((8, C), f32),
        V((l1, 8, C), f32), V((32, C), f32), V((2, 32, C), f32), V((n1, 32, C), f32), V((S, 8, W), f32), V((S, 8, W), f32),
        dma((10,)), dma((2, S)), dma((4, l1)), dma((4, l1)), dma((2, n1)), dma((2, n1)),
        dma((2, n1)), dma((2, n1)), dma((l1,)), dma((l1,)), dma((S,)), dma((S,)),
        dma((4, tiles)), dma((4, tiles)), dma((3,)), dma((3,)), dma((3, n1)), dma((3, n1)),
        dma((3, n1)), dma((3, n1)), dma((3, seqs)), dma((3, seqs)),
        dma, dma, dma((n1,)), dma((n1,)), dma((l1,)), dma((l1,)), dma((n1,)), dma((n1,)),
        dma((max(own // SR, 1),)), dma((max(own // SR, 1),)), dma((l1,)), dma((l1,)), dma((seqs,)), dma((seqs,)),
    ]
    outs, dnorm, grads, state_out, small = pl.pallas_call(
        functools.partial(block, (S, L, seqs, lines, tiles)),
        out_shape=[
            jax.ShapeDtypeStruct((T, D), bf16), jax.ShapeDtypeStruct((T, D), bf16),
            jax.ShapeDtypeStruct((3, D, C), bf16), jax.ShapeDtypeStruct((D // C, 2 * own, C), f32),
            jax.ShapeDtypeStruct((32, C), f32),
        ],
        in_specs=[hbm, hbm, vm, hbm, hbm, hbm, hbm, hbm, hbm, vm, vm, vm, vm],
        out_specs=[vm] * 5,
        scratch_shapes=scratch,
        name="block",
        compiler_params=pltpu.CompilerParams(
            collective_id=0, has_side_effects=True, vmem_limit_bytes=67043328
        ),
    )(x, cot, gain, gate_proj, value_proj, spt, stp, out_proj, cst, cwv, hp, sk, gg)
    block_out, input_grad, gate_grad, value_grad, out_grad = pl.pallas_call(
        finish,
        out_shape=[
            jax.ShapeDtypeStruct((T, D), bf16), jax.ShapeDtypeStruct((T, D), f32),
            jax.ShapeDtypeStruct((D, C), f32), jax.ShapeDtypeStruct((D, C), f32),
            jax.ShapeDtypeStruct((C, D), f32),
        ],
        in_specs=[vm] * 6,
        out_specs=[vm] * 5,
        name="finish",
        compiler_params=pltpu.CompilerParams(vmem_limit_bytes=60 * 2**20),
    )(x, cot, gain, dnorm, outs, grads)
    ph = lax.axis_index("head")
    state_grad = state_out.reshape(D // C, 2, own, C).transpose(1, 0, 3, 2).reshape(2, D, own)
    step_grad = small[8:24].reshape(D // C, heads, C).transpose(0, 2, 1).reshape(D, heads)
    cs = lax.dynamic_slice_in_dim(small[24:29, 0 : 2 * Q].reshape(5, 2, Q), ph * own, own, 2)
    return (
        block_out.reshape(S, L, D), input_grad.reshape(S, L, D), small[29:31].reshape(D), gate_grad,
        value_grad, state_grad, step_grad, small[0:4], cs[0:4], small[4], cs[4], small[7, 0:heads],
        small[7, Q : Q + heads], jnp.sum(small[6].reshape(heads, C // heads), axis=1), small[5], out_grad,
    )


def solution(mesh):
    tokens = P("sample", "seq", None)
    params = (
        P(), P(None, "head"), P(None, "head"), P(None, None, "head"), P(None, "head"),
        P(None, "head"), P(None, None, "head"), P("head"), P(None, "head"), P("head"),
        P("head"), P("head"), P("head"), P("head", None),
    )
    return jax.shard_map(
        per_device,
        mesh=mesh,
        in_specs=(tokens, tokens) + params,
        out_specs=(tokens, tokens) + params,
        check_vma=False,
    )
```

```python
import functools

import jax
import jax.numpy as jnp
from jax import lax
from jax.experimental import pallas as pl
from jax.experimental.pallas import tpu as pltpu
from jax.sharding import PartitionSpec as P

f32, bf16 = jnp.float32, jnp.bfloat16
HI = lax.Precision.HIGHEST
MESH = pl.DeviceIdType.MESH
Q = 128
TILE = 32
HALO = 16
EPS = 1e-05
NN, NT, TN = ((1,), (0,)), ((1,), (1,)), ((0,), (0,))


def mm(a, b, dims=NN, precision=None):
    return lax.dot_general(
        a, b, (dims, ((), ())), preferred_element_type=f32, precision=precision
    )


def mm2(a, b, dims=NN):
    high = b.astype(bf16)
    return mm(a, high, dims) + mm(a, (b - high.astype(f32)).astype(bf16), dims)


def at(i, n):
    return pl.ds(pl.multiple_of(i * n, n), n)


def loop(count, body, each=1):
    def step(i, carry):
        for j in range(each):
            body(i * each + j)
        return carry

    lax.fori_loop(0, count // each, step, 0)


def iota(shape, axis):
    return lax.broadcasted_iota(jnp.int32, shape, axis)


def lane_heads(heads, width):
    shift = (width // heads).bit_length() - 1
    return ((iota((Q, width), 1) >> shift) == iota((Q, width), 0)).astype(f32)


def triangle(keep):
    return jnp.where(keep(iota((Q, Q), 0), iota((Q, Q), 1)), 1.0, 0.0)


def fold8(v):
    return jnp.sum(v.reshape(v.shape[0] // 8, 8, v.shape[1]), axis=0)


def row_of(v, e):
    return mm(jnp.broadcast_to(v, (8, Q)), e, precision=HI)[0:1]


def normalize(v, gain):
    inv = lax.rsqrt(jnp.mean(v * v, axis=1, keepdims=True) + EPS)
    return (v * inv * gain).astype(bf16), inv


def remote(src, dst, send, recv, **place):
    return pltpu.make_async_remote_copy(
        src_ref=src, dst_ref=dst, send_sem=send, recv_sem=recv, device_id=place, device_id_type=MESH
    )


class Fold:
    def __init__(self, part, near, far, sems, tiles):
        self.part, self.near, self.far, self.tiles = part, near, far, tiles
        self.a, self.b, self.c, self.d = sems
        self.rows = part.shape[0] // tiles
        place = lax.axis_index("head")
        self.inner = (place == 1) | (place == 2)
        self.beside = jnp.where(place < 2, 1 - place, 5 - place)
        self.across = 3 - place

    def outward(self, i, src):
        r = at(i, self.rows)
        return remote(src.at[r], self.near.at[r], self.a.at[i], self.b.at[i], head=self.beside)

    def middle(self, i):
        r = at(i, self.rows)
        return remote(self.part.at[r], self.far.at[r], self.c.at[i], self.d.at[i], head=self.across)

    def begin(self, first, count):
        @pl.when(jnp.logical_not(self.inner))
        def _():
            loop(count, lambda i: self.outward(first + i, self.part).start())

    def add(self, dst, u, v, i):
        def tile(j):
            r = at(i * (self.rows // TILE) + j, TILE)
            dst[r, :] = (u[r, :].astype(f32) + v[r, :].astype(f32)).astype(bf16)

        loop(self.rows // TILE, tile)

    def one(self, i):
        @pl.when(self.inner)
        def _():
            self.outward(i, self.near).wait_recv()
            self.add(self.part, self.part, self.near, i)
            self.middle(i).start()

    def two(self, i):
        @pl.when(self.inner)
        def _():
            self.middle(i).wait_recv()
            self.add(self.near, self.part, self.far, i)
            self.outward(i, self.near).start()

    def step(self, j, lag=2):
        if isinstance(j, int):
            if j < self.tiles:
                self.one(j)
            if 0 <= j - lag < self.tiles:
                self.two(j - lag)
            return

        @pl.when(j < self.tiles)
        def _():
            self.one(j)

        @pl.when((j >= lag) & (j < self.tiles + lag))
        def _():
            self.two(j - lag)

    def end(self):
        @pl.when(self.inner)
        def _():
            def done(i):
                self.middle(i).wait_send()
                self.outward(i, self.near).wait_send()

            loop(self.tiles, done)

        @pl.when(jnp.logical_not(self.inner))
        def _():
            def done(i):
                self.outward(i, self.part).wait_send()
                self.outward(i, self.near).wait_recv()

            loop(self.tiles, done)


class Relay:
    def __init__(self, seq, blocks, slots, sems, count, way):
        self.seq, self.blocks, self.slots, self.sems = seq, blocks, slots, sems
        self.count, self.way = count, way
        self.place = lax.axis_index("seq")

    def copies(self, d, source):
        to = self.place + self.way * d
        return [
            remote(
                b.at[self.seq], s.at[source, self.seq], self.sems.at[0, j, self.seq, d - 1],
                self.sems.at[1, j, self.seq, d - 1], seq=to,
            )
            for j, (b, s) in enumerate(zip(self.blocks, self.slots))
        ]

    def reaches(self, d):
        return self.place + d < self.count if self.way > 0 else self.place >= d

    def hears(self, d):
        return self.place >= d if self.way > 0 else self.place + d < self.count

    def start(self):
        for d in range(1, self.count):

            @pl.when(self.reaches(d))
            def _():
                for c in self.copies(d, self.place):
                    c.start()

    def gather(self, state, e):
        q = self.seq
        state[q] = jnp.zeros(state.shape[1:], f32)
        for d in range(self.count - 1, 0, -1):

            @pl.when(self.hears(d))
            def _():
                source = self.place - self.way * d
                for c in self.copies(d, source):
                    c.wait_recv()
                decay = mm(jnp.exp(self.slots[1][source, q]), e[...], precision=HI)[0:1]
                state[q] = state[q] * decay + self.slots[0][source, q].astype(f32)

    def finish(self):
        for d in range(1, self.count):

            @pl.when(self.reaches(d))
            def _():
                for c in self.copies(d, self.place):
                    c.wait_send()


def block(
    dims,
    x_in, cot_in, gain, wg_in, wv_in, spt, stp, wo_in, cs, csb, cv, cvb, sbias, dlog_in, skip, gg,
    outs, dnorm, grads, state_out, small_out,
    xb, cot, wg, wv, wst, wo, tapb, taps, cw, hp, sk, xh,
    nt, inv, gate, pad, slope, act, dt, sg, cum, cum_t, dt_t, entry, ys, dy, gn, dg, later,
    dcs, e, st, work, off, tt, stats, stats_t, stats_in,
    fin, tot, slots, slots_t, chained,
    part1, far1, part2, far2,
    gr, gr_in, gr_pieces, gr_sum, sg_in, sg_pieces, sg_line, sg_sum,
    acc, hsums, sums, nsums, smallz, smallz_in, small, small_two, small_in, nx, edge8,
    load, halo_sem, wt_s, wt_r, f_sem, b_sem, st_s, st_r, nx_s, nx_r,
    z1, z2, ga_s, ga_r, gb_s, gb_r, gc_s, gc_r, gd_s, gd_r,
    sa_s, sa_r, sb_s, sb_r, sz_s, sz_r, sc_s, sc_r, sd_s, sd_r, m1_s, m1_r, m2_s, m2_r,
):
    S, L, seqs, lines, tiles = dims
    T, D = xb.shape
    C = wg.shape[1]
    W = C + 2 * Q
    NC = L // Q
    own = spt.shape[0] // 2
    full = C * lines
    ps, pc, ph = lax.axis_index("seq"), lax.axis_index("sample"), lax.axis_index("head")
    other = 1 - pc
    group = 2 * seqs
    DC = D // C
    mine = ps * 2 + pc
    near1, near2 = outs, dnorm
    nb = part1

    def peer(i):
        p = lax.rem(mine + i, group)
        return {"seq": p // 2, "sample": lax.rem(p, 2)}

    def line(i):
        return lax.rem(ph + i, lines)

    def ring(i):
        return lax.rem(ps + i, seqs)

    moves = [pltpu.make_async_copy(x_in.at[pl.ds(s * L, L)], xb.at[pl.ds(s * L, L)], load.at[s]) for s in range(S)]
    moves += [
        pltpu.make_async_copy(wg_in, wg, load.at[S]),
        pltpu.make_async_copy(wv_in, wv, load.at[S + 1]),
        pltpu.make_async_copy(spt.at[pl.ds(0, own)], wst.at[at(ph, own)], load.at[S + 2]),
        pltpu.make_async_copy(
            spt.at[pl.ds(own, own)], wst.at[pl.ds(pl.multiple_of(Q + ph * own, own), own)], load.at[S + 3]
        ),
        pltpu.make_async_copy(cot_in, cot, load.at[S + 4]),
        pltpu.make_async_copy(wo_in, wo, load.at[S + 5]),
    ]
    for m in moves:
        m.start()
    barrier = pltpu.get_barrier_semaphore()
    for i in range(1, group):
        pl.semaphore_signal(barrier, inc=1, device_id=peer(i), device_id_type=MESH)
    for i in range(1, lines):
        pl.semaphore_signal(barrier, inc=1, device_id={"head": line(i)}, device_id_type=MESH)
    heads = stp.shape[0]
    tapb[...] = jnp.zeros_like(tapb)
    hp[...] = jnp.zeros_like(hp)
    for j in range(2):
        tapb[0:4, j * own : (j + 1) * own] = cs[:, j, :]
        tapb[4:5, j * own : (j + 1) * own] = csb[j : j + 1, :]
    taps[ph] = tapb[...]
    hp[0:1, 0:heads] = sbias[...]
    hp[1:2, 0:heads] = -jnp.exp(dlog_in[...])
    hp[2:3, 0:heads] = skip[...]
    wst[2 * Q :, :] = jnp.zeros((Q, D), bf16)
    wst[2 * Q : 2 * Q + heads, :] = stp[...]
    e[...] = lane_heads(C // 64, C)
    sk[...] = mm(hp[...], e[...], precision=HI)[2:3]
    pl.semaphore_wait(barrier, group - 1 + lines - 1)

    def halo(s):
        return remote(
            x_in.at[pl.ds(s * L + L - HALO, HALO)], xh.at[pl.ds(s * HALO, HALO)],
            halo_sem.at[0, s], halo_sem.at[1, s], seq=ps + 1,
        )

    @pl.when(ps < seqs - 1)
    def _():
        for s in range(S):
            halo(s).start()

    @pl.when(ps == 0)
    def _():
        xh[...] = jnp.zeros_like(xh)

    def weights(i, source):
        low = at(source, own)
        high = pl.ds(pl.multiple_of(Q + source * own, own), own)
        parts = [(spt.at[pl.ds(0, own)], wst.at[low]), (spt.at[pl.ds(own, own)], wst.at[high]), (tapb, taps.at[source])]
        return [
            remote(a, b, wt_s.at[j, i - 1], wt_r.at[j, i - 1], head=line(i))
            for j, (a, b) in enumerate(parts)
        ]

    for i in range(1, lines):
        for c in weights(i, ph):
            c.start()

    for s in range(S):
        moves[s].wait()

        def norm_rows(r):
            rows = at(s * (L // 16) + r, 16)
            v = xb[rows, :].astype(f32)
            i = lax.rsqrt(jnp.mean(v * v, axis=1, keepdims=True) + EPS)
            nb[rows, :] = (v * i * gain[...]).astype(bf16)
            inv[rows, :] = jnp.broadcast_to(i, (16, Q))

        loop(L // 16, norm_rows, 4)
        if s == 0:
            moves[S].wait()
            moves[S + 1].wait()
        seq_rows = slice(s * L, (s + 1) * L)
        gate[seq_rows, :] = mm(nb[seq_rows, :], wg[...]).astype(bf16)
        pad[s, HALO:, 0:C] = mm(nb[seq_rows, :], wv[...]).astype(bf16)
    moves[S + 2].wait()
    moves[S + 3].wait()
    for i in range(1, lines):
        for c in weights(i, line(lines - i)):
            c.wait_recv()
    cw[0:4, 0:C] = cv[...]
    cw[4:5, 0:C] = cvb[...]
    for h in range(lines):
        for j in range(2):
            cw[:, C + j * Q + h * own : C + j * Q + (h + 1) * own] = taps[h, :, j * own : (j + 1) * own]

    relays, relays2 = [], []
    for s in range(S):
        seq_rows = slice(s * L, (s + 1) * L)
        both = mm(nb[seq_rows, :], wst[...], NT)
        pad[s, HALO:, C:] = both[:, 0 : 2 * Q].astype(bf16)
        sg[seq_rows, :] = both[:, 2 * Q :]

        @pl.when(ps > 0)
        def _():
            halo(s).wait_recv()

        edge, unused = normalize(xh[s * HALO : (s + 1) * HALO, :].astype(f32), gain[...])
        pad[s, 0:HALO, 0:C] = mm(edge, wv[...]).astype(bf16)
        pad[s, 0:HALO, C:] = mm(edge, wst[0 : 2 * Q, :], NT).astype(bf16)

        def conv_rows(r):
            for lo in range(0, W, 256):
                lanes = slice(lo, lo + 256)
                w = pad[s, pl.ds(pl.multiple_of(r * TILE, TILE), TILE + HALO), lanes].astype(f32)
                v = cw[4:5, lanes] + cw[0:1, lanes] * w[13 : 13 + TILE]
                for k in range(1, 4):
                    v = v + cw[k : k + 1, lanes] * w[13 + k : 13 + k + TILE]
                g = jax.nn.sigmoid(v)
                rows = at(r + s * (L // TILE), TILE)
                act[rows, lanes] = (v * g).astype(bf16)
                slope[rows, lanes] = g * (1.0 + v * (1.0 - g))

        loop(L // TILE, conv_rows)

        def steps(k):
            c = s * NC + k
            z = sg[at(c, Q), :] + hp[0:1, :]
            d = jax.nn.softplus(z)
            dt[at(c, Q), :] = d
            sg[at(c, Q), :] = jax.nn.sigmoid(z)
            run = mm(triangle(lambda i, j: i >= j), d * hp[1:2, :], precision=HI)
            cum[at(c, Q), :] = run
            cum_t[:, at(c, Q)] = run.T[0:8]
            dt_t[:, at(c, Q)] = d.T[0:8]

        loop(NC, steps, 2)
        st[...] = jnp.zeros_like(st)
        tot[s] = jnp.zeros((8, Q), f32)

        def chunk(k):
            c = s * NC + k
            run = cum[at(c, Q), :]
            last = run[Q - 1 : Q, :]
            tail = mm(jnp.exp(last - run) * dt[at(c, Q), :], e[...], precision=HI)
            xt = act[at(c, Q), 0:C].astype(f32) * tail
            entry[c] = st[...]
            st[...] = st[...] * row_of(jnp.exp(last), e[...]) + mm2(act[at(c, Q), C : C + Q], xt, TN)
            tot[s] += jnp.broadcast_to(last, (8, Q))

        loop(NC, chunk)
        fin[s] = st[...].astype(bf16)
        relays.append(Relay(s, (fin, tot), (slots, slots_t), f_sem, seqs, 1))
        relays[s].start()

    def weights_of(h, here, causal):
        gap = cum[here, h : h + 1] - cum_t[h : h + 1, here]
        return jnp.exp(jnp.where(causal, gap, -1e30)) * dt_t[h : h + 1, here]

    def within(c):
        here = at(c, Q)
        scores = mm(act[here, C + Q :], act[here, C : C + Q], NT)
        causal = iota((Q, Q), 0) >= iota((Q, Q), 1)
        upper = iota((Q, Q), 1) >= 64
        for p in range(C // Q):
            xp = act[here, p * Q : (p + 1) * Q]
            y = jnp.zeros((Q, Q), f32)
            for o in range(2):
                m = (scores * weights_of(2 * p + o, here, causal)).astype(bf16)
                y = y + mm(m, jnp.where(upper == bool(o), xp, jnp.zeros_like(xp)))
            ys[here, p * Q : (p + 1) * Q] = y

    loop(T // Q, within)
    moves[S + 4].wait()
    moves[S + 5].wait()
    for s in range(S):
        seq_rows = slice(s * L, (s + 1) * L)
        dy[seq_rows, :] = mm(cot[seq_rows, :], wo[...], NT)

    def stat(s, i):
        part = pl.ds(s * L, L)
        return remote(
            stats_t.at[:, part], stats_in.at[i - 1, :, part], st_s.at[s, i - 1], st_r.at[s, i - 1], head=line(i)
        )

    stats_t[...] = jnp.zeros_like(stats_t)
    for s in range(S):
        relays[s].gather(chained, e)
        off[...] = jnp.zeros_like(off)

        def across(k):
            c = s * NC + k
            here = at(c, Q)
            si = entry[c] + row_of(jnp.exp(off[0:1, :]), e[...]) * chained[s]
            entry[c] = si
            run = cum[here, :]
            work[0] = mm(jnp.exp(run), e[...], precision=HI) * mm2(act[here, C + Q :], si)
            off[...] += jnp.broadcast_to(run[Q - 1 : Q, :], (8, Q))

            def tile(r):
                rows = at(c * (Q // TILE) + r, TILE)
                y = ys[rows, :] + work[0, at(r, TILE), :]
                ys[rows, :] = y
                m = y + sk[...] * act[rows, 0:C].astype(f32)
                g = gate[rows, :].astype(f32)
                gated = m * (g * jax.nn.sigmoid(g))
                a = gated * gated
                b = dy[rows, :] * gg[...] * gated
                stats[0, at(r, TILE), :] = sum(a[:, p * Q : (p + 1) * Q] for p in range(C // Q))
                stats[1, at(r, TILE), :] = sum(b[:, p * Q : (p + 1) * Q] for p in range(C // Q))

            loop(Q // TILE, tile, 2)
            for j in range(2):
                stats_t[j : j + 1, here] = jnp.sum(stats[j].T, axis=0, keepdims=True)

        loop(NC, across)
        for i in range(1, lines):
            stat(s, i).start()

    for r in relays:
        r.finish()
    sums[...] = jnp.zeros_like(sums)
    fold1 = Fold(part1, near1, far1, [z1.at[j] for j in range(4)], tiles)
    fold2 = Fold(part2, near2, far2, [z2.at[j] for j in range(4)], tiles)

    def spread_dy(c):
        return mm(jnp.exp(cum[at(c, Q), :]), e[...], precision=HI) * dy[at(c, Q), :]

    for s in range(S):
        for i in range(1, lines):
            stat(s, i).wait_recv()

        def gate_back(k):
            c = s * NC + k
            here = at(c, Q)
            t = stats_t[:, here]
            for i in range(1, lines):
                t = t + stats_in[i - 1, :, here]
            t = t.T
            rms = lax.rsqrt(t[:, 0:1] / full + EPS)
            tt[:, 0:1] = rms
            tt[:, 1:2] = rms * rms * rms * (t[:, 1:2] / full)

            def tile(r):
                rows = at(c * (Q // TILE) + r, TILE)
                near = at(r, TILE)
                rm, co = tt[near, 0:1], tt[near, 1:2]
                x = act[rows, 0:C].astype(f32)
                m = ys[rows, :] + sk[...] * x
                g = gate[rows, :].astype(f32)
                sig = jax.nn.sigmoid(g)
                ga = g * sig
                gated = m * ga
                scaled_rows = gated * rm
                gn[rows, :] = (scaled_rows * gg[...]).astype(bf16)
                d = dy[rows, :]
                dgd = rm * (d * gg[...]) - gated * co
                dmix = dgd * ga
                dg[rows, :] = (dgd * m * (sig * (1.0 + g * (1.0 - sig)))).astype(bf16)
                dy[rows, :] = dmix
                sums[0:8, :] += fold8(d * scaled_rows)
                sums[8:16, :] += fold8(dmix * x)

            loop(Q // TILE, tile, 2)
            if s > 0:

                @pl.when(lax.rem(k, 2) == 1)
                def _():
                    fold1.step(lax.div(k, 2))

        loop(NC, gate_back)
        part1[s * L : (s + 1) * L, :] = mm(gn[s * L : (s + 1) * L, :], wo[...]).astype(bf16)
        fold1.begin(s * (tiles // S), tiles // S)

    for s in range(S):
        st[...] = jnp.zeros_like(st)

        def back(k):
            c = s * NC + NC - 1 - k
            last = cum[pl.ds(pl.multiple_of(c * Q + Q - 8, 8), 8), :][7:8]
            later[c] = st[...]
            st[...] = st[...] * row_of(jnp.exp(last), e[...]) + mm2(act[at(c, Q), C + Q :], spread_dy(c), TN)

        loop(NC, back)
        fin[s] = st[...].astype(bf16)
        relays2.append(Relay(s, (fin, tot), (slots, slots_t), b_sem, seqs, -1))
        relays2[s].start()
        fold1.step(2 + s)

    HG = D // 2
    PR = HG // seqs

    def pair(k):
        return remote(gr.at[k, at(other, HG)], gr_in.at[k], ga_s.at[k], ga_r.at[k], sample=other)

    for i in range(D // C):
        gr[0, i * C : (i + 1) * C, :] = mm(gn[...], cot[:, i * C : (i + 1) * C], TN).astype(bf16)
    pair(0).start()
    fold1.step(4)

    def turn(i):
        rows = at(i, 256)
        nt[:, rows] = (xb[rows, :].astype(f32) * inv[rows, 0:1] * gain[...]).astype(bf16).T

    loop(T // 256, turn)
    fold1.step(5)

    def outer2(i):
        gr[1, at(i, 512), :] = mm(nt[at(i, 512), :], dg[...]).astype(bf16)

    loop(D // 512, outer2)
    pair(1).start()
    fold1.step(6)

    hsums[...] = jnp.zeros_like(hsums)
    acc[...] = jnp.zeros_like(acc)
    nsums[...] = jnp.zeros_like(nsums)
    LT = L // TILE

    def next_rows(s):
        return remote(edge8.at[s], nx.at[s], nx_s.at[s], nx_r.at[s], seq=ps - 1)

    @pl.when(ps == seqs - 1)
    def _():
        nx[...] = jnp.zeros_like(nx)

    def settle(k):
        pair(k).wait_recv()

        def tile(i):
            r = pl.ds(pl.multiple_of(pc * HG + i * TILE, TILE), TILE)
            v = gr[k, r, :].astype(f32) + gr_in[k, at(i, TILE), :].astype(f32)
            gr[k, r, :] = v.astype(bf16)

        loop(HG // TILE, tile)

    def piece(k, i):
        r = pl.ds(pl.multiple_of(pc * HG + ring(i) * PR, PR), PR)
        return remote(gr.at[k, r], gr_pieces.at[k, i - 1], gb_s.at[k, i - 1], gb_r.at[k, i - 1], seq=ring(i))

    for s in range(S):
        relays2[s].gather(chained, e)
        off[...] = jnp.zeros_like(off)

        def state_back(k):
            kk = NC - 1 - k
            c = s * NC + kk
            here = at(c, Q)
            run = cum[here, :]
            last = run[Q - 1 : Q, :]
            ds = later[c] + row_of(jnp.exp(off[0:1, :]), e[...]) * chained[s]
            off[...] += jnp.broadcast_to(last, (8, Q))
            upper = iota((Q, Q), 1) >= 64
            causal = iota((Q, Q), 0) >= iota((Q, Q), 1)
            b, r = act[here, C : C + Q], act[here, C + Q :]
            scores = mm(r, b, NT)
            dsc = jnp.zeros((Q, Q), f32)
            for p in range(C // Q):
                lanes = slice(p * Q, (p + 1) * Q)
                xp = act[here, lanes]
                dyp = dy[here, lanes].astype(bf16)
                dyl = (dy[here, lanes] - dyp.astype(f32)).astype(bf16)
                dx = jnp.zeros((Q, Q), f32)
                for o in range(2):
                    keep = upper == bool(o)
                    dym = jnp.where(keep, dyp, jnp.zeros_like(dyp))
                    dyn = jnp.where(keep, dyl, jnp.zeros_like(dyl))
                    w = weights_of(2 * p + o, here, causal)
                    dsc = dsc + (mm(dym, xp, NT) + mm(dyn, xp, NT)) * w
                    dx = dx + mm((scores * w).astype(bf16), dym, TN)
                work[0, :, lanes] = dx
            d = dt[here, :]
            work[2] = mm(jnp.exp(last - run) * d, e[...], precision=HI)
            work[1] = work[2] * mm2(b, ds)
            bf, rf = b.astype(f32), r.astype(f32)
            d_read = mm(dsc, bf, precision=HI) + mm(spread_dy(c), entry[c], NT, HI)
            d_in = mm(dsc, rf, TN, HI) + mm(act[here, 0:C].astype(f32) * work[2], ds, NT, HI)
            slope[here, C : C + Q] = d_in * slope[here, C : C + Q]
            slope[here, C + Q :] = d_read * slope[here, C + Q :]

            def tile(i):
                rows = at(c * (Q // TILE) + i, TILE)
                near = at(i, TILE)
                x = act[rows, 0:C].astype(f32)
                g = dy[rows, :]
                a, o = work[0, near, :], work[1, near, :]
                work[3, near, :] = g.astype(bf16).astype(f32) * ys[rows, :] - x * a
                work[4, near, :] = x * o
                both = a + o
                work[5, near, :] = x * both
                slope[rows, 0:C] = (both + sk[...] * g) * slope[rows, 0:C]

            loop(Q // TILE, tile, 2)
            ha = mm(work[3], e[...], NT, HI)
            hb = mm(work[4], e[...], NT, HI)
            hc = mm(work[5], e[...], NT, HI)
            crossing = mm(fold8(entry[c] * ds), e[...], NT, HI)
            crossing = jnp.sum(crossing, axis=0, keepdims=True) * jnp.exp(last)
            dlog = (
                mm(triangle(lambda i, j: i <= j), ha, precision=HI)
                + mm(triangle(lambda i, j: i > j), hb, precision=HI)
                + crossing
            )
            g = sg[here, :]
            ratio = jnp.where(d > 1e-30, g / jnp.maximum(d, 1e-30), 1.0)
            rate = hp[1:2, :]
            draw = rate * dlog * g + hc * ratio
            dcs[here, 2 * Q :] = draw.astype(bf16)
            hsums[0:8, :] += fold8(draw)
            hsums[8:16, :] += fold8(rate * dlog * d)
            fold1.step((7 if s == 0 else 13) + k)

        loop(NC, state_back)
        edge8[s] = slope[s * L : s * L + 8, :]

        @pl.when(ps > 0)
        def _():
            next_rows(s).start()

        settle(s)
        for i in range(1, seqs):
            piece(s, i).start()

        @pl.when(ps < seqs - 1)
        def _():
            next_rows(s).wait_recv()

        def conv_back(r, last):
            for lo in range(0, W, 256):
                lanes = slice(lo, lo + 256)
                if last:
                    w = jnp.concatenate([slope[(s + 1) * L - TILE : (s + 1) * L, lanes], nx[s, :, lanes]], axis=0)
                else:
                    w = slope[pl.ds(pl.multiple_of(s * L + r * TILE, TILE), TILE + 8), lanes]
                u = pad[s, pl.ds(pl.multiple_of(r * TILE, TILE), TILE + HALO), lanes].astype(f32)
                d = w[0:TILE]
                v = cw[3:4, lanes] * d
                for k in range(3):
                    v = v + cw[k : k + 1, lanes] * w[3 - k : 3 - k + TILE]
                rows = at(r + s * LT, TILE)
                if lo < C:
                    gate[rows, lanes] = v.astype(bf16)
                else:
                    dcs[rows, lo - C : lo - C + 256] = v.astype(bf16)
                for k in range(4):
                    acc[8 * k : 8 * k + 8, lanes] += fold8(d * u[13 + k : 13 + k + TILE])
                acc[32:40, lanes] += fold8(d)

        loop(LT - 1, lambda r: conv_back(r, False))
        conv_back(LT - 1, True)
        if s == 0:
            fold1.step(11)
        else:
            fold1.step(17)

        def into(k):
            i = s * (L // 256) + k
            rows = at(i, 256)
            v = mm(dg[rows, :], wg[...], NT) + mm(gate[rows, :], wv[...], NT) + mm(dcs[rows, :], wst[...])
            part2[rows, :] = v.astype(bf16)
            nsums[...] += fold8(v * xb[rows, :].astype(f32) * inv[rows, 0:1])
            per = tiles * 256 // T
            fold2.begin(i * per, per)

        loop(L // 256, into)
        if s == 0:
            fold1.step(12)
        else:
            fold2.step(0)

    def outer3(i):
        gr[2, at(i, 512), :] = mm(nt[at(i, 512), :], gate[...]).astype(bf16)

    loop(D // 512, outer3)
    pair(2).start()
    fold2.step(1)
    for k in range(D // Q):
        t = mm(nt[k * Q : (k + 1) * Q, :], dcs[...])
        for j in range(2):
            later[j * DC + k * Q // C, :, k * Q % C : k * Q % C + Q] = t[:, j * Q : (j + 1) * Q].T
        row = 8 + 8 * (k * Q // C)
        small[row : row + 8, k * Q % C : k * Q % C + Q] = t[:, 2 * Q :].T[0:8]

    SR = Q // seqs
    keep_state = at(pc, DC)

    def state_pair():
        return remote(later.at[at(other, DC)], sg_in, sa_s, sa_r, sample=other)

    state_pair().start()
    fold2.step(2)
    for k in range(5):
        row = jnp.sum(acc[8 * k : 8 * k + 8, :], axis=0, keepdims=True)
        small[k : k + 1, :] = row[:, 0:C]
        smallz[k : k + 1, 0 : 2 * Q] = row[:, C:]
        smallz[k : k + 1, 2 * Q :] = jnp.zeros((1, C - 2 * Q), f32)
    small[5:6, :] = jnp.sum(sums[0:8, :], axis=0, keepdims=True)
    small[6:7, :] = jnp.sum(sums[8:16, :], axis=0, keepdims=True)
    small[7:8, :] = jnp.zeros((1, C), f32)
    small[7:8, 0:Q] = jnp.sum(hsums[0:8, :], axis=0, keepdims=True)
    small[7:8, Q : 2 * Q] = jnp.sum(hsums[8:16, :], axis=0, keepdims=True)
    ngrad = jnp.sum(nsums[...], axis=0, keepdims=True)
    for j in range(D // C):
        smallz[5 + j : 6 + j, :] = ngrad[:, j * C : (j + 1) * C]
    smallz[7:8, :] = jnp.zeros((1, C), f32)

    def to_line(i):
        return remote(smallz, smallz_in.at[i - 1], m1_s.at[i - 1], m1_r.at[i - 1], head=line(i))

    for i in range(1, lines):
        to_line(i).start()
    settle(2)
    for i in range(1, seqs):
        piece(2, i).start()
    fold2.step(3)

    def gather_pieces(k):
        for i in range(1, seqs):
            piece(k, i).wait_recv()

        def tile(j):
            r = at(j, TILE)
            v = gr[k, pl.ds(pl.multiple_of(pc * HG + ps * PR + j * TILE, TILE), TILE), :].astype(f32)
            for i in range(1, seqs):
                v = v + gr_pieces[k, i - 1, r, :].astype(f32)
            gr_sum[k, r, :] = v.astype(bf16)
            grads[k, pl.ds(pl.multiple_of(pc * HG + ps * PR + j * TILE, TILE), TILE), :] = v.astype(bf16)

        loop(PR // TILE, tile)

    def spread(k, i):
        r = pl.ds(pl.multiple_of(pc * HG + ps * PR, PR), PR)
        return remote(gr_sum.at[k], grads.at[k, r], gc_s.at[k, i - 1], gc_r.at[k, i - 1], seq=ring(i))

    def hand(k, i):
        q = lax.rem(ps + seqs - i, seqs)
        r = pl.ds(pl.multiple_of(pc * HG + q * PR, PR), PR)
        src = gr_sum.at[k] if i == 0 else grads.at[k, r]
        return remote(src, grads.at[k, r], gd_s.at[k, i], gd_r.at[k, i], sample=other)

    def send_out(k):
        gather_pieces(k)
        for i in range(1, seqs):
            spread(k, i).start()
        hand(k, 0).start()

    def hand_on(k):
        for i in range(1, seqs):
            q = lax.rem(ps + seqs - i, seqs)
            r = pl.ds(pl.multiple_of(pc * HG + q * PR, PR), PR)
            remote(gr_sum.at[k], grads.at[k, r], gc_s.at[k, i - 1], gc_r.at[k, i - 1], seq=ring(i)).wait_recv()
            hand(k, i).start()

    send_out(0)
    fold2.step(4)
    send_out(1)
    fold2.step(5)
    state_pair().wait_recv()
    later[keep_state] = later[keep_state] + sg_in[...]

    def state_piece(i):
        return remote(later.at[keep_state, at(ring(i), SR)], sg_pieces.at[i - 1], sb_s.at[i - 1], sb_r.at[i - 1], seq=ring(i))

    for i in range(1, seqs):
        state_piece(i).start()
    fold2.step(6)
    total = smallz[...]
    for i in range(1, lines):
        to_line(i).wait_recv()
        total = total + smallz_in[i - 1]
    small[24:32, :] = total

    def to_core():
        return remote(small, small_two.at[0], m2_s.at[seqs - 1], m2_r.at[seqs - 1], sample=other)

    def to_peer(i):
        return remote(small_two.at[1], small_in.at[i - 1], m2_s.at[i - 1], m2_r.at[i - 1], seq=ring(i))

    to_core().start()
    fold2.step(7)
    to_core().wait_recv()
    small_two[1] = small[...] + small_two[0]
    for i in range(1, seqs):
        to_peer(i).start()
    hand_on(0)
    fold2.step(8)
    send_out(2)
    fold2.step(9)

    for i in range(1, seqs):
        state_piece(i).wait_recv()
    v = later[keep_state, at(ps, SR), :]
    for i in range(1, seqs):
        v = v + sg_pieces[i - 1]
    sg_sum[0] = v
    owner = (ps * SR) // own

    def to_owner(i):
        return remote(sg_sum.at[0], sg_line.at[i - 1], sz_s.at[i - 1], sz_r.at[i - 1], head=line(i))

    for i in range(1, lines):

        @pl.when(line(i) == owner)
        def _():
            to_owner(i).start()

    fold2.step(10)
    hand_on(1)
    fold2.step(11)
    fold2.step(12)
    span = max(own // SR, 1)

    def place_row(q, core):
        return pl.ds(pl.multiple_of(core * own + lax.rem(q * SR, own), SR), SR)

    def state_out_to(i):
        return remote(sg_sum.at[1], state_out.at[:, place_row(ps, pc)], sc_s.at[i - 1], sc_r.at[i - 1], seq=ring(i))

    def state_hand(j, src):
        q = ph * span + j
        return remote(src, state_out.at[:, place_row(q, pc)], sd_s.at[j], sd_r.at[j], sample=other)

    @pl.when(ph == owner)
    def _():
        t = sg_sum[0]
        for i in range(1, lines):
            to_owner(i).wait_recv()
            t = t + sg_line[i - 1]
        sg_sum[1] = t
        state_out[:, place_row(ps, pc), :] = t
        for i in range(1, seqs):
            state_out_to(i).start()

    fold2.step(13)
    hand_on(2)
    fold2.step(14)
    fold2.step(15)
    for j in range(span):
        q = ph * span + j

        @pl.when(q == ps)
        def _():
            state_hand(j, sg_sum.at[1]).start()

        for i in range(1, seqs):

            @pl.when(ring(seqs - i) == q)
            def _():
                remote(
                    sg_sum.at[1], state_out.at[:, place_row(q, pc)], sc_s.at[i - 1], sc_r.at[i - 1], seq=ring(i)
                ).wait_recv()
                state_hand(j, state_out.at[:, place_row(q, pc)]).start()

    fold2.step(16)
    total = small_two[1]
    for i in range(1, seqs):
        to_peer(i).wait_recv()
        total = total + small_in[i - 1]
    small_out[...] = total
    fold2.step(17)

    fold1.end()
    fold2.end()
    for r in relays2:
        r.finish()
    for i in range(1, lines):
        for c in weights(i, ph):
            c.wait_send()
        for s in range(S):
            stat(s, i).wait_send()
        to_line(i).wait_send()

        @pl.when(line(i) == owner)
        def _():
            to_owner(i).wait_send()

    @pl.when(ps < seqs - 1)
    def _():
        for s in range(S):
            halo(s).wait_send()

    @pl.when(ps > 0)
    def _():
        for s in range(S):
            next_rows(s).wait_send()

    for k in range(3):
        pair(k).wait_send()
        for i in range(1, seqs):
            piece(k, i).wait_send()
            spread(k, i).wait_send()
        for i in range(seqs):
            q = lax.rem(ps + seqs - i, seqs)
            r = pl.ds(pl.multiple_of(other * HG + q * PR, PR), PR)
            remote(gr_sum.at[k], grads.at[k, r], gd_s.at[k, i], gd_r.at[k, i], sample=other).wait()
    state_pair().wait_send()
    for i in range(1, seqs):
        state_piece(i).wait_send()

        @pl.when(ph == owner)
        def _():
            state_out_to(i).wait_send()

    for j in range(span):
        q = ph * span + j
        remote(sg_sum.at[1], state_out.at[:, place_row(q, other)], sd_s.at[j], sd_r.at[j], sample=other).wait()
    to_core().wait_send()
    for i in range(1, seqs):
        to_peer(i).wait_send()


def finish(
    lines, x, cot, gain, dn, outs, g_out, g_gate, g_value, state, small,
    block_out, input_grad, gate_grad, value_grad, out_grad,
    state_grad, norm_grad, step_grad, cv, cs, cvb, csb, sbias, dlog, skip, gated_gain,
):
    rows, width = x.shape
    for j in range(rows // 16):
        r = slice(j * 16, (j + 1) * 16)
        v = x[r, :].astype(f32)
        block_out[r, :] = (v + outs[r, :].astype(f32)).astype(bf16)
        s = dn[r, :].astype(f32) * gain[...]
        i1 = lax.rsqrt(jnp.mean(v * v, axis=1, keepdims=True) + EPS)
        m = jnp.mean(s * v, axis=1, keepdims=True)
        input_grad[r, :] = cot[r, :].astype(f32) + i1 * s - v * (i1 * i1 * i1 * m)
    half = g_gate.shape[1]
    for j in range(width // half):
        out_grad[:, j * half : (j + 1) * half] = g_out[j].astype(f32)
    gate_grad[...] = g_gate[...].astype(f32)
    value_grad[...] = g_value[...].astype(f32)

    @pl.when(pl.program_id(0) == 0)
    def _():
        heads, own = sbias.shape[1], csb.shape[1]
        for j in range(width // half):
            lanes = slice(j * half, (j + 1) * half)
            state_grad[:, lanes] = state[j]
            norm_grad[:, lanes] = small[29 + j : 30 + j, :]
            step_grad[:, lanes] = small[8 + 8 * j : 16 + 8 * j, :]
        cv[...] = small[0:4, :]
        cvb[...] = small[4:5, :]
        gated_gain[...] = small[5:6, :]
        e = lane_heads(half // 64, half)
        skip[...] = mm(jnp.broadcast_to(small[6:7, :], (8, half)), e, NT, HI)[0:1, 0:heads]
        sbias[...] = small[7:8, 0:heads]
        dlog[...] = small[7:8, Q : Q + heads]
        for h in range(lines):

            @pl.when(lax.axis_index("head") == h)
            def _():
                for j in range(2):
                    lanes = slice(j * Q + h * own, j * Q + (h + 1) * own)
                    cs[:, j, :] = small[24:28, lanes]
                    csb[j : j + 1, :] = small[28:29, lanes]


def per_device(
    block_in, out_cotangent, norm_gain, gate_proj, value_proj, state_proj, step_proj,
    conv_value, conv_state, conv_value_bias, conv_state_bias, step_bias, decay_log,
    skip_gain, gated_gain, out_proj,
):
    S, L, D = block_in.shape
    T = S * L
    heads = step_proj.shape[1]
    C = gate_proj.shape[1]
    own = state_proj.shape[2]
    W = C + 2 * Q
    NCH = T // Q
    seqs, lines = lax.axis_size("seq"), lax.axis_size("head")
    tiles = 16
    H = D // 2
    PR = H // seqs
    SR = Q // seqs
    x = block_in.reshape(T, D)
    cot = out_cotangent.reshape(T, D)
    spt = state_proj.transpose(0, 2, 1).reshape(2 * own, D)
    gain = norm_gain[None]
    vm = pl.BlockSpec(memory_space=pltpu.VMEM)
    hbm = pl.BlockSpec(memory_space=pl.ANY)
    dma = pltpu.SemaphoreType.DMA
    n1, l1 = seqs - 1, lines - 1
    V = pltpu.VMEM
    scratch = [
        V((T, D), bf16), V((T, D), bf16), V((D, C), bf16), V((D, C), bf16), V((3 * Q, D), bf16),
        V((C, D), bf16), V((8, Q), f32), V((lines, 8, Q), f32), V((8, W), f32), V((8, Q), f32), V((1, C), f32),
        V((S * HALO, D), bf16),
        V((D, T), bf16), V((T, Q), f32), V((T, C), bf16), V((S, HALO + L, W), bf16), V((T, W), f32),
        V((T, W), bf16), V((T, Q), f32), V((T, Q), f32), V((T, Q), f32), V((8, T), f32), V((8, T), f32),
        V((NCH, Q, C), f32), V((T, C), f32), V((T, C), f32), V((T, C), bf16), V((T, C), bf16),
        V((NCH, Q, C), f32),
        V((T, 3 * Q), bf16), V((Q, C), f32), V((Q, C), f32), V((6, Q, C), f32),
        V((8, Q), f32), V((Q, Q), f32), V((2, Q, Q), f32), V((8, T), f32), V((l1, 8, T), f32),
        V((S, Q, C), bf16), V((S, 8, Q), f32), V((seqs, S, Q, C), bf16), V((seqs, S, 8, Q), f32),
        V((S, Q, C), f32),
        V((T, D), bf16), V((T, D), bf16), V((T, D), bf16), V((T, D), bf16),
        V((3, D, C), bf16), V((3, H, C), bf16), V((3, n1, PR, C), bf16), V((3, PR, C), bf16),
        V((D // C, Q, C), f32), V((n1, D // C, SR, C), f32), V((l1, D // C, SR, C), f32),
        V((2, D // C, SR, C), f32),
        V((40, W), f32), V((16, Q), f32), V((16, C), f32), V((8, D), f32), V((8, C), f32),
        V((l1, 8, C), f32), V((32, C), f32), V((2, 32, C), f32), V((n1, 32, C), f32), V((S, 8, W), f32), V((S, 8, W), f32),
        dma((S + 6,)), dma((2, S)), dma((3, l1)), dma((3, l1)), dma((2, 2, S, n1)), dma((2, 2, S, n1)),
        dma((S, l1)), dma((S, l1)), dma((S,)), dma((S,)),
        dma((4, tiles)), dma((4, tiles)), dma((3,)), dma((3,)), dma((3, n1)), dma((3, n1)),
        dma((3, n1)), dma((3, n1)), dma((3, seqs)), dma((3, seqs)),
        dma, dma, dma((n1,)), dma((n1,)), dma((l1,)), dma((l1,)), dma((n1,)), dma((n1,)),
        dma((max(own // SR, 1),)), dma((max(own // SR, 1),)), dma((l1,)), dma((l1,)), dma((seqs,)), dma((seqs,)),
    ]
    outs, dnorm, grads, state_out, small = pl.pallas_call(
        functools.partial(block, (S, L, seqs, lines, tiles)),
        out_shape=[
            jax.ShapeDtypeStruct((T, D), bf16), jax.ShapeDtypeStruct((T, D), bf16),
            jax.ShapeDtypeStruct((3, D, C), bf16), jax.ShapeDtypeStruct((D // C, 2 * own, C), f32),
            jax.ShapeDtypeStruct((32, C), f32),
        ],
        in_specs=[hbm, hbm, vm, hbm, hbm, hbm, vm, hbm] + [vm] * 8,
        out_specs=[vm] * 5,
        scratch_shapes=scratch,
        name="block",
        compiler_params=pltpu.CompilerParams(
            collective_id=0, has_side_effects=True, vmem_limit_bytes=67043328
        ),
    )(
        x, cot, gain, gate_proj, value_proj, spt, step_proj.T, out_proj, conv_state, conv_state_bias,
        conv_value, conv_value_bias[None], step_bias[None], decay_log[None], skip_gain[None], gated_gain[None],
    )
    steps = 8

    def whole(*shape):
        return pl.BlockSpec(shape, lambda i: (0,) * len(shape))

    by_rows = pl.BlockSpec((T // steps, D), lambda i: (i, 0))
    by_grad = pl.BlockSpec((D // steps, C), lambda i: (i, 0))
    shape = jax.ShapeDtypeStruct
    (block_out, input_grad, gate_grad, value_grad, out_grad, state_grad, norm_grad, step_grad, cv, cs, cvb, csb,
     sbias, dlog, skip, gated) = pl.pallas_call(
        functools.partial(finish, lines),
        grid=(steps,),
        out_shape=[
            shape((T, D), bf16), shape((T, D), f32), shape((D, C), f32), shape((D, C), f32), shape((C, D), f32),
            shape((2 * own, D), f32), shape((1, D), f32), shape((heads, D), f32), shape((4, C), f32),
            shape((4, 2, own), f32), shape((1, C), f32), shape((2, own), f32), shape((1, heads), f32),
            shape((1, heads), f32), shape((1, heads), f32), shape((1, C), f32),
        ],
        in_specs=[
            by_rows, by_rows, whole(1, D), by_rows, by_rows,
            pl.BlockSpec((None, D // C, C // steps, C), lambda i: (0, 0, i, 0)),
            pl.BlockSpec((None, D // steps, C), lambda i: (1, i, 0)),
            pl.BlockSpec((None, D // steps, C), lambda i: (2, i, 0)),
            whole(D // C, 2 * own, C), whole(32, C),
        ],
        out_specs=[
            by_rows, by_rows, by_grad, by_grad, pl.BlockSpec((C // steps, D), lambda i: (i, 0)),
            whole(2 * own, D), whole(1, D), whole(heads, D), whole(4, C), whole(4, 2, own), whole(1, C),
            whole(2, own), whole(1, heads), whole(1, heads), whole(1, heads), whole(1, C),
        ],
        name="finish",
        compiler_params=pltpu.CompilerParams(vmem_limit_bytes=60 * 2**20),
    )(x, cot, gain, dnorm, outs, grads.reshape(3, D // C, C, C), grads, grads, state_out, small)
    return (
        block_out.reshape(S, L, D), input_grad.reshape(S, L, D), norm_grad[0], gate_grad, value_grad,
        state_grad.reshape(2, own, D).transpose(0, 2, 1), step_grad.T, cv, cs, cvb[0], csb, sbias[0], dlog[0],
        skip[0], gated[0], out_grad,
    )


def solution(mesh):
    tokens = P("sample", "seq", None)
    params = (
        P(), P(None, "head"), P(None, "head"), P(None, None, "head"), P(None, "head"),
        P(None, "head"), P(None, None, "head"), P("head"), P(None, "head"), P("head"),
        P("head"), P("head"), P("head"), P("head", None),
    )
    return jax.shard_map(
        per_device,
        mesh=mesh,
        in_specs=(tokens, tokens) + params,
        out_specs=(tokens, tokens) + params,
        check_vma=False,
    )
```

```python
import functools

import jax
import jax.numpy as jnp
from jax import lax
from jax.experimental import pallas as pl
from jax.experimental.pallas import tpu as pltpu
from jax.sharding import PartitionSpec as P

f32, bf16 = jnp.float32, jnp.bfloat16
HI = lax.Precision.HIGHEST
MESH = pl.DeviceIdType.MESH
Q = 128
TILE = 32
HALO = 16
EPS = 1e-05
NN, NT, TN = ((1,), (0,)), ((1,), (1,)), ((0,), (0,))


def mm(a, b, dims=NN, precision=None):
    return lax.dot_general(
        a, b, (dims, ((), ())), preferred_element_type=f32, precision=precision
    )


def halves(v):
    high = v.astype(bf16)
    return high, (v - high.astype(f32)).astype(bf16)


def mm2(a, b, dims=NN):
    if a.dtype == bf16:
        high, low = halves(b)
        return mm(a, high, dims) + mm(a, low, dims)
    high, low = halves(a)
    return mm(high, b, dims) + mm(low, b, dims)


def mm3(a, b, dims=NN):
    ah, al = halves(a)
    bh, bl = halves(b)
    return mm(ah, bh, dims) + (mm(ah, bl, dims) + mm(al, bh, dims))


def at(i, n):
    return pl.ds(pl.multiple_of(i * n, n), n)


def loop(count, body, each=1):
    def step(i, carry):
        for j in range(each):
            body(i * each + j)
        return carry

    lax.fori_loop(0, count // each, step, 0)


def iota(shape, axis):
    return lax.broadcasted_iota(jnp.int32, shape, axis)


def lane_heads(heads, width):
    shift = (width // heads).bit_length() - 1
    return ((iota((Q, width), 1) >> shift) == iota((Q, width), 0)).astype(f32).astype(bf16)


def triangle(keep):
    return jnp.where(keep(iota((Q, Q), 0), iota((Q, Q), 1)), 1.0, 0.0)


def fold8(v):
    return jnp.sum(v.reshape(v.shape[0] // 8, 8, v.shape[1]), axis=0)


def row_of(v, e):
    return mm2(jnp.broadcast_to(v, (8, Q)), e)[0:1]


def sigmoid(v):
    return 0.5 * jnp.tanh(0.5 * v) + 0.5


def normalize(v, gain):
    inv = lax.rsqrt(jnp.mean(v * v, axis=1, keepdims=True) + EPS)
    return (v * inv * gain).astype(bf16), inv


def remote(src, dst, send, recv, **place):
    return pltpu.make_async_remote_copy(
        src_ref=src, dst_ref=dst, send_sem=send, recv_sem=recv, device_id=place, device_id_type=MESH
    )


class Fold:
    def __init__(self, part, near, far, result, sems, tiles):
        self.part, self.near, self.far, self.result, self.tiles = part, near, far, result, tiles
        (self.b, self.d), (self.a, self.c, self.e) = sems
        self.rows = part.shape[0] // tiles
        place = lax.axis_index("head")
        self.inner = (place == 1) | (place == 2)
        self.beside = jnp.where(place < 2, 1 - place, 5 - place)
        self.across = 3 - place

    def outward(self, i, src):
        r = at(i, self.rows)
        return remote(src.at[r], self.near.at[r], self.a, self.b.at[i], head=self.beside)

    def middle(self, i):
        r = at(i, self.rows)
        return remote(self.part.at[r], self.far.at[r], self.c, self.d.at[i], head=self.across)

    def store(self, i):
        r = at(i, self.rows)
        return pltpu.make_async_copy(self.near.at[r], self.result.at[r], self.e)

    def take(self, i):
        @pl.when(jnp.logical_not(self.inner))
        def _():
            self.outward(i, self.near).wait_recv()
            self.store(i).start()

    def begin(self, first, count):
        @pl.when(jnp.logical_not(self.inner))
        def _():
            loop(count, lambda i: self.outward(first + i, self.part).start())

    def add(self, dst, u, v, i):
        def tile(j):
            r = at(i * (self.rows // TILE) + j, TILE)
            dst[r, :] = (u[r, :].astype(f32) + v[r, :].astype(f32)).astype(bf16)

        loop(self.rows // TILE, tile)

    def one(self, i):
        @pl.when(self.inner)
        def _():
            self.outward(i, self.near).wait_recv()
            self.add(self.part, self.part, self.near, i)
            self.middle(i).start()

    def two(self, i):
        @pl.when(self.inner)
        def _():
            self.middle(i).wait_recv()
            self.add(self.near, self.part, self.far, i)
            self.outward(i, self.near).start()
            self.store(i).start()

    def step(self, j):
        for ago, move in ((0, self.one), (2, self.two), (4, self.take)):
            if isinstance(j, int):
                if 0 <= 2 * (j - ago) < self.tiles:
                    loop(2, lambda q: move(2 * (j - ago) + q))
            else:

                @pl.when((j >= ago) & (2 * j < self.tiles + 2 * ago))
                def _():
                    loop(2, lambda q: move(2 * (j - ago) + q))

    def last(self, j, parts):
        o, t, k = 2 * j + 2, 2 * j - 2, 2 * j - 6
        moves = []
        while k < self.tiles:
            if o < self.tiles:
                moves.append((self.one, o))
                o += 1
            for unused in range(2):
                if t < self.tiles and (t < o - 2 or o == self.tiles):
                    moves.append((self.two, t))
                    t += 1
            for unused in range(2):
                if k < self.tiles and (k < t - 3 or t == self.tiles):
                    moves.append((self.take, k))
                    k += 1
        size = -(-len(moves) // parts)
        return [moves[i : i + size] for i in range(0, len(moves), size)]

    def end(self):
        pltpu.make_async_copy(self.near, self.result, self.e).wait()
        remote(self.part, self.near, self.a, self.b.at[0], head=self.beside).wait_send()

        @pl.when(self.inner)
        def _():
            remote(self.part, self.far, self.c, self.d.at[0], head=self.across).wait_send()


def fold_sems(tiles, streams):
    return [tiles.at[j] for j in range(2)], [streams.at[j] for j in range(3)]


class Relay:
    def __init__(self, seq, blocks, slots, sems, count, way):
        self.seq, self.blocks, self.slots, self.sems = seq, blocks, slots, sems
        self.count, self.way = count, way
        self.place = lax.axis_index("seq")

    def copies(self, d, source):
        to = self.place + self.way * d
        return [
            remote(
                b.at[self.seq], s.at[source, self.seq], self.sems.at[0, j, self.seq, d - 1],
                self.sems.at[1, j, self.seq, d - 1], seq=to,
            )
            for j, (b, s) in enumerate(zip(self.blocks, self.slots))
        ]

    def reaches(self, d):
        return self.place + d < self.count if self.way > 0 else self.place >= d

    def hears(self, d):
        return self.place >= d if self.way > 0 else self.place + d < self.count

    def start(self):
        for d in range(1, self.count):

            @pl.when(self.reaches(d))
            def _():
                for c in self.copies(d, self.place):
                    c.start()

    def gather(self, state, e):
        q = self.seq
        state[q] = jnp.zeros(state.shape[1:], f32)
        for d in range(self.count - 1, 0, -1):

            @pl.when(self.hears(d))
            def _():
                source = self.place - self.way * d
                for c in self.copies(d, source):
                    c.wait_recv()
                decay = mm2(jnp.exp(self.slots[1][source, q]), e[...])[0:1]
                state[q] = state[q] * decay + self.slots[0][source, q].astype(f32)

    def finish(self):
        for d in range(1, self.count):

            @pl.when(self.reaches(d))
            def _():
                for c in self.copies(d, self.place):
                    c.wait_send()


def block(
    dims,
    x_in, cot_in, gain, wg_in, wv_in, spt, stp, wo_in, cs, csb, cv, cvb, sbias, dlog_in, skip, gg,
    outs, dnorm, grads_out, state_out, small_out,
    xb, cot, wg, wv, wst, wo, tapb, taps, cw, hp, sk, xh,
    nt, inv, gate, pad, slope, act, dt, sg, cum, cum_t, dt_t, entry, ys, dy, gn, dg, later,
    dcs, e, st, work, off, tt, stats, stats_t, stats_in,
    fin, tot, slots, slots_t, chained,
    part1, near1, far1, part2, near2, far2, grads,
    gr, gr_in, gr_pieces, gr_sum, sg_in, sg_pieces, sg_line, sg_wire, sg_sum,
    acc, hsums, sums, nsums, smallz, smallz_in, small, small_two, small_in, nx, edge8,
    load, halo_sem, wt_s, wt_r, f_sem, b_sem, st_s, st_r, nx_s, nx_r,
    z1, y1, z2, y2, ga_s, ga_r, gb_s, gb_r, gc_s, gc_r, gd_s, gd_r,
    out_sem, sa_s, sa_r, sb_s, sb_r, sz_s, sz_r, sc_s, sc_r, sd_s, sd_r, m1_s, m1_r, m2_s, m2_r,
):
    S, L, seqs, lines, tiles = dims
    T, D = xb.shape
    C = wg.shape[1]
    W = C + 2 * Q
    NC = L // Q
    own = spt.shape[0] // 2
    full = C * lines
    ps, pc, ph = lax.axis_index("seq"), lax.axis_index("sample"), lax.axis_index("head")
    other = 1 - pc
    group = 2 * seqs
    DC = D // C
    mine = ps * 2 + pc
    nb = part1

    def peer(i):
        p = lax.rem(mine + i, group)
        return {"seq": p // 2, "sample": lax.rem(p, 2)}

    def line(i):
        return lax.rem(ph + i, lines)

    def ring(i):
        return lax.rem(ps + i, seqs)

    moves = [pltpu.make_async_copy(x_in.at[pl.ds(s * L, L)], xb.at[pl.ds(s * L, L)], load.at[s]) for s in range(S)]
    moves += [
        pltpu.make_async_copy(wg_in, wg, load.at[S]),
        pltpu.make_async_copy(wv_in, wv, load.at[S + 1]),
        pltpu.make_async_copy(
            spt.at[at(pc, own)], wst.at[pl.ds(pl.multiple_of(pc * Q + ph * own, own), own)], load.at[S + 2]
        ),
        pltpu.make_async_copy(wo_in, wo, load.at[S + 3]),
        pltpu.make_async_copy(cot_in, cot, load.at[S + 4]),
    ]
    for m in moves:
        m.start()
    barrier = pltpu.get_barrier_semaphore()
    for i in range(1, group):
        pl.semaphore_signal(barrier, inc=1, device_id=peer(i), device_id_type=MESH)
    for i in range(1, lines):
        pl.semaphore_signal(barrier, inc=1, device_id={"head": line(i)}, device_id_type=MESH)
    heads = stp.shape[0]
    tapb[...] = jnp.zeros_like(tapb)
    hp[...] = jnp.zeros_like(hp)
    for j in range(2):
        tapb[0:4, j * own : (j + 1) * own] = cs[:, j, :]
        tapb[4:5, j * own : (j + 1) * own] = csb[j : j + 1, :]
    taps[ph] = tapb[...]
    hp[0:1, 0:heads] = sbias[...]
    hp[1:2, 0:heads] = -jnp.exp(dlog_in[...])
    hp[2:3, 0:heads] = skip[...]
    wst[2 * Q :, :] = jnp.zeros((Q, D), bf16)
    wst[2 * Q : 2 * Q + heads, :] = stp[...]
    e[...] = lane_heads(C // 64, C)
    sk[...] = mm(hp[...], e[...].astype(f32), precision=HI)[2:3]

    def norm(s):
        moves[s].wait()

        def norm_rows(r):
            rows = at(s * (L // 16) + r, 16)
            v = xb[rows, :].astype(f32)
            i = lax.rsqrt(jnp.mean(v * v, axis=1, keepdims=True) + EPS)
            nb[rows, :] = (v * i * gain[...]).astype(bf16)
            inv[rows, :] = jnp.broadcast_to(i, (16, Q))

        loop(L // 16, norm_rows, 4)

    norm(0)
    pl.semaphore_wait(barrier, group - 1 + lines - 1)

    def halo(s):
        return remote(
            x_in.at[pl.ds(s * L + L - HALO, HALO)], xh.at[pl.ds(s * HALO, HALO)],
            halo_sem.at[0, s], halo_sem.at[1, s], seq=ps + 1,
        )

    @pl.when(ps < seqs - 1)
    def _():
        for s in range(S):
            halo(s).start()

    @pl.when(ps == 0)
    def _():
        xh[...] = jnp.zeros_like(xh)

    def weights(i, source):
        r = pl.ds(pl.multiple_of(pc * Q + source * own, own), own)
        parts = [(spt.at[at(pc, own)], wst.at[r]), (tapb, taps.at[source])]
        return [
            remote(a, b, wt_s.at[j, i - 1], wt_r.at[j, i - 1], head=line(i))
            for j, (a, b) in enumerate(parts)
        ]

    for i in range(1, lines):
        for c in weights(i, ph):
            c.start()

    for s in range(S):
        if s > 0:
            norm(s)
        else:
            moves[S].wait()
            moves[S + 1].wait()
        seq_rows = slice(s * L, (s + 1) * L)
        gate[seq_rows, :] = mm(nb[seq_rows, :], wg[...]).astype(bf16)
        pad[s, HALO:, 0:C] = mm(nb[seq_rows, :], wv[...]).astype(bf16)

    def conv(s, first, end):
        def conv_rows(r):
            for lo in range(first, end, 256):
                lanes = slice(lo, lo + 256)
                w = pad[s, pl.ds(pl.multiple_of(r * TILE, TILE), TILE + HALO), lanes].astype(f32)
                v = cw[4:5, lanes] + cw[0:1, lanes] * w[13 : 13 + TILE]
                for k in range(1, 4):
                    v = v + cw[k : k + 1, lanes] * w[13 + k : 13 + k + TILE]
                g = sigmoid(v)
                rows = at(r + s * (L // TILE), TILE)
                act[rows, lanes] = (v * g).astype(bf16)
                slope[rows, lanes] = g * (1.0 + v * (1.0 - g))

        loop(L // TILE, conv_rows, 2)

    cw[0:4, 0:C] = cv[...]
    cw[4:5, 0:C] = cvb[...]
    edges = []
    for s in range(S):

        @pl.when(ps > 0)
        def _():
            halo(s).wait_recv()

        edges.append(normalize(xh[s * HALO : (s + 1) * HALO, :].astype(f32), gain[...])[0])
        pad[s, 0:HALO, 0:C] = mm(edges[s], wv[...]).astype(bf16)
        conv(s, 0, C)
    moves[S + 3].wait()
    moves[S + 4].wait()
    for s in range(S):
        seq_rows = slice(s * L, (s + 1) * L)
        dy[seq_rows, :] = mm(cot[seq_rows, :], wo[...], NT)

    def share():
        r = at(pc, Q)
        return remote(wst.at[r], wst.at[r], wt_s.at[0, lines - 1], wt_r.at[0, lines - 1], sample=other)

    moves[S + 2].wait()
    for i in range(1, lines):
        for c in weights(i, line(lines - i)):
            c.wait_recv()
    share().start()
    for h in range(lines):
        for j in range(2):
            cw[:, C + j * Q + h * own : C + j * Q + (h + 1) * own] = taps[h, :, j * own : (j + 1) * own]
    r = at(other, Q)
    remote(wst.at[r], wst.at[r], wt_s.at[0, lines - 1], wt_r.at[0, lines - 1], sample=other).wait_recv()

    relays, relays2 = [], []
    for s in range(S):
        seq_rows = slice(s * L, (s + 1) * L)
        both = mm(nb[seq_rows, :], wst[...], NT)
        pad[s, HALO:, C:] = both[:, 0 : 2 * Q].astype(bf16)
        sg[seq_rows, :] = both[:, 2 * Q :]
        pad[s, 0:HALO, C:] = mm(edges[s], wst[0 : 2 * Q, :], NT).astype(bf16)
        conv(s, C, W)

        def steps(k):
            c = s * NC + k
            z = sg[at(c, Q), :] + hp[0:1, :]
            d = jax.nn.softplus(z)
            dt[at(c, Q), :] = d
            sg[at(c, Q), :] = jax.nn.sigmoid(z)
            run = mm(triangle(lambda i, j: i >= j), d * hp[1:2, :], precision=HI)
            cum[at(c, Q), :] = run
            cum_t[:, at(c, Q)] = run.T[0:8]
            dt_t[:, at(c, Q)] = d.T[0:8]

        loop(NC, steps, 2)
        st[...] = jnp.zeros_like(st)
        tot[s] = jnp.zeros((8, Q), f32)

        def chunk(k):
            c = s * NC + k
            run = cum[at(c, Q), :]
            last = run[Q - 1 : Q, :]
            tail = mm2(jnp.exp(last - run) * dt[at(c, Q), :], e[...])
            xt = act[at(c, Q), 0:C].astype(f32) * tail
            entry[c] = st[...]
            st[...] = st[...] * row_of(jnp.exp(last), e[...]) + mm2(act[at(c, Q), C : C + Q], xt, TN)
            tot[s] += jnp.broadcast_to(last, (8, Q))

        loop(NC, chunk, NC)
        fin[s] = st[...].astype(bf16)
        relays.append(Relay(s, (fin, tot), (slots, slots_t), f_sem, seqs, 1))
        relays[s].start()

    def weights_of(h, here, causal):
        gap = cum[here, h : h + 1] - cum_t[h : h + 1, here]
        return jnp.exp(jnp.where(causal, gap, -1e30)) * dt_t[h : h + 1, here]

    def within(c):
        here = at(c, Q)
        scores = mm(act[here, C + Q :], act[here, C : C + Q], NT)
        causal = iota((Q, Q), 0) >= iota((Q, Q), 1)
        upper = iota((Q, Q), 1) >= 64
        for p in range(C // Q):
            xp = act[here, p * Q : (p + 1) * Q]
            y = jnp.zeros((Q, Q), f32)
            for o in range(2):
                m = (scores * weights_of(2 * p + o, here, causal)).astype(bf16)
                y = y + mm(m, jnp.where(upper == bool(o), xp, jnp.zeros_like(xp)))
            ys[here, p * Q : (p + 1) * Q] = y

    loop(NC, within)

    def stat(s, i):
        part = pl.ds(s * L, L)
        return remote(
            stats_t.at[:, part], stats_in.at[i - 1, :, part], st_s.at[s, i - 1], st_r.at[s, i - 1], head=line(i)
        )

    stats_t[...] = jnp.zeros_like(stats_t)

    def cross(s):
        relays[s].gather(chained, e)
        off[...] = jnp.zeros_like(off)

        def across(k):
            c = s * NC + k
            here = at(c, Q)
            si = entry[c] + row_of(jnp.exp(off[0:1, :]), e[...]) * chained[s]
            entry[c] = si
            run = cum[here, :]
            work[0] = mm2(jnp.exp(run), e[...]) * mm2(act[here, C + Q :], si)
            off[...] += jnp.broadcast_to(run[Q - 1 : Q, :], (8, Q))

            def tile(r):
                rows = at(c * (Q // TILE) + r, TILE)
                y = ys[rows, :] + work[0, at(r, TILE), :]
                ys[rows, :] = y
                m = y + sk[...] * act[rows, 0:C].astype(f32)
                g = gate[rows, :].astype(f32)
                gated = m * (g * sigmoid(g))
                a = gated * gated
                b = dy[rows, :] * gg[...] * gated
                stats[0, at(r, TILE), :] = sum(a[:, p * Q : (p + 1) * Q] for p in range(C // Q))
                stats[1, at(r, TILE), :] = sum(b[:, p * Q : (p + 1) * Q] for p in range(C // Q))

            loop(Q // TILE, tile, 4)
            for j in range(2):
                stats_t[j : j + 1, here] = jnp.sum(stats[j].T, axis=0, keepdims=True)

        loop(NC, across)
        for i in range(1, lines):
            stat(s, i).start()

    cross(0)
    loop(NC, lambda k: within(NC + k))
    sums[...] = jnp.zeros_like(sums)
    fold1 = Fold(part1, near1, far1, outs, fold_sems(z1, y1), tiles)
    fold2 = Fold(part2, near2, far2, dnorm, fold_sems(z2, y2), tiles)

    def spread_dy(c):
        return mm2(jnp.exp(cum[at(c, Q), :]), e[...]) * dy[at(c, Q), :]

    def gating(s):
        for i in range(1, lines):
            stat(s, i).wait_recv()

        def gate_back(k):
            c = s * NC + k
            here = at(c, Q)
            t = stats_t[:, here]
            for i in range(1, lines):
                t = t + stats_in[i - 1, :, here]
            t = t.T
            rms = lax.rsqrt(t[:, 0:1] / full + EPS)
            tt[:, 0:1] = rms
            tt[:, 1:2] = rms * rms * rms * (t[:, 1:2] / full)

            def tile(r):
                rows = at(c * (Q // TILE) + r, TILE)
                near = at(r, TILE)
                rm, co = tt[near, 0:1], tt[near, 1:2]
                x = act[rows, 0:C].astype(f32)
                m = ys[rows, :] + sk[...] * x
                g = gate[rows, :].astype(f32)
                sig = sigmoid(g)
                ga = g * sig
                gated = m * ga
                scaled_rows = gated * rm
                gn[rows, :] = (scaled_rows * gg[...]).astype(bf16)
                d = dy[rows, :]
                dgd = rm * (d * gg[...]) - gated * co
                dmix = dgd * ga
                dg[rows, :] = (dgd * m * (sig * (1.0 + g * (1.0 - sig)))).astype(bf16)
                dy[rows, :] = dmix
                sums[0:8, :] += fold8(d * scaled_rows)
                sums[8:16, :] += fold8(dmix * x)

            loop(Q // TILE, tile, 4)
        loop(NC, gate_back)
        part1[s * L : (s + 1) * L, :] = mm(gn[s * L : (s + 1) * L, :], wo[...]).astype(bf16)
        fold1.begin(s * (tiles // S), tiles // S)

    def rewind(s):
        st[...] = jnp.zeros_like(st)

        def back(k):
            c = s * NC + NC - 1 - k
            last = cum[pl.ds(pl.multiple_of(c * Q + Q - 8, 8), 8), :][7:8]
            later[c] = st[...]
            st[...] = st[...] * row_of(jnp.exp(last), e[...]) + mm2(act[at(c, Q), C + Q :], spread_dy(c), TN)

        loop(NC, back, NC)
        fin[s] = st[...].astype(bf16)
        relays2.append(Relay(s, (fin, tot), (slots, slots_t), b_sem, seqs, -1))
        relays2[s].start()

    cross(1)
    gating(0)
    for r in relays:
        r.finish()
    gating(1)
    rewind(0)
    fold1.step(0)
    rewind(1)
    fold1.step(1)

    HG = D // 2
    PR = HG // seqs

    def pair(k):
        return remote(gr.at[k, at(other, HG)], gr_in.at[k], ga_s.at[k], ga_r.at[k], sample=other)

    for i in range(D // C):
        gr[0, i * C : (i + 1) * C, :] = mm(gn[...], cot[:, i * C : (i + 1) * C], TN).astype(bf16)
    pair(0).start()
    fold1.step(2)

    def turn(i):
        rows = at(i, 256)
        nt[:, rows] = (xb[rows, :].astype(f32) * inv[rows, 0:1] * gain[...]).astype(bf16).T

    loop(T // 256, turn)
    fold1.step(3)

    def outer2(i):
        gr[1, at(i, 512), :] = mm(nt[at(i, 512), :], dg[...]).astype(bf16)

    loop(D // 512, outer2)
    pair(1).start()
    fold1.step(4)

    hsums[...] = jnp.zeros_like(hsums)
    acc[...] = jnp.zeros_like(acc)
    nsums[...] = jnp.zeros_like(nsums)
    LT = L // TILE

    def next_rows(s):
        return remote(edge8.at[s], nx.at[s], nx_s.at[s], nx_r.at[s], seq=ps - 1)

    @pl.when(ps == seqs - 1)
    def _():
        nx[...] = jnp.zeros_like(nx)

    def settle(k):
        pair(k).wait_recv()

        def tile(i):
            r = pl.ds(pl.multiple_of(pc * HG + i * TILE, TILE), TILE)
            v = gr[k, r, :].astype(f32) + gr_in[k, at(i, TILE), :].astype(f32)
            gr[k, r, :] = v.astype(bf16)

        loop(HG // TILE, tile)

    def piece(k, i):
        r = pl.ds(pl.multiple_of(pc * HG + ring(i) * PR, PR), PR)
        return remote(gr.at[k, r], gr_pieces.at[k, i - 1], gb_s.at[k, i - 1], gb_r.at[k, i - 1], seq=ring(i))

    def gather_pieces(k):
        for i in range(1, seqs):
            piece(k, i).wait_recv()

        def tile(j):
            r = at(j, TILE)
            v = gr[k, pl.ds(pl.multiple_of(pc * HG + ps * PR + j * TILE, TILE), TILE), :].astype(f32)
            for i in range(1, seqs):
                v = v + gr_pieces[k, i - 1, r, :].astype(f32)
            gr_sum[k, r, :] = v.astype(bf16)
            grads[k, pl.ds(pl.multiple_of(pc * HG + ps * PR + j * TILE, TILE), TILE), :] = v.astype(bf16)

        loop(PR // TILE, tile)

    def spread(k, i):
        r = pl.ds(pl.multiple_of(pc * HG + ps * PR, PR), PR)
        return remote(gr_sum.at[k], grads.at[k, r], gc_s.at[k, i - 1], gc_r.at[k, i - 1], seq=ring(i))

    def hand(k, i):
        q = lax.rem(ps + seqs - i, seqs)
        r = pl.ds(pl.multiple_of(pc * HG + q * PR, PR), PR)
        src = gr_sum.at[k] if i == 0 else grads.at[k, r]
        return remote(src, grads.at[k, r], gd_s.at[k, i], gd_r.at[k, i], sample=other)

    def send_out(k):
        gather_pieces(k)
        for i in range(1, seqs):
            spread(k, i).start()
        hand(k, 0).start()

    def hand_on(k):
        for i in range(1, seqs):
            q = lax.rem(ps + seqs - i, seqs)
            r = pl.ds(pl.multiple_of(pc * HG + q * PR, PR), PR)
            remote(gr_sum.at[k], grads.at[k, r], gc_s.at[k, i - 1], gc_r.at[k, i - 1], seq=ring(i)).wait_recv()
            hand(k, i).start()

    def result(k):
        return pltpu.make_async_copy(grads.at[k], grads_out.at[k], out_sem.at[k])

    def complete(k):
        for i in range(seqs):
            q = lax.rem(ps + seqs - i, seqs)
            r = pl.ds(pl.multiple_of(other * HG + q * PR, PR), PR)
            remote(gr_sum.at[k], grads.at[k, r], gd_s.at[k, i], gd_r.at[k, i], sample=other).wait()
        result(k).start()

    def send_pieces(k):
        settle(k)
        for i in range(1, seqs):
            piece(k, i).start()

    send_pieces(0)
    send_pieces(1)
    fold1.step(5)
    for s in range(S):
        relays2[s].gather(chained, e)
        off[...] = jnp.zeros_like(off)

        def state_back(k):
            kk = NC - 1 - k
            c = s * NC + kk
            here = at(c, Q)
            run = cum[here, :]
            last = run[Q - 1 : Q, :]
            ds = later[c] + row_of(jnp.exp(off[0:1, :]), e[...]) * chained[s]
            off[...] += jnp.broadcast_to(last, (8, Q))
            upper = iota((Q, Q), 1) >= 64
            causal = iota((Q, Q), 0) >= iota((Q, Q), 1)
            b, r = act[here, C : C + Q], act[here, C + Q :]
            scores = mm(r, b, NT)
            dsc = jnp.zeros((Q, Q), f32)
            for p in range(C // Q):
                lanes = slice(p * Q, (p + 1) * Q)
                xp = act[here, lanes]
                dyp = dy[here, lanes].astype(bf16)
                dyl = (dy[here, lanes] - dyp.astype(f32)).astype(bf16)
                dx = jnp.zeros((Q, Q), f32)
                for o in range(2):
                    keep = upper == bool(o)
                    dym = jnp.where(keep, dyp, jnp.zeros_like(dyp))
                    dyn = jnp.where(keep, dyl, jnp.zeros_like(dyl))
                    w = weights_of(2 * p + o, here, causal)
                    dsc = dsc + (mm(dym, xp, NT) + mm(dyn, xp, NT)) * w
                    dx = dx + mm((scores * w).astype(bf16), dym, TN)
                work[0, :, lanes] = dx
            d = dt[here, :]
            work[2] = mm2(jnp.exp(last - run) * d, e[...])
            work[1] = work[2] * mm2(b, ds)
            d_read = mm2(dsc, b) + mm3(spread_dy(c), entry[c], NT)
            d_in = mm2(dsc, r, TN) + mm3(act[here, 0:C].astype(f32) * work[2], ds, NT)
            slope[here, C : C + Q] = d_in * slope[here, C : C + Q]
            slope[here, C + Q :] = d_read * slope[here, C + Q :]

            def tile(i):
                rows = at(c * (Q // TILE) + i, TILE)
                near = at(i, TILE)
                x = act[rows, 0:C].astype(f32)
                g = dy[rows, :]
                a, o = work[0, near, :], work[1, near, :]
                work[3, near, :] = g.astype(bf16).astype(f32) * ys[rows, :] - x * a
                work[4, near, :] = x * o
                both = a + o
                work[5, near, :] = x * both
                slope[rows, 0:C] = (both + sk[...] * g) * slope[rows, 0:C]

            loop(Q // TILE, tile, 4)
            ha = mm2(work[3], e[...], NT)
            hb = mm2(work[4], e[...], NT)
            hc = mm2(work[5], e[...], NT)
            crossing = mm2(fold8(entry[c] * ds), e[...], NT)
            crossing = jnp.sum(crossing, axis=0, keepdims=True) * jnp.exp(last)
            dlog = (
                mm2(triangle(lambda i, j: i <= j).astype(bf16), ha)
                + mm2(triangle(lambda i, j: i > j).astype(bf16), hb)
                + crossing
            )
            g = sg[here, :]
            ratio = jnp.where(d > 1e-30, g / jnp.maximum(d, 1e-30), 1.0)
            rate = hp[1:2, :]
            draw = rate * dlog * g + hc * ratio
            dcs[here, 2 * Q :] = draw.astype(bf16)
            hsums[0:8, :] += fold8(draw)
            hsums[8:16, :] += fold8(rate * dlog * d)
            fold1.step((6 if s == 0 else 12) + k)

        loop(NC, state_back)
        edge8[s] = slope[s * L : s * L + 8, :]

        @pl.when(ps > 0)
        def _():
            next_rows(s).start()

        def conv_back(r, last):
            for lo in range(0, W, 256):
                lanes = slice(lo, lo + 256)
                if last:
                    w = jnp.concatenate([slope[(s + 1) * L - TILE : (s + 1) * L, lanes], nx[s, :, lanes]], axis=0)
                else:
                    w = slope[pl.ds(pl.multiple_of(s * L + r * TILE, TILE), TILE + 8), lanes]
                u = pad[s, pl.ds(pl.multiple_of(r * TILE, TILE), TILE + HALO), lanes].astype(f32)
                d = w[0:TILE]
                v = cw[3:4, lanes] * d
                for k in range(3):
                    v = v + cw[k : k + 1, lanes] * w[3 - k : 3 - k + TILE]
                rows = at(r + s * LT, TILE)
                if lo < C:
                    gate[rows, lanes] = v.astype(bf16)
                else:
                    dcs[rows, lo - C : lo - C + 256] = v.astype(bf16)
                for k in range(4):
                    acc[8 * k : 8 * k + 8, lanes] += fold8(d * u[13 + k : 13 + k + TILE])
                acc[32:40, lanes] += fold8(d)

        loop(LT - 1, lambda r: conv_back(r, False))
        if s == 0:
            fold1.step(10)
        else:
            fold1.step(16)
            fold1.step(17)
            fold2.step(0)

        @pl.when(ps < seqs - 1)
        def _():
            next_rows(s).wait_recv()

        conv_back(LT - 1, True)
        if s > 0:
            fold2.step(1)

        def into(k):
            i = s * (L // 256) + k
            rows = at(i, 256)
            v = mm(dg[rows, :], wg[...], NT) + mm(gate[rows, :], wv[...], NT) + mm(dcs[rows, :], wst[...])
            part2[rows, :] = v.astype(bf16)
            nsums[...] += fold8(v * xb[rows, :].astype(f32) * inv[rows, 0:1])

        loop(L // 256, into)
        if s == 0:
            fold2.begin(0, tiles // S)
            fold1.step(11)
            send_out(0)

    for k in range(5):
        row = jnp.sum(acc[8 * k : 8 * k + 8, :], axis=0, keepdims=True)
        small[k : k + 1, :] = row[:, 0:C]
        smallz[k : k + 1, 0 : 2 * Q] = row[:, C:]
        smallz[k : k + 1, 2 * Q :] = jnp.zeros((1, C - 2 * Q), f32)
    ngrad = jnp.sum(nsums[...], axis=0, keepdims=True)
    for j in range(D // C):
        smallz[5 + j : 6 + j, :] = ngrad[:, j * C : (j + 1) * C]
    smallz[7:8, :] = jnp.zeros((1, C), f32)

    def to_line(i):
        return remote(smallz, smallz_in.at[i - 1], m1_s.at[i - 1], m1_r.at[i - 1], head=line(i))

    for i in range(1, lines):
        to_line(i).start()
    held = 6
    fold2.begin(tiles // S, tiles - tiles // S - held)
    fold1.step(18)
    fold1.step(19)
    fold2.step(2)

    rest = fold2.last(13, 6)
    for k in range(D // Q):
        t = mm(nt[k * Q : (k + 1) * Q, :], dcs[...])
        for j in range(2):
            later[j * DC + k * Q // C, :, k * Q % C : k * Q % C + Q] = t[:, j * Q : (j + 1) * Q].T
        row = 8 + 8 * (k * Q // C)
        small[row : row + 8, k * Q % C : k * Q % C + Q] = t[:, 2 * Q :].T[0:8]

    SR = Q // seqs
    keep_state = at(pc, DC)

    def state_pair():
        return remote(later.at[at(other, DC)], sg_in, sa_s, sa_r, sample=other)

    state_pair().start()
    small[5:6, :] = jnp.sum(sums[0:8, :], axis=0, keepdims=True)
    small[6:7, :] = jnp.sum(sums[8:16, :], axis=0, keepdims=True)
    small[7:8, :] = jnp.zeros((1, C), f32)
    small[7:8, 0:Q] = jnp.sum(hsums[0:8, :], axis=0, keepdims=True)
    small[7:8, Q : 2 * Q] = jnp.sum(hsums[8:16, :], axis=0, keepdims=True)
    fold2.step(3)
    def outer3(i):
        gr[2, at(i, 512), :] = mm(nt[at(i, 512), :], gate[...]).astype(bf16)

    loop(D // 512, outer3)
    pair(2).start()
    fold2.step(4)
    state_pair().wait_recv()
    later[keep_state] = later[keep_state] + sg_in[...]

    def state_piece(i):
        return remote(later.at[keep_state, at(ring(i), SR)], sg_pieces.at[i - 1], sb_s.at[i - 1], sb_r.at[i - 1], seq=ring(i))

    for i in range(1, seqs):
        state_piece(i).start()
    fold2.step(5)
    send_pieces(2)
    fold2.step(6)
    hand_on(0)
    fold2.step(7)
    fold2.step(8)
    for i in range(1, seqs):
        state_piece(i).wait_recv()
    v = later[keep_state, at(ps, SR), :]
    for i in range(1, seqs):
        v = v + sg_pieces[i - 1]
    sg_wire[...] = v.astype(bf16)
    sg_sum[...] = v
    owner = (ps * SR) // own

    def to_owner(i):
        return remote(sg_wire, sg_line.at[i - 1], sz_s.at[i - 1], sz_r.at[i - 1], head=line(i))

    for i in range(1, lines):

        @pl.when(line(i) == owner)
        def _():
            to_owner(i).start()

    fold2.begin(tiles - held, held)
    fold2.step(9)
    send_out(1)
    fold2.step(10)
    total = smallz[...]
    for i in range(1, lines):
        to_line(i).wait_recv()
        total = total + smallz_in[i - 1]
    small[24:32, :] = total

    def to_core():
        return remote(small, small_two.at[0], m2_s.at[seqs - 1], m2_r.at[seqs - 1], sample=other)

    def to_peer(i):
        return remote(small_two.at[1], small_in.at[i - 1], m2_s.at[i - 1], m2_r.at[i - 1], seq=ring(i))

    to_core().start()
    fold2.step(11)
    send_out(2)
    fold2.step(12)
    to_core().wait_recv()
    small_two[1] = small[...] + small_two[0]
    for i in range(1, seqs):
        to_peer(i).start()
    fold2.step(13)
    span = max(own // SR, 1)

    def place_row(q, core):
        return pl.ds(pl.multiple_of(core * own + lax.rem(q * SR, own), SR), SR)

    def state_out_to(i):
        return remote(sg_sum, state_out.at[:, place_row(ps, pc)], sc_s.at[i - 1], sc_r.at[i - 1], seq=ring(i))

    def state_hand(j, src):
        q = ph * span + j
        return remote(src, state_out.at[:, place_row(q, pc)], sd_s.at[j], sd_r.at[j], sample=other)

    @pl.when(ph == owner)
    def _():
        t = sg_sum[...]
        for i in range(1, lines):
            to_owner(i).wait_recv()
            t = t + sg_line[i - 1].astype(f32)
        sg_sum[...] = t
        state_out[:, place_row(ps, pc), :] = t
        for i in range(1, seqs):
            state_out_to(i).start()

    for move, i in rest[0]:
        move(i)
    hand_on(1)
    complete(0)
    for move, i in rest[1]:
        move(i)
    for move, i in rest[2]:
        move(i)
    hand_on(2)
    complete(1)
    for move, i in rest[3]:
        move(i)
    total = small_two[1]
    for i in range(1, seqs):
        to_peer(i).wait_recv()
        total = total + small_in[i - 1]
    small_out[...] = total
    for move, i in rest[4]:
        move(i)
    for move, i in rest[5]:
        move(i)
    for j in range(span):
        q = ph * span + j

        @pl.when(q == ps)
        def _():
            state_hand(j, sg_sum).start()

        for i in range(1, seqs):

            @pl.when(ring(seqs - i) == q)
            def _():
                remote(
                    sg_sum, state_out.at[:, place_row(q, pc)], sc_s.at[i - 1], sc_r.at[i - 1], seq=ring(i)
                ).wait_recv()
                state_hand(j, state_out.at[:, place_row(q, pc)]).start()


    complete(2)
    fold1.end()
    fold2.end()
    for r in relays2:
        r.finish()
    for i in range(1, lines):
        for c in weights(i, ph):
            c.wait_send()
        for s in range(S):
            stat(s, i).wait_send()
        to_line(i).wait_send()

        @pl.when(line(i) == owner)
        def _():
            to_owner(i).wait_send()

    @pl.when(ps < seqs - 1)
    def _():
        for s in range(S):
            halo(s).wait_send()

    @pl.when(ps > 0)
    def _():
        for s in range(S):
            next_rows(s).wait_send()

    for k in range(3):
        pair(k).wait_send()
        for i in range(1, seqs):
            piece(k, i).wait_send()
            spread(k, i).wait_send()
        result(k).wait()
    state_pair().wait_send()
    share().wait_send()
    for i in range(1, seqs):
        state_piece(i).wait_send()

        @pl.when(ph == owner)
        def _():
            state_out_to(i).wait_send()

    for j in range(span):
        q = ph * span + j
        remote(sg_sum, state_out.at[:, place_row(q, other)], sd_s.at[j], sd_r.at[j], sample=other).wait()
    to_core().wait_send()
    for i in range(1, seqs):
        to_peer(i).wait_send()


def finish(
    lines, x, cot, gain, dn, outs, g_out, g_gate, g_value, state, small,
    block_out, input_grad, gate_grad, value_grad, out_grad,
    state_grad, norm_grad, step_grad, cv, cs, cvb, csb, sbias, dlog, skip, gated_gain,
):
    rows, width = x.shape
    for j in range(rows // 16):
        r = slice(j * 16, (j + 1) * 16)
        v = x[r, :].astype(f32)
        block_out[r, :] = (v + outs[r, :].astype(f32)).astype(bf16)
        s = dn[r, :].astype(f32) * gain[...]
        i1 = lax.rsqrt(jnp.mean(v * v, axis=1, keepdims=True) + EPS)
        m = jnp.mean(s * v, axis=1, keepdims=True)
        input_grad[r, :] = cot[r, :].astype(f32) + i1 * s - v * (i1 * i1 * i1 * m)
    half = g_gate.shape[1]
    for j in range(width // half):
        out_grad[:, j * half : (j + 1) * half] = g_out[j].astype(f32)
    gate_grad[...] = g_gate[...].astype(f32)
    value_grad[...] = g_value[...].astype(f32)

    @pl.when(pl.program_id(0) == 0)
    def _():
        heads, own = sbias.shape[1], csb.shape[1]
        for j in range(width // half):
            lanes = slice(j * half, (j + 1) * half)
            state_grad[:, lanes] = state[j]
            norm_grad[:, lanes] = small[29 + j : 30 + j, :]
            step_grad[:, lanes] = small[8 + 8 * j : 16 + 8 * j, :]
        cv[...] = small[0:4, :]
        cvb[...] = small[4:5, :]
        gated_gain[...] = small[5:6, :]
        e = lane_heads(half // 64, half)
        skip[...] = mm(jnp.broadcast_to(small[6:7, :], (8, half)), e.astype(f32), NT, HI)[0:1, 0:heads]
        sbias[...] = small[7:8, 0:heads]
        dlog[...] = small[7:8, Q : Q + heads]
        for h in range(lines):

            @pl.when(lax.axis_index("head") == h)
            def _():
                for j in range(2):
                    lanes = slice(j * Q + h * own, j * Q + (h + 1) * own)
                    cs[:, j, :] = small[24:28, lanes]
                    csb[j : j + 1, :] = small[28:29, lanes]


def per_device(
    block_in, out_cotangent, norm_gain, gate_proj, value_proj, state_proj, step_proj,
    conv_value, conv_state, conv_value_bias, conv_state_bias, step_bias, decay_log,
    skip_gain, gated_gain, out_proj,
):
    S, L, D = block_in.shape
    T = S * L
    heads = step_proj.shape[1]
    C = gate_proj.shape[1]
    own = state_proj.shape[2]
    W = C + 2 * Q
    NCH = T // Q
    seqs, lines = lax.axis_size("seq"), lax.axis_size("head")
    tiles = 32
    H = D // 2
    PR = H // seqs
    SR = Q // seqs
    x = block_in.reshape(T, D)
    cot = out_cotangent.reshape(T, D)
    spt = state_proj.transpose(0, 2, 1).reshape(2 * own, D)
    gain = norm_gain[None]
    vm = pl.BlockSpec(memory_space=pltpu.VMEM)
    hbm = pl.BlockSpec(memory_space=pl.ANY)
    dma = pltpu.SemaphoreType.DMA
    n1, l1 = seqs - 1, lines - 1
    V = pltpu.VMEM
    scratch = [
        V((T, D), bf16), V((T, D), bf16), V((D, C), bf16), V((D, C), bf16), V((3 * Q, D), bf16),
        V((C, D), bf16), V((8, Q), f32), V((lines, 8, Q), f32), V((8, W), f32), V((8, Q), f32), V((1, C), f32),
        V((S * HALO, D), bf16),
        V((D, T), bf16), V((T, Q), f32), V((T, C), bf16), V((S, HALO + L, W), bf16), V((T, W), f32),
        V((T, W), bf16), V((T, Q), f32), V((T, Q), f32), V((T, Q), f32), V((8, T), f32), V((8, T), f32),
        V((NCH, Q, C), f32), V((T, C), f32), V((T, C), f32), V((T, C), bf16), V((T, C), bf16),
        V((NCH, Q, C), f32),
        V((T, 3 * Q), bf16), V((Q, C), bf16), V((Q, C), f32), V((6, Q, C), f32),
        V((8, Q), f32), V((Q, Q), f32), V((2, Q, Q), f32), V((8, T), f32), V((l1, 8, T), f32),
        V((S, Q, C), bf16), V((S, 8, Q), f32), V((seqs, S, Q, C), bf16), V((seqs, S, 8, Q), f32),
        V((S, Q, C), f32),
        V((T, D), bf16), V((T, D), bf16), V((T, D), bf16), V((T, D), bf16), V((T, D), bf16), V((T, D), bf16),
        V((3, D, C), bf16), V((3, D, C), bf16), V((3, H, C), bf16), V((3, n1, PR, C), bf16), V((3, PR, C), bf16),
        V((D // C, Q, C), f32), V((n1, D // C, SR, C), f32), V((l1, D // C, SR, C), bf16),
        V((D // C, SR, C), bf16), V((D // C, SR, C), f32),
        V((40, W), f32), V((16, Q), f32), V((16, C), f32), V((8, D), f32), V((8, C), f32),
        V((l1, 8, C), f32), V((32, C), f32), V((2, 32, C), f32), V((n1, 32, C), f32), V((S, 8, W), f32), V((S, 8, W), f32),
        dma((S + 5,)), dma((2, S)), dma((2, lines)), dma((2, lines)), dma((2, 2, S, n1)), dma((2, 2, S, n1)),
        dma((S, l1)), dma((S, l1)), dma((S,)), dma((S,)),
        dma((2, tiles)), dma((3,)), dma((2, tiles)), dma((3,)), dma((3,)), dma((3,)), dma((3, n1)), dma((3, n1)),
        dma((3, n1)), dma((3, n1)), dma((3, seqs)), dma((3, seqs)),
        dma((3,)), dma, dma, dma((n1,)), dma((n1,)), dma((l1,)), dma((l1,)), dma((n1,)), dma((n1,)),
        dma((max(own // SR, 1),)), dma((max(own // SR, 1),)), dma((l1,)), dma((l1,)), dma((seqs,)), dma((seqs,)),
    ]
    outs, dnorm, grads, state_out, small = pl.pallas_call(
        functools.partial(block, (S, L, seqs, lines, tiles)),
        out_shape=[
            jax.ShapeDtypeStruct((T, D), bf16), jax.ShapeDtypeStruct((T, D), bf16),
            jax.ShapeDtypeStruct((3, D, C), bf16), jax.ShapeDtypeStruct((D // C, 2 * own, C), f32),
            jax.ShapeDtypeStruct((32, C), f32),
        ],
        in_specs=[hbm, hbm, vm, hbm, hbm, hbm, vm, hbm] + [vm] * 8,
        out_specs=[hbm, hbm, hbm, vm, vm],
        scratch_shapes=scratch,
        name="block",
        compiler_params=pltpu.CompilerParams(
            collective_id=0, has_side_effects=True, vmem_limit_bytes=67043328
        ),
    )(
        x, cot, gain, gate_proj, value_proj, spt, step_proj.T, out_proj, conv_state, conv_state_bias,
        conv_value, conv_value_bias[None], step_bias[None], decay_log[None], skip_gain[None], gated_gain[None],
    )
    steps = 4

    def whole(*shape):
        return pl.BlockSpec(shape, lambda i: (0,) * len(shape))

    by_rows = pl.BlockSpec((T // steps, D), lambda i: (i, 0))
    by_grad = pl.BlockSpec((D // steps, C), lambda i: (i, 0))
    shape = jax.ShapeDtypeStruct
    (block_out, input_grad, gate_grad, value_grad, out_grad, state_grad, norm_grad, step_grad, cv, cs, cvb, csb,
     sbias, dlog, skip, gated) = pl.pallas_call(
        functools.partial(finish, lines),
        grid=(steps,),
        out_shape=[
            shape((T, D), bf16), shape((T, D), f32), shape((D, C), f32), shape((D, C), f32), shape((C, D), f32),
            shape((2 * own, D), f32), shape((1, D), f32), shape((heads, D), f32), shape((4, C), f32),
            shape((4, 2, own), f32), shape((1, C), f32), shape((2, own), f32), shape((1, heads), f32),
            shape((1, heads), f32), shape((1, heads), f32), shape((1, C), f32),
        ],
        in_specs=[
            by_rows, by_rows, whole(1, D), by_rows, by_rows,
            pl.BlockSpec((None, D // C, C // steps, C), lambda i: (0, 0, i, 0)),
            pl.BlockSpec((None, D // steps, C), lambda i: (1, i, 0)),
            pl.BlockSpec((None, D // steps, C), lambda i: (2, i, 0)),
            whole(D // C, 2 * own, C), whole(32, C),
        ],
        out_specs=[
            by_rows, by_rows, by_grad, by_grad, pl.BlockSpec((C // steps, D), lambda i: (i, 0)),
            whole(2 * own, D), whole(1, D), whole(heads, D), whole(4, C), whole(4, 2, own), whole(1, C),
            whole(2, own), whole(1, heads), whole(1, heads), whole(1, heads), whole(1, C),
        ],
        name="finish",
        compiler_params=pltpu.CompilerParams(vmem_limit_bytes=60 * 2**20),
    )(x, cot, gain, dnorm, outs, grads.reshape(3, D // C, C, C), grads, grads, state_out, small)
    return (
        block_out.reshape(S, L, D), input_grad.reshape(S, L, D), norm_grad[0], gate_grad, value_grad,
        state_grad.reshape(2, own, D).transpose(0, 2, 1), step_grad.T, cv, cs, cvb[0], csb, sbias[0], dlog[0],
        skip[0], gated[0], out_grad,
    )


def solution(mesh):
    tokens = P("sample", "seq", None)
    params = (
        P(), P(None, "head"), P(None, "head"), P(None, None, "head"), P(None, "head"),
        P(None, "head"), P(None, None, "head"), P("head"), P(None, "head"), P("head"),
        P("head"), P("head"), P("head"), P("head", None),
    )
    return jax.shard_map(
        per_device,
        mesh=mesh,
        in_specs=(tokens, tokens) + params,
        out_specs=(tokens, tokens) + params,
        check_vma=False,
    )
```

```python
import functools

import jax
import jax.numpy as jnp
from jax import lax
from jax.experimental import pallas as pl
from jax.experimental.pallas import tpu as pltpu
from jax.sharding import PartitionSpec as P

f32, bf16 = jnp.float32, jnp.bfloat16
HI = lax.Precision.HIGHEST
MESH = pl.DeviceIdType.MESH
Q = 128
TILE = 32
HALO = 16
EPS = 1e-05
NN, NT, TN = ((1,), (0,)), ((1,), (1,)), ((0,), (0,))


def mm(a, b, dims=NN, precision=None):
    return lax.dot_general(
        a, b, (dims, ((), ())), preferred_element_type=f32, precision=precision
    )


def halves(v):
    high = v.astype(bf16)
    return high, (v - high.astype(f32)).astype(bf16)


def mm2(a, b, dims=NN):
    if a.dtype == bf16:
        high, low = halves(b)
        return mm(a, high, dims) + mm(a, low, dims)
    high, low = halves(a)
    return mm(high, b, dims) + mm(low, b, dims)


def mm3(a, b, dims=NN):
    ah, al = halves(a)
    bh, bl = halves(b)
    return mm(ah, bh, dims) + (mm(ah, bl, dims) + mm(al, bh, dims))


def at(i, n):
    return pl.ds(i * n if isinstance(i, int) else pl.multiple_of(i * n, n), n)


def loop(count, body, each=1):
    def step(i, carry):
        for j in range(each):
            body(i * each + j)
        return carry

    if count == each:
        for i in range(count):
            body(i)
    else:
        lax.fori_loop(0, count // each, step, 0)


def iota(shape, axis):
    return lax.broadcasted_iota(jnp.int32, shape, axis)


def lane_heads(heads, width):
    shift = (width // heads).bit_length() - 1
    return ((iota((Q, width), 1) >> shift) == iota((Q, width), 0)).astype(f32).astype(bf16)


def triangle(keep):
    return jnp.where(keep(iota((Q, Q), 0), iota((Q, Q), 1)), 1.0, 0.0)


def fold8(v):
    return jnp.sum(v.reshape(v.shape[0] // 8, 8, v.shape[1]), axis=0)


def row_of(v, e):
    return mm2(jnp.broadcast_to(v, (8, Q)), e)[0:1]


def sigmoid(v):
    return 0.5 * jnp.tanh(0.5 * v) + 0.5


def normalize(v, gain):
    inv = lax.rsqrt(jnp.mean(v * v, axis=1, keepdims=True) + EPS)
    return (v * inv * gain).astype(bf16), inv


def remote(src, dst, send, recv, **place):
    return pltpu.make_async_remote_copy(
        src_ref=src, dst_ref=dst, send_sem=send, recv_sem=recv, device_id=place, device_id_type=MESH
    )


class Fold:
    def __init__(self, part, near, far, result, sems, tiles):
        self.part, self.near, self.far, self.result, self.tiles = part, near, far, result, tiles
        (self.b, self.d), (self.a, self.c, self.e) = sems
        self.rows = part.shape[0] // tiles
        place = lax.axis_index("head")
        self.inner = (place == 1) | (place == 2)
        self.beside = jnp.where(place < 2, 1 - place, 5 - place)
        self.across = 3 - place

    def outward(self, i, src):
        r = at(i, self.rows)
        return remote(src.at[r], self.near.at[r], self.a, self.b.at[i], head=self.beside)

    def middle(self, i):
        r = at(i, self.rows)
        return remote(self.part.at[r], self.far.at[r], self.c, self.d.at[i], head=self.across)

    def store(self, i):
        r = at(i, self.rows)
        return pltpu.make_async_copy(self.near.at[r], self.result.at[r], self.e)

    def take(self, i):
        @pl.when(jnp.logical_not(self.inner))
        def _():
            self.outward(i, self.near).wait_recv()
            self.store(i).start()

    def begin(self, first, count):
        @pl.when(jnp.logical_not(self.inner))
        def _():
            loop(count, lambda i: self.outward(first + i, self.part).start())

    def add(self, dst, u, v, i):
        def tile(j):
            r = at(i * (self.rows // TILE) + j, TILE)
            dst[r, :] = (u[r, :].astype(f32) + v[r, :].astype(f32)).astype(bf16)

        loop(self.rows // TILE, tile)

    def one(self, i):
        @pl.when(self.inner)
        def _():
            self.outward(i, self.near).wait_recv()
            self.add(self.part, self.part, self.near, i)
            self.middle(i).start()

    def two(self, i):
        @pl.when(self.inner)
        def _():
            self.middle(i).wait_recv()
            self.add(self.near, self.part, self.far, i)
            self.outward(i, self.near).start()
            self.store(i).start()

    def step(self, j):
        for ago, move in ((0, self.one), (4, self.two), (8, self.take)):
            if isinstance(j, int):
                first, end = max(2 * j - ago, 0), min(2 * j - ago + 2, self.tiles)
                if first < end:
                    loop(end - first, lambda q: move(first + q))
            else:
                for q in range(2):
                    i = 2 * j - ago + q

                    @pl.when((i >= 0) & (i < self.tiles))
                    def _():
                        move(i)

    def closely(self, j):
        def tile(q):
            self.one(2 * j + q)
            self.two(2 * j - 3 + q)
            if 2 * j >= 7:
                self.take(2 * j - 7 + q)

        loop(2, tile)

    def last(self, j, parts):
        o, t, k = 2 * j + 2, 2 * j - 1, 2 * j - 5
        moves = []
        while k < self.tiles:
            if o < self.tiles:
                moves.append((self.one, o))
                o += 1
            for unused in range(2):
                if t < self.tiles and (t < o - 2 or o == self.tiles):
                    moves.append((self.two, t))
                    t += 1
            for unused in range(2):
                if k < self.tiles and (k < t - 3 or t == self.tiles):
                    moves.append((self.take, k))
                    k += 1
        size = -(-len(moves) // parts)
        return [moves[i : i + size] for i in range(0, len(moves), size)]

    def end(self):
        pltpu.make_async_copy(self.near, self.result, self.e).wait()
        remote(self.part, self.near, self.a, self.b.at[0], head=self.beside).wait_send()

        @pl.when(self.inner)
        def _():
            remote(self.part, self.far, self.c, self.d.at[0], head=self.across).wait_send()


def fold_sems(tiles, streams):
    return [tiles.at[j] for j in range(2)], [streams.at[j] for j in range(3)]


class Relay:
    def __init__(self, seq, blocks, slots, sems, count, way):
        self.seq, self.blocks, self.slots, self.sems = seq, blocks, slots, sems
        self.count, self.way = count, way
        self.place = lax.axis_index("seq")

    def copies(self, d, source):
        to = self.place + self.way * d
        return [
            remote(
                b.at[self.seq], s.at[source, self.seq], self.sems.at[0, j, self.seq, d - 1],
                self.sems.at[1, j, self.seq, d - 1], seq=to,
            )
            for j, (b, s) in enumerate(zip(self.blocks, self.slots))
        ]

    def reaches(self, d):
        return self.place + d < self.count if self.way > 0 else self.place >= d

    def hears(self, d):
        return self.place >= d if self.way > 0 else self.place + d < self.count

    def start(self):
        for d in range(1, self.count):

            @pl.when(self.reaches(d))
            def _():
                for c in self.copies(d, self.place):
                    c.start()

    def gather(self, state, e):
        q = self.seq
        state[q] = jnp.zeros(state.shape[1:], f32)
        for d in range(self.count - 1, 0, -1):

            @pl.when(self.hears(d))
            def _():
                source = self.place - self.way * d
                for c in self.copies(d, source):
                    c.wait_recv()
                decay = mm2(jnp.exp(self.slots[1][source, q]), e[...])[0:1]
                state[q] = state[q] * decay + self.slots[0][source, q].astype(f32)

    def finish(self):
        for d in range(1, self.count):

            @pl.when(self.reaches(d))
            def _():
                for c in self.copies(d, self.place):
                    c.wait_send()


def block(
    dims,
    x_in, cot_in, gain, wg_in, wv_in, spt, stp, wo_in, cs, csb, cv, cvb, sbias, dlog_in, skip, gg,
    outs, dnorm, grads_out, state_result, small_result,
    xb, cot, wg, wv, wst, wo, tapb, taps, cw, hp, sk, xh,
    nt, inv, gate, pad, slope, act, dt, sg, cum, cum_t, dt_t, entry, ys, dy, gn, dg, later,
    dcs, e, st, work, off, tt, stats, stats_t, stats_in,
    fin, tot, slots, slots_t, chained,
    part1, near1, far1, part2, near2, far2, grads, state_out, small_out,
    gr, gr_in, gr_pieces, gr_sum, sg_in, sg_pieces, sg_line, sg_wire, sg_sum, sg_done,
    acc, hsums, sums, nsums, smallz, smallz_in, small, small_two, small_in, nx, edge8,
    load, halo_sem, wt_s, wt_r, f_sem, b_sem, st_s, st_r, nx_s, nx_r,
    z1, y1, z2, y2, ga_s, ga_r, gb_s, gb_r, gc_s, gc_r, gd_s, gd_r,
    out_sem, sa_s, sa_r, sb_s, sb_r, sz_s, sz_r, sc_s, sc_r, sd_s, sd_r, m1_s, m1_r, m2_s, m2_r,
):
    S, L, seqs, lines, tiles = dims
    T, D = xb.shape
    C = wg.shape[1]
    W = C + 2 * Q
    NC = L // Q
    own = spt.shape[0] // 2
    full = C * lines
    ps, pc, ph = lax.axis_index("seq"), lax.axis_index("sample"), lax.axis_index("head")
    other = 1 - pc
    group = 2 * seqs
    DC = D // C
    mine = ps * 2 + pc
    nb = part1

    def peer(i):
        p = lax.rem(mine + i, group)
        return {"seq": p // 2, "sample": lax.rem(p, 2)}

    def line(i):
        return lax.rem(ph + i, lines)

    def ring(i):
        return lax.rem(ps + i, seqs)

    moves = [pltpu.make_async_copy(x_in.at[pl.ds(s * L, L)], xb.at[pl.ds(s * L, L)], load.at[s]) for s in range(S)]
    moves += [
        pltpu.make_async_copy(wg_in, wg, load.at[S]),
        pltpu.make_async_copy(wv_in, wv, load.at[S + 1]),
        pltpu.make_async_copy(
            spt.at[at(pc, own)], wst.at[pl.ds(pl.multiple_of(pc * Q + ph * own, own), own)], load.at[S + 2]
        ),
        pltpu.make_async_copy(wo_in, wo, load.at[S + 3]),
        pltpu.make_async_copy(cot_in, cot, load.at[S + 4]),
    ]
    for m in moves:
        m.start()
    barrier = pltpu.get_barrier_semaphore()
    for i in range(1, group):
        pl.semaphore_signal(barrier, inc=1, device_id=peer(i), device_id_type=MESH)
    for i in range(1, lines):
        pl.semaphore_signal(barrier, inc=1, device_id={"head": line(i)}, device_id_type=MESH)
    heads = stp.shape[0]
    tapb[...] = jnp.zeros_like(tapb)
    hp[...] = jnp.zeros_like(hp)
    for j in range(2):
        tapb[0:4, j * own : (j + 1) * own] = cs[:, j, :]
        tapb[4:5, j * own : (j + 1) * own] = csb[j : j + 1, :]
    taps[ph] = tapb[...]
    hp[0:1, 0:heads] = sbias[...]
    hp[1:2, 0:heads] = -jnp.exp(dlog_in[...])
    hp[2:3, 0:heads] = skip[...]
    wst[2 * Q :, :] = jnp.zeros((Q, D), bf16)
    wst[2 * Q : 2 * Q + heads, :] = stp[...]
    e[...] = lane_heads(C // 64, C)
    sk[...] = mm(hp[...], e[...].astype(f32), precision=HI)[2:3]

    def norm(s):
        moves[s].wait()

        def norm_rows(r):
            rows = at(s * (L // 16) + r, 16)
            v = xb[rows, :].astype(f32)
            i = lax.rsqrt(jnp.mean(v * v, axis=1, keepdims=True) + EPS)
            nb[rows, :] = (v * i * gain[...]).astype(bf16)
            inv[rows, :] = jnp.broadcast_to(i, (16, Q))

        loop(L // 16, norm_rows, 4)

    norm(0)
    pl.semaphore_wait(barrier, group - 1 + lines - 1)

    def halo(s):
        return remote(
            x_in.at[pl.ds(s * L + L - HALO, HALO)], xh.at[pl.ds(s * HALO, HALO)],
            halo_sem.at[0, s], halo_sem.at[1, s], seq=ps + 1,
        )

    @pl.when(ps < seqs - 1)
    def _():
        for s in range(S):
            halo(s).start()

    @pl.when(ps == 0)
    def _():
        xh[...] = jnp.zeros_like(xh)

    def weights(i, source):
        r = pl.ds(pl.multiple_of(pc * Q + source * own, own), own)
        parts = [(spt.at[at(pc, own)], wst.at[r]), (tapb, taps.at[source])]
        return [
            remote(a, b, wt_s.at[j, i - 1], wt_r.at[j, i - 1], head=line(i))
            for j, (a, b) in enumerate(parts)
        ]

    for i in range(1, lines):
        for c in weights(i, ph):
            c.start()

    for s in range(S):
        if s > 0:
            norm(s)
        else:
            moves[S].wait()
            moves[S + 1].wait()
        seq_rows = slice(s * L, (s + 1) * L)
        gate[seq_rows, :] = mm(nb[seq_rows, :], wg[...]).astype(bf16)
        pad[s, HALO:, 0:C] = mm(nb[seq_rows, :], wv[...]).astype(bf16)

    def conv(s, first, end):
        def conv_rows(r):
            for lo in range(first, end, 256):
                lanes = slice(lo, lo + 256)
                w = pad[s, pl.ds(pl.multiple_of(r * TILE, TILE), TILE + HALO), lanes].astype(f32)
                v = cw[4:5, lanes] + cw[0:1, lanes] * w[13 : 13 + TILE]
                for k in range(1, 4):
                    v = v + cw[k : k + 1, lanes] * w[13 + k : 13 + k + TILE]
                g = sigmoid(v)
                rows = at(r + s * (L // TILE), TILE)
                act[rows, lanes] = (v * g).astype(bf16)
                slope[rows, lanes] = g * (1.0 + v * (1.0 - g))

        loop(L // TILE, conv_rows, 2)

    cw[0:4, 0:C] = cv[...]
    cw[4:5, 0:C] = cvb[...]
    edges = []
    for s in range(S):

        @pl.when(ps > 0)
        def _():
            halo(s).wait_recv()

        edges.append(normalize(xh[s * HALO : (s + 1) * HALO, :].astype(f32), gain[...])[0])
        pad[s, 0:HALO, 0:C] = mm(edges[s], wv[...]).astype(bf16)
        conv(s, 0, C)
    moves[S + 3].wait()
    moves[S + 4].wait()
    for s in range(S):
        seq_rows = slice(s * L, (s + 1) * L)
        dy[seq_rows, :] = mm(cot[seq_rows, :], wo[...], NT)

    def share():
        r = at(pc, Q)
        return remote(wst.at[r], wst.at[r], wt_s.at[0, lines - 1], wt_r.at[0, lines - 1], sample=other)

    moves[S + 2].wait()
    for i in range(1, lines):
        for c in weights(i, line(lines - i)):
            c.wait_recv()
    share().start()
    for h in range(lines):
        for j in range(2):
            cw[:, C + j * Q + h * own : C + j * Q + (h + 1) * own] = taps[h, :, j * own : (j + 1) * own]
    r = at(other, Q)
    remote(wst.at[r], wst.at[r], wt_s.at[0, lines - 1], wt_r.at[0, lines - 1], sample=other).wait_recv()

    relays, relays2 = [], []
    for s in range(S):
        seq_rows = slice(s * L, (s + 1) * L)
        both = mm(nb[seq_rows, :], wst[...], NT)
        pad[s, HALO:, C:] = both[:, 0 : 2 * Q].astype(bf16)
        sg[seq_rows, :] = both[:, 2 * Q :]
        pad[s, 0:HALO, C:] = mm(edges[s], wst[0 : 2 * Q, :], NT).astype(bf16)
        conv(s, C, W)

        def steps(k):
            c = s * NC + k
            z = sg[at(c, Q), :] + hp[0:1, :]
            d = jax.nn.softplus(z)
            dt[at(c, Q), :] = d
            sg[at(c, Q), :] = sigmoid(z)
            step = d * hp[1:2, :]
            high, rest = halves(step)
            middle, low = halves(step - high.astype(f32))
            tri = triangle(lambda i, j: i >= j).astype(bf16)
            run = mm(tri, high) + (mm(tri, middle) + mm(tri, low))
            cum[at(c, Q), :] = run
            cum_t[:, at(c, Q)] = run.T[0:8]
            dt_t[:, at(c, Q)] = d.T[0:8]

        loop(NC, steps, 2)
        st[...] = jnp.zeros_like(st)
        tot[s] = jnp.zeros((8, Q), f32)

        def chunk(k):
            c = s * NC + k
            run = cum[at(c, Q), :]
            last = run[Q - 1 : Q, :]
            tail = mm2(jnp.exp(last - run) * dt[at(c, Q), :], e[...])
            xt = act[at(c, Q), 0:C].astype(f32) * tail
            entry[c] = st[...]
            st[...] = st[...] * row_of(jnp.exp(last), e[...]) + mm2(act[at(c, Q), C : C + Q], xt, TN)
            tot[s] += jnp.broadcast_to(last, (8, Q))

        loop(NC, chunk, NC)
        fin[s] = st[...].astype(bf16)
        relays.append(Relay(s, (fin, tot), (slots, slots_t), f_sem, seqs, 1))
        if s == 0:
            relays[s].start()

    def weights_of(h, here, causal):
        gap = cum[here, h : h + 1] - cum_t[h : h + 1, here]
        return jnp.exp(jnp.where(causal, gap, -1e30)) * dt_t[h : h + 1, here]

    def within(c):
        here = at(c, Q)
        scores = mm(act[here, C + Q :], act[here, C : C + Q], NT)
        causal = iota((Q, Q), 0) >= iota((Q, Q), 1)
        upper = iota((Q, Q), 1) >= 64
        for p in range(C // Q):
            xp = act[here, p * Q : (p + 1) * Q]
            y = jnp.zeros((Q, Q), f32)
            for o in range(2):
                m = (scores * weights_of(2 * p + o, here, causal)).astype(bf16)
                y = y + mm(m, jnp.where(upper == bool(o), xp, jnp.zeros_like(xp)))
            ys[here, p * Q : (p + 1) * Q] = y

    loop(NC, within)
    relays[1].start()

    def stat(s, i):
        part = pl.ds(s * L, L)
        return remote(
            stats_t.at[:, part], stats_in.at[i - 1, :, part], st_s.at[s, i - 1], st_r.at[s, i - 1], head=line(i)
        )

    stats_t[...] = jnp.zeros_like(stats_t)

    def cross(s):
        relays[s].gather(chained, e)
        off[...] = jnp.zeros_like(off)

        def across(k, lane=0):
            c = s * NC + k
            here = at(c, Q)
            si = entry[c] + row_of(jnp.exp(off[0:1, :]), e[...]) * chained[s]
            entry[c] = si
            run = cum[here, :]
            work[lane] = mm2(jnp.exp(run), e[...]) * mm2(act[here, C + Q :], si)
            off[...] += jnp.broadcast_to(run[Q - 1 : Q, :], (8, Q))

            def tile(r):
                rows = at(c * (Q // TILE) + r, TILE)
                y = ys[rows, :] + work[lane, at(r, TILE), :]
                ys[rows, :] = y
                m = y + sk[...] * act[rows, 0:C].astype(f32)
                g = gate[rows, :].astype(f32)
                gated = m * (g * sigmoid(g))
                a = gated * gated
                b = dy[rows, :] * gg[...] * gated
                stats[2 * lane, at(r, TILE), :] = sum(a[:, p * Q : (p + 1) * Q] for p in range(C // Q))
                stats[2 * lane + 1, at(r, TILE), :] = sum(b[:, p * Q : (p + 1) * Q] for p in range(C // Q))

            loop(Q // TILE, tile, 4)
            for j in range(2):
                stats_t[j : j + 1, here] = jnp.sum(stats[2 * lane + j].T, axis=0, keepdims=True)

        def pair_of(k):
            across(2 * k, 0)
            across(2 * k + 1, 1)

        loop(NC // 2, pair_of)
        for i in range(1, lines):
            stat(s, i).start()

    cross(0)
    loop(NC, lambda k: within(NC + k))
    sums[...] = jnp.zeros_like(sums)
    fold1 = Fold(part1, near1, far1, outs, fold_sems(z1, y1), tiles)
    fold2 = Fold(part2, near2, far2, dnorm, fold_sems(z2, y2), tiles)

    def spread_dy(c):
        return mm2(jnp.exp(cum[at(c, Q), :]), e[...]) * dy[at(c, Q), :]

    def gating(s):
        for i in range(1, lines):
            stat(s, i).wait_recv()

        def gate_back(k):
            c = s * NC + k
            here = at(c, Q)
            t = stats_t[:, here]
            for i in range(1, lines):
                t = t + stats_in[i - 1, :, here]
            t = t.T
            rms = lax.rsqrt(t[:, 0:1] / full + EPS)
            tt[:, 0:1] = rms
            tt[:, 1:2] = rms * rms * rms * (t[:, 1:2] / full)

            def tile(r):
                rows = at(c * (Q // TILE) + r, TILE)
                near = at(r, TILE)
                rm, co = tt[near, 0:1], tt[near, 1:2]
                x = act[rows, 0:C].astype(f32)
                m = ys[rows, :] + sk[...] * x
                g = gate[rows, :].astype(f32)
                sig = sigmoid(g)
                ga = g * sig
                gated = m * ga
                scaled_rows = gated * rm
                gn[rows, :] = (scaled_rows * gg[...]).astype(bf16)
                d = dy[rows, :]
                dgd = rm * (d * gg[...]) - gated * co
                dmix = dgd * ga
                dg[rows, :] = (dgd * m * (sig * (1.0 + g * (1.0 - sig)))).astype(bf16)
                dy[rows, :] = dmix
                sums[0:8, :] += fold8(d * scaled_rows)
                sums[8:16, :] += fold8(dmix * x)

            loop(Q // TILE, tile, 4)
            part1[here, :] = mm(gn[here, :], wo[...]).astype(bf16)
            fold1.begin(c * (tiles * Q // T), tiles * Q // T)
        loop(NC, gate_back)

    def rewind(s):
        st[...] = jnp.zeros_like(st)

        def back(k):
            c = s * NC + NC - 1 - k
            last = cum[pl.ds(pl.multiple_of(c * Q + Q - 8, 8), 8), :][7:8]
            later[c] = st[...]
            st[...] = st[...] * row_of(jnp.exp(last), e[...]) + mm2(act[at(c, Q), C + Q :], spread_dy(c), TN)

        loop(NC, back, NC)
        fin[s] = st[...].astype(bf16)
        relays2.append(Relay(s, (fin, tot), (slots, slots_t), b_sem, seqs, -1))
        relays2[s].start()

    cross(1)
    gating(0)
    for r in relays:
        r.finish()
    rewind(0)
    fold1.step(0)
    gating(1)
    rewind(1)
    fold1.step(1)

    HG = D // 2
    PR = HG // seqs

    def pair(k):
        return remote(gr.at[k, at(other, HG)], gr_in.at[k], ga_s.at[k], ga_r.at[k], sample=other)

    for i in range(D // C):
        gr[0, i * C : (i + 1) * C, :] = mm(gn[...], cot[:, i * C : (i + 1) * C], TN).astype(bf16)
    pair(0).start()

    def turn(i):
        rows = at(i, 256)
        nt[:, rows] = (xb[rows, :].astype(f32) * inv[rows, 0:1] * gain[...]).astype(bf16).T

    loop(T // 256, turn)
    fold1.step(2)

    def outer2(i):
        gr[1, at(i, 512), :] = mm(nt[at(i, 512), :], dg[...]).astype(bf16)

    loop(D // 512, outer2)
    pair(1).start()
    fold1.step(3)

    hsums[...] = jnp.zeros_like(hsums)
    acc[...] = jnp.zeros_like(acc)
    nsums[...] = jnp.zeros_like(nsums)
    LT = L // TILE

    def next_rows(s):
        return remote(edge8.at[s], nx.at[s], nx_s.at[s], nx_r.at[s], seq=ps - 1)

    @pl.when(ps == seqs - 1)
    def _():
        nx[...] = jnp.zeros_like(nx)

    def settle(k):
        pair(k).wait_recv()

        def tile(i):
            r = pl.ds(pl.multiple_of(pc * HG + i * TILE, TILE), TILE)
            v = gr[k, r, :].astype(f32) + gr_in[k, at(i, TILE), :].astype(f32)
            gr[k, r, :] = v.astype(bf16)

        loop(HG // TILE, tile)

    def piece(k, i):
        r = pl.ds(pl.multiple_of(pc * HG + ring(i) * PR, PR), PR)
        return remote(gr.at[k, r], gr_pieces.at[k, i - 1], gb_s.at[k, i - 1], gb_r.at[k, i - 1], seq=ring(i))

    def gather_pieces(k):
        for i in range(1, seqs):
            piece(k, i).wait_recv()

        def tile(j):
            r = at(j, TILE)
            v = gr[k, pl.ds(pl.multiple_of(pc * HG + ps * PR + j * TILE, TILE), TILE), :].astype(f32)
            for i in range(1, seqs):
                v = v + gr_pieces[k, i - 1, r, :].astype(f32)
            gr_sum[k, r, :] = v.astype(bf16)
            grads[k, pl.ds(pl.multiple_of(pc * HG + ps * PR + j * TILE, TILE), TILE), :] = v.astype(bf16)

        loop(PR // TILE, tile)

    def spread(k, i):
        r = pl.ds(pl.multiple_of(pc * HG + ps * PR, PR), PR)
        return remote(gr_sum.at[k], grads.at[k, r], gc_s.at[k, i - 1], gc_r.at[k, i - 1], seq=ring(i))

    def hand(k, i):
        q = lax.rem(ps + seqs - i, seqs)
        r = pl.ds(pl.multiple_of(pc * HG + q * PR, PR), PR)
        src = gr_sum.at[k] if i == 0 else grads.at[k, r]
        return remote(src, grads.at[k, r], gd_s.at[k, i], gd_r.at[k, i], sample=other)

    def send_out(k):
        gather_pieces(k)
        for i in range(1, seqs):
            spread(k, i).start()
        hand(k, 0).start()

    def hand_on(k):
        for i in range(1, seqs):
            q = lax.rem(ps + seqs - i, seqs)
            r = pl.ds(pl.multiple_of(pc * HG + q * PR, PR), PR)
            remote(gr_sum.at[k], grads.at[k, r], gc_s.at[k, i - 1], gc_r.at[k, i - 1], seq=ring(i)).wait_recv()
            hand(k, i).start()

    def result(k):
        return pltpu.make_async_copy(grads.at[k], grads_out.at[k], out_sem.at[k])

    def complete(k):
        for i in range(seqs):
            q = lax.rem(ps + seqs - i, seqs)
            r = pl.ds(pl.multiple_of(other * HG + q * PR, PR), PR)
            remote(gr_sum.at[k], grads.at[k, r], gd_s.at[k, i], gd_r.at[k, i], sample=other).wait()
        result(k).start()

    def send_pieces(k):
        settle(k)
        for i in range(1, seqs):
            piece(k, i).start()

    send_pieces(0)
    send_pieces(1)
    fold1.step(4)
    for s in range(S):
        relays2[s].gather(chained, e)
        off[...] = jnp.zeros_like(off)

        def state_back(k):
            kk = NC - 1 - k
            c = s * NC + kk
            here = at(c, Q)
            run = cum[here, :]
            last = run[Q - 1 : Q, :]
            ds = later[c] + row_of(jnp.exp(off[0:1, :]), e[...]) * chained[s]
            off[...] += jnp.broadcast_to(last, (8, Q))
            upper = iota((Q, Q), 1) >= 64
            causal = iota((Q, Q), 0) >= iota((Q, Q), 1)
            b, r = act[here, C : C + Q], act[here, C + Q :]
            scores = mm(r, b, NT)
            dsc = jnp.zeros((Q, Q), f32)
            for p in range(C // Q):
                lanes = slice(p * Q, (p + 1) * Q)
                xp = act[here, lanes]
                dyp = dy[here, lanes].astype(bf16)
                dyl = (dy[here, lanes] - dyp.astype(f32)).astype(bf16)
                dx = jnp.zeros((Q, Q), f32)
                for o in range(2):
                    keep = upper == bool(o)
                    dym = jnp.where(keep, dyp, jnp.zeros_like(dyp))
                    dyn = jnp.where(keep, dyl, jnp.zeros_like(dyl))
                    w = weights_of(2 * p + o, here, causal)
                    dsc = dsc + (mm(dym, xp, NT) + mm(dyn, xp, NT)) * w
                    dx = dx + mm((scores * w).astype(bf16), dym, TN)
                work[0, :, lanes] = dx
            d = dt[here, :]
            work[2] = mm2(jnp.exp(last - run) * d, e[...])
            work[1] = work[2] * mm2(b, ds)
            d_read = mm2(dsc, b) + mm3(spread_dy(c), entry[c], NT)
            d_in = mm2(dsc, r, TN) + mm3(act[here, 0:C].astype(f32) * work[2], ds, NT)
            slope[here, C : C + Q] = d_in * slope[here, C : C + Q]
            slope[here, C + Q :] = d_read * slope[here, C + Q :]

            def tile(i):
                rows = at(c * (Q // TILE) + i, TILE)
                near = at(i, TILE)
                x = act[rows, 0:C].astype(f32)
                g = dy[rows, :]
                a, o = work[0, near, :], work[1, near, :]
                work[3, near, :] = g.astype(bf16).astype(f32) * ys[rows, :] - x * a
                work[4, near, :] = x * o
                both = a + o
                work[5, near, :] = x * both
                slope[rows, 0:C] = (both + sk[...] * g) * slope[rows, 0:C]

            loop(Q // TILE, tile, 4)
            ha = mm2(work[3], e[...], NT)
            hb = mm2(work[4], e[...], NT)
            hc = mm2(work[5], e[...], NT)
            crossing = mm2(fold8(entry[c] * ds), e[...], NT)
            crossing = jnp.sum(crossing, axis=0, keepdims=True) * jnp.exp(last)
            dlog = (
                mm2(triangle(lambda i, j: i <= j).astype(bf16), ha)
                + mm2(triangle(lambda i, j: i > j).astype(bf16), hb)
                + crossing
            )
            g = sg[here, :]
            ratio = jnp.where(d > 1e-30, g / jnp.maximum(d, 1e-30), 1.0)
            rate = hp[1:2, :]
            draw = rate * dlog * g + hc * ratio
            dcs[here, 2 * Q :] = draw.astype(bf16)
            hsums[0:8, :] += fold8(draw)
            hsums[8:16, :] += fold8(rate * dlog * d)
            fold1.step((5 if s == 0 else 11) + k)

        loop(NC, state_back)
        edge8[s] = slope[s * L : s * L + 8, :]

        @pl.when(ps > 0)
        def _():
            next_rows(s).start()

        def conv_back(r, last):
            for lo in range(0, W, 256):
                lanes = slice(lo, lo + 256)
                if last:
                    w = jnp.concatenate([slope[(s + 1) * L - TILE : (s + 1) * L, lanes], nx[s, :, lanes]], axis=0)
                else:
                    w = slope[pl.ds(pl.multiple_of(s * L + r * TILE, TILE), TILE + 8), lanes]
                u = pad[s, pl.ds(pl.multiple_of(r * TILE, TILE), TILE + HALO), lanes].astype(f32)
                d = w[0:TILE]
                v = cw[3:4, lanes] * d
                for k in range(3):
                    v = v + cw[k : k + 1, lanes] * w[3 - k : 3 - k + TILE]
                rows = at(r + s * LT, TILE)
                if lo < C:
                    gate[rows, lanes] = v.astype(bf16)
                else:
                    dcs[rows, lo - C : lo - C + 256] = v.astype(bf16)
                for k in range(4):
                    acc[8 * k : 8 * k + 8, lanes] += fold8(d * u[13 + k : 13 + k + TILE])
                acc[32:40, lanes] += fold8(d)

        loop(LT - 1, lambda r: conv_back(r, False))
        fold1.step(9 if s == 0 else 15)
        if s > 0:
            fold1.step(16)
            fold2.step(0)

        @pl.when(ps < seqs - 1)
        def _():
            next_rows(s).wait_recv()

        conv_back(LT - 1, True)
        if s > 0:
            fold1.step(17)
            fold2.step(1)

        def into(k):
            i = s * (L // 256) + k
            rows = at(i, 256)
            v = mm(dg[rows, :], wg[...], NT) + mm(gate[rows, :], wv[...], NT) + mm(dcs[rows, :], wst[...])
            part2[rows, :] = v.astype(bf16)
            nsums[...] += fold8(v * xb[rows, :].astype(f32) * inv[rows, 0:1])

        loop(L // 256, into)
        if s == 0:
            fold2.begin(0, tiles // S)
            fold1.step(10)
            send_out(0)

    for k in range(5):
        row = jnp.sum(acc[8 * k : 8 * k + 8, :], axis=0, keepdims=True)
        small[k : k + 1, :] = row[:, 0:C]
        smallz[k : k + 1, 0 : 2 * Q] = row[:, C:]
        smallz[k : k + 1, 2 * Q :] = jnp.zeros((1, C - 2 * Q), f32)
    ngrad = jnp.sum(nsums[...], axis=0, keepdims=True)
    for j in range(D // C):
        smallz[5 + j : 6 + j, :] = ngrad[:, j * C : (j + 1) * C]
    smallz[7:8, :] = jnp.zeros((1, C), f32)

    def to_line(i):
        return remote(smallz, smallz_in.at[i - 1], m1_s.at[i - 1], m1_r.at[i - 1], head=line(i))

    for i in range(1, lines):
        to_line(i).start()
    held = 4
    fold2.begin(tiles // S, tiles - tiles // S - held)
    fold2.step(2)
    fold1.step(18)
    fold1.step(19)

    rest = fold2.last(13, 6)
    for k in range(D // Q):
        t = mm(nt[k * Q : (k + 1) * Q, :], dcs[...])
        for j in range(2):
            turned = t[:, j * Q : (j + 1) * Q].T
            for g in range(own // 8):
                for h in range(lines):
                    later[j * DC + k * Q // C, 8 * (g * lines + h) : 8 * (g * lines + h) + 8, k * Q % C : k * Q % C + Q] = (
                        turned[h * own + 8 * g : h * own + 8 * g + 8]
                    )
        row = 8 + 8 * (k * Q // C)
        small[row : row + 8, k * Q % C : k * Q % C + Q] = t[:, 2 * Q :].T[0:8]

    SR = Q // seqs
    keep_state = at(pc, DC)

    def state_pair():
        return remote(later.at[at(other, DC)], sg_in, sa_s, sa_r, sample=other)

    state_pair().start()
    small[5:6, :] = jnp.sum(sums[0:8, :], axis=0, keepdims=True)
    small[6:7, :] = jnp.sum(sums[8:16, :], axis=0, keepdims=True)
    small[7:8, :] = jnp.zeros((1, C), f32)
    small[7:8, 0:Q] = jnp.sum(hsums[0:8, :], axis=0, keepdims=True)
    small[7:8, Q : 2 * Q] = jnp.sum(hsums[8:16, :], axis=0, keepdims=True)
    fold2.step(3)
    def outer3(i):
        gr[2, at(i, 512), :] = mm(nt[at(i, 512), :], gate[...]).astype(bf16)

    loop(D // 512, outer3)
    pair(2).start()
    fold2.two(4)
    fold2.take(0)
    fold2.closely(4)
    state_pair().wait_recv()
    later[keep_state] = later[keep_state] + sg_in[...]

    def state_piece(i):
        return remote(later.at[keep_state, at(ring(i), SR)], sg_pieces.at[i - 1], sb_s.at[i - 1], sb_r.at[i - 1], seq=ring(i))

    for i in range(1, seqs):
        state_piece(i).start()
    fold2.closely(5)
    send_pieces(2)
    fold2.closely(6)
    hand_on(0)
    fold2.closely(7)
    fold2.closely(8)
    for i in range(1, seqs):
        state_piece(i).wait_recv()
    v = later[keep_state, at(ps, SR), :]
    for i in range(1, seqs):
        v = v + sg_pieces[i - 1]
    sg_sum[...] = v
    blocks = SR // 8

    def block_of(h):
        return lax.rem(h + lines * blocks - lax.rem(ps * blocks, lines), lines)

    for k in range(blocks):
        sg_wire[k] = v[:, 8 * k : 8 * k + 8, :].astype(bf16)
    owns = block_of(ph) < blocks

    def to_owner(i):
        return remote(sg_wire.at[lax.rem(block_of(line(i)), blocks)], sg_line.at[i - 1], sz_s.at[i - 1], sz_r.at[i - 1], head=line(i))

    for i in range(1, lines):

        @pl.when(block_of(line(i)) < blocks)
        def _():
            to_owner(i).start()

    fold2.begin(tiles - held, held)
    fold2.closely(9)
    send_out(1)
    fold2.closely(10)
    total = smallz[...]
    for i in range(1, lines):
        to_line(i).wait_recv()
        total = total + smallz_in[i - 1]
    small[24:32, :] = total

    def to_core():
        return remote(small, small_two.at[0], m2_s.at[seqs - 1], m2_r.at[seqs - 1], sample=other)

    def to_peer(i):
        return remote(small_two.at[1], small_in.at[i - 1], m2_s.at[i - 1], m2_r.at[i - 1], seq=ring(i))

    to_core().start()
    fold2.closely(11)
    send_out(2)
    fold2.closely(12)
    to_core().wait_recv()
    small_two[1] = small[...] + small_two[0]
    for i in range(1, seqs):
        to_peer(i).start()
    fold2.closely(13)
    span = own // 8

    def place_row(g, core):
        return pl.ds(pl.multiple_of(core * own + g * 8, 8), 8)

    my_row = lax.div(ps * blocks, lines)

    def state_out_to(i):
        return remote(sg_done, state_out.at[:, place_row(my_row, pc)], sc_s.at[i - 1], sc_r.at[i - 1], seq=ring(i))

    def holder(g):
        return lax.div(g * lines + ph, blocks)

    def state_hand(g, src):
        return remote(src, state_out.at[:, place_row(g, pc)], sd_s.at[g], sd_r.at[g], sample=other)

    @pl.when(owns)
    def _():
        t = sg_sum[:, pl.ds(pl.multiple_of(8 * block_of(ph), 8), 8), :]
        for i in range(1, lines):
            to_owner(i).wait_recv()
            t = t + sg_line[i - 1].astype(f32)
        sg_done[...] = t
        state_out[:, place_row(my_row, pc), :] = t
        for i in range(1, seqs):
            state_out_to(i).start()

    for move, i in rest[0]:
        move(i)
    hand_on(1)
    complete(0)
    for move, i in rest[1]:
        move(i)
    for move, i in rest[2]:
        move(i)
    hand_on(2)
    complete(1)
    for move, i in rest[3]:
        move(i)
    total = small_two[1]
    for i in range(1, seqs):
        to_peer(i).wait_recv()
        total = total + small_in[i - 1]
    small_out[...] = total
    small_copy = pltpu.make_async_copy(small_out, small_result, out_sem.at[3])
    small_copy.start()
    for move, i in rest[4]:
        move(i)
    for move, i in rest[5]:
        move(i)
    for g in range(span):

        @pl.when(holder(g) == ps)
        def _():
            state_hand(g, sg_done).start()

        for i in range(1, seqs):

            @pl.when(ring(seqs - i) == holder(g))
            def _():
                remote(
                    sg_done, state_out.at[:, place_row(g, pc)], sc_s.at[i - 1], sc_r.at[i - 1], seq=ring(i)
                ).wait_recv()
                state_hand(g, state_out.at[:, place_row(g, pc)]).start()

    for g in range(span):
        remote(sg_done, state_out.at[:, place_row(g, other)], sd_s.at[g], sd_r.at[g], sample=other).wait()
    state_copy = pltpu.make_async_copy(state_out, state_result, out_sem.at[4])
    state_copy.start()
    complete(2)
    fold1.end()
    fold2.end()
    for r in relays2:
        r.finish()
    for i in range(1, lines):
        for c in weights(i, ph):
            c.wait_send()
        for s in range(S):
            stat(s, i).wait_send()
        to_line(i).wait_send()

        @pl.when(block_of(line(i)) < blocks)
        def _():
            to_owner(i).wait_send()

    @pl.when(ps < seqs - 1)
    def _():
        for s in range(S):
            halo(s).wait_send()

    @pl.when(ps > 0)
    def _():
        for s in range(S):
            next_rows(s).wait_send()

    for k in range(3):
        pair(k).wait_send()
        for i in range(1, seqs):
            piece(k, i).wait_send()
            spread(k, i).wait_send()
        result(k).wait()
    small_copy.wait()
    state_copy.wait()
    state_pair().wait_send()
    share().wait_send()
    for i in range(1, seqs):
        state_piece(i).wait_send()

        @pl.when(owns)
        def _():
            state_out_to(i).wait_send()

    to_core().wait_send()
    for i in range(1, seqs):
        to_peer(i).wait_send()


def finish(
    lines, x, cot, gain, dn, outs, g_out, g_gate, g_value, state, small,
    block_out, input_grad, gate_grad, value_grad, out_grad,
    state_grad, norm_grad, step_grad, cv, cs, cvb, csb, sbias, dlog, skip, gated_gain,
):
    rows, width = x.shape
    for j in range(rows // 16):
        r = slice(j * 16, (j + 1) * 16)
        v = x[r, :].astype(f32)
        block_out[r, :] = (v + outs[r, :].astype(f32)).astype(bf16)
        s = dn[r, :].astype(f32) * gain[...]
        i1 = lax.rsqrt(jnp.mean(v * v, axis=1, keepdims=True) + EPS)
        m = jnp.mean(s * v, axis=1, keepdims=True)
        input_grad[r, :] = cot[r, :].astype(f32) + i1 * s - v * (i1 * i1 * i1 * m)
    half = g_gate.shape[1]
    for j in range(width // half):
        out_grad[:, j * half : (j + 1) * half] = g_out[j].astype(f32)
    gate_grad[...] = g_gate[...].astype(f32)
    value_grad[...] = g_value[...].astype(f32)

    @pl.when(pl.program_id(0) == 0)
    def _():
        heads, own = sbias.shape[1], csb.shape[1]
        for j in range(width // half):
            lanes = slice(j * half, (j + 1) * half)
            state_grad[:, lanes] = state[j]
            norm_grad[:, lanes] = small[29 + j : 30 + j, :]
            step_grad[:, lanes] = small[8 + 8 * j : 16 + 8 * j, :]
        cv[...] = small[0:4, :]
        cvb[...] = small[4:5, :]
        gated_gain[...] = small[5:6, :]
        e = lane_heads(half // 64, half)
        skip[...] = mm(jnp.broadcast_to(small[6:7, :], (8, half)), e.astype(f32), NT, HI)[0:1, 0:heads]
        sbias[...] = small[7:8, 0:heads]
        dlog[...] = small[7:8, Q : Q + heads]
        for h in range(lines):

            @pl.when(lax.axis_index("head") == h)
            def _():
                for j in range(2):
                    lanes = slice(j * Q + h * own, j * Q + (h + 1) * own)
                    cs[:, j, :] = small[24:28, lanes]
                    csb[j : j + 1, :] = small[28:29, lanes]


def per_device(
    block_in, out_cotangent, norm_gain, gate_proj, value_proj, state_proj, step_proj,
    conv_value, conv_state, conv_value_bias, conv_state_bias, step_bias, decay_log,
    skip_gain, gated_gain, out_proj,
):
    S, L, D = block_in.shape
    T = S * L
    heads = step_proj.shape[1]
    C = gate_proj.shape[1]
    own = state_proj.shape[2]
    W = C + 2 * Q
    NCH = T // Q
    seqs, lines = lax.axis_size("seq"), lax.axis_size("head")
    tiles = 32
    H = D // 2
    PR = H // seqs
    SR = Q // seqs
    x = block_in.reshape(T, D)
    cot = out_cotangent.reshape(T, D)
    spt = state_proj.transpose(0, 2, 1).reshape(2 * own, D)
    gain = norm_gain[None]
    vm = pl.BlockSpec(memory_space=pltpu.VMEM)
    hbm = pl.BlockSpec(memory_space=pl.ANY)
    dma = pltpu.SemaphoreType.DMA
    n1, l1 = seqs - 1, lines - 1
    V = pltpu.VMEM
    scratch = [
        V((T, D), bf16), V((T, D), bf16), V((D, C), bf16), V((D, C), bf16), V((3 * Q, D), bf16),
        V((C, D), bf16), V((8, Q), f32), V((lines, 8, Q), f32), V((8, W), f32), V((8, Q), f32), V((1, C), f32),
        V((S * HALO, D), bf16),
        V((D, T), bf16), V((T, Q), f32), V((T, C), bf16), V((S, HALO + L, W), bf16), V((T, W), f32),
        V((T, W), bf16), V((T, Q), f32), V((T, Q), f32), V((T, Q), f32), V((8, T), f32), V((8, T), f32),
        V((NCH, Q, C), f32), V((T, C), f32), V((T, C), f32), V((T, C), bf16), V((T, C), bf16),
        V((NCH, Q, C), f32),
        V((T, 3 * Q), bf16), V((Q, C), bf16), V((Q, C), f32), V((6, Q, C), f32),
        V((8, Q), f32), V((Q, Q), f32), V((4, Q, Q), f32), V((8, T), f32), V((l1, 8, T), f32),
        V((S, Q, C), bf16), V((S, 8, Q), f32), V((seqs, S, Q, C), bf16), V((seqs, S, 8, Q), f32),
        V((S, Q, C), f32),
        V((T, D), bf16), V((T, D), bf16), V((T, D), bf16), V((T, D), bf16), V((T, D), bf16), V((T, D), bf16),
        V((3, D, C), bf16), V((D // C, 2 * own, C), f32), V((32, C), f32), V((3, D, C), bf16), V((3, H, C), bf16), V((3, n1, PR, C), bf16), V((3, PR, C), bf16),
        V((D // C, Q, C), f32), V((n1, D // C, SR, C), f32), V((l1, D // C, 8, C), bf16),
        V((SR // 8, D // C, 8, C), bf16), V((D // C, SR, C), f32), V((D // C, 8, C), f32),
        V((40, W), f32), V((16, Q), f32), V((16, C), f32), V((8, D), f32), V((8, C), f32),
        V((l1, 8, C), f32), V((32, C), f32), V((2, 32, C), f32), V((n1, 32, C), f32), V((S, 8, W), f32), V((S, 8, W), f32),
        dma((S + 5,)), dma((2, S)), dma((2, lines)), dma((2, lines)), dma((2, 2, S, n1)), dma((2, 2, S, n1)),
        dma((S, l1)), dma((S, l1)), dma((S,)), dma((S,)),
        dma((2, tiles)), dma((3,)), dma((2, tiles)), dma((3,)), dma((3,)), dma((3,)), dma((3, n1)), dma((3, n1)),
        dma((3, n1)), dma((3, n1)), dma((3, seqs)), dma((3, seqs)),
        dma((5,)), dma, dma, dma((n1,)), dma((n1,)), dma((l1,)), dma((l1,)), dma((n1,)), dma((n1,)),
        dma((own // 8,)), dma((own // 8,)), dma((l1,)), dma((l1,)), dma((seqs,)), dma((seqs,)),
    ]
    outs, dnorm, grads, state_out, small = pl.pallas_call(
        functools.partial(block, (S, L, seqs, lines, tiles)),
        out_shape=[
            jax.ShapeDtypeStruct((T, D), bf16), jax.ShapeDtypeStruct((T, D), bf16),
            jax.ShapeDtypeStruct((3, D, C), bf16), jax.ShapeDtypeStruct((D // C, 2 * own, C), f32),
            jax.ShapeDtypeStruct((32, C), f32),
        ],
        in_specs=[hbm, hbm, vm, hbm, hbm, hbm, vm, hbm] + [vm] * 8,
        out_specs=[hbm] * 5,
        scratch_shapes=scratch,
        name="block",
        compiler_params=pltpu.CompilerParams(
            collective_id=0, has_side_effects=True, vmem_limit_bytes=67043328
        ),
    )(
        x, cot, gain, gate_proj, value_proj, spt, step_proj.T, out_proj, conv_state, conv_state_bias,
        conv_value, conv_value_bias[None], step_bias[None], decay_log[None], skip_gain[None], gated_gain[None],
    )
    steps = 2

    def whole(*shape):
        return pl.BlockSpec(shape, lambda i: (0,) * len(shape))

    by_rows = pl.BlockSpec((T // steps, D), lambda i: (i, 0))
    by_grad = pl.BlockSpec((D // steps, C), lambda i: (i, 0))
    shape = jax.ShapeDtypeStruct
    (block_out, input_grad, gate_grad, value_grad, out_grad, state_grad, norm_grad, step_grad, cv, cs, cvb, csb,
     sbias, dlog, skip, gated) = pl.pallas_call(
        functools.partial(finish, lines),
        grid=(steps,),
        out_shape=[
            shape((T, D), bf16), shape((T, D), f32), shape((D, C), f32), shape((D, C), f32), shape((C, D), f32),
            shape((2 * own, D), f32), shape((1, D), f32), shape((heads, D), f32), shape((4, C), f32),
            shape((4, 2, own), f32), shape((1, C), f32), shape((2, own), f32), shape((1, heads), f32),
            shape((1, heads), f32), shape((1, heads), f32), shape((1, C), f32),
        ],
        in_specs=[
            by_rows, by_rows, whole(1, D), by_rows, by_rows,
            pl.BlockSpec((None, D // C, C // steps, C), lambda i: (0, 0, i, 0)),
            pl.BlockSpec((None, D // steps, C), lambda i: (1, i, 0)),
            pl.BlockSpec((None, D // steps, C), lambda i: (2, i, 0)),
            whole(D // C, 2 * own, C), whole(32, C),
        ],
        out_specs=[
            by_rows, by_rows, by_grad, by_grad, pl.BlockSpec((C // steps, D), lambda i: (i, 0)),
            whole(2 * own, D), whole(1, D), whole(heads, D), whole(4, C), whole(4, 2, own), whole(1, C),
            whole(2, own), whole(1, heads), whole(1, heads), whole(1, heads), whole(1, C),
        ],
        name="finish",
        compiler_params=pltpu.CompilerParams(vmem_limit_bytes=60 * 2**20),
    )(x, cot, gain, dnorm, outs, grads.reshape(3, D // C, C, C), grads, grads, state_out, small)
    return (
        block_out.reshape(S, L, D), input_grad.reshape(S, L, D), norm_grad[0], gate_grad, value_grad,
        state_grad.reshape(2, own, D).transpose(0, 2, 1), step_grad.T, cv, cs, cvb[0], csb, sbias[0], dlog[0],
        skip[0], gated[0], out_grad,
    )


def solution(mesh):
    tokens = P("sample", "seq", None)
    params = (
        P(), P(None, "head"), P(None, "head"), P(None, None, "head"), P(None, "head"),
        P(None, "head"), P(None, None, "head"), P("head"), P(None, "head"), P("head"),
        P("head"), P("head"), P("head"), P("head", None),
    )
    return jax.shard_map(
        per_device,
        mesh=mesh,
        in_specs=(tokens, tokens) + params,
        out_specs=(tokens, tokens) + params,
        check_vma=False,
    )
```

```python
import functools

import jax
import jax.numpy as jnp
from jax import lax
from jax.experimental import pallas as pl
from jax.experimental.pallas import tpu as pltpu
from jax.sharding import PartitionSpec as P

f32, bf16 = jnp.float32, jnp.bfloat16
HI = lax.Precision.HIGHEST
MESH = pl.DeviceIdType.MESH
Q = 128
TILE = 32
HALO = 16
EPS = 1e-05
NN, NT, TN = ((1,), (0,)), ((1,), (1,)), ((0,), (0,))


def mm(a, b, dims=NN, precision=None):
    return lax.dot_general(
        a, b, (dims, ((), ())), preferred_element_type=f32, precision=precision
    )


def halves(v):
    high = v.astype(bf16)
    return high, (v - high.astype(f32)).astype(bf16)


def mm2(a, b, dims=NN):
    if a.dtype == bf16:
        high, low = halves(b)
        return mm(a, high, dims) + mm(a, low, dims)
    high, low = halves(a)
    return mm(high, b, dims) + mm(low, b, dims)


def mm3(a, b, dims=NN):
    ah, al = halves(a)
    bh, bl = halves(b)
    return mm(ah, bh, dims) + (mm(ah, bl, dims) + mm(al, bh, dims))


def at(i, n):
    return pl.ds(i * n if isinstance(i, int) else pl.multiple_of(i * n, n), n)


def loop(count, body, each=1):
    def step(i, carry):
        for j in range(each):
            body(i * each + j)
        return carry

    if count == each:
        for i in range(count):
            body(i)
    else:
        lax.fori_loop(0, count // each, step, 0)


def iota(shape, axis):
    return lax.broadcasted_iota(jnp.int32, shape, axis)


def lane_heads(heads, width):
    shift = (width // heads).bit_length() - 1
    return ((iota((Q, width), 1) >> shift) == iota((Q, width), 0)).astype(f32).astype(bf16)


def triangle(keep):
    return jnp.where(keep(iota((Q, Q), 0), iota((Q, Q), 1)), 1.0, 0.0)


def fold8(v):
    return jnp.sum(v.reshape(v.shape[0] // 8, 8, v.shape[1]), axis=0)


def row_of(v, e):
    return mm2(jnp.broadcast_to(v, (8, Q)), e)[0:1]


def sigmoid(v):
    return 0.5 * jnp.tanh(0.5 * v) + 0.5


def normalize(v, gain):
    inv = lax.rsqrt(jnp.mean(v * v, axis=1, keepdims=True) + EPS)
    return (v * inv * gain).astype(bf16), inv


def remote(src, dst, send, recv, **place):
    return pltpu.make_async_remote_copy(
        src_ref=src, dst_ref=dst, send_sem=send, recv_sem=recv, device_id=place, device_id_type=MESH
    )


class Fold:
    def __init__(self, part, near, far, result, sems, tiles):
        self.part, self.near, self.far, self.result, self.tiles = part, near, far, result, tiles
        (self.b, self.d), (self.a, self.c, self.e) = sems
        self.rows = part.shape[0] // tiles
        place = lax.axis_index("head")
        self.inner = (place == 1) | (place == 2)
        self.beside = jnp.where(place < 2, 1 - place, 5 - place)
        self.across = 3 - place

    def outward(self, i, src):
        r = at(i, self.rows)
        return remote(src.at[r], self.near.at[r], self.a, self.b.at[i], head=self.beside)

    def middle(self, i):
        r = at(i, self.rows)
        return remote(self.part.at[r], self.far.at[r], self.c, self.d.at[i], head=self.across)

    def store(self, i):
        r = at(i, self.rows)
        return pltpu.make_async_copy(self.near.at[r], self.result.at[r], self.e)

    def take(self, i):
        @pl.when(jnp.logical_not(self.inner))
        def _():
            self.outward(i, self.near).wait_recv()
            self.store(i).start()

    def begin(self, first, count):
        @pl.when(jnp.logical_not(self.inner))
        def _():
            loop(count, lambda i: self.outward(first + i, self.part).start())

    def add(self, dst, u, v, i):
        def tile(j):
            r = at(i * (self.rows // TILE) + j, TILE)
            dst[r, :] = (u[r, :].astype(f32) + v[r, :].astype(f32)).astype(bf16)

        loop(self.rows // TILE, tile)

    def one(self, i):
        @pl.when(self.inner)
        def _():
            self.outward(i, self.near).wait_recv()
            self.add(self.part, self.part, self.near, i)
            self.middle(i).start()

    def two(self, i):
        @pl.when(self.inner)
        def _():
            self.middle(i).wait_recv()
            self.add(self.near, self.part, self.far, i)
            self.outward(i, self.near).start()
            self.store(i).start()

    def step(self, j):
        for ago, move in ((0, self.one), (4, self.two), (8, self.take)):
            if isinstance(j, int):
                first, end = max(2 * j - ago, 0), min(2 * j - ago + 2, self.tiles)
                if first < end:
                    loop(end - first, lambda q: move(first + q))
            else:
                for q in range(2):
                    i = 2 * j - ago + q

                    @pl.when((i >= 0) & (i < self.tiles))
                    def _():
                        move(i)

    def closely(self, j):
        def tile(q):
            self.one(2 * j + q)
            self.two(2 * j - 3 + q)
            if 2 * j >= 7:
                self.take(2 * j - 7 + q)

        loop(2, tile)

    def last(self, j, parts):
        o, t, k = 2 * j + 2, 2 * j - 1, 2 * j - 5
        moves = []
        while k < self.tiles:
            if o < self.tiles:
                moves.append((self.one, o))
                o += 1
            for unused in range(2):
                if t < self.tiles and (t < o - 2 or o == self.tiles):
                    moves.append((self.two, t))
                    t += 1
            for unused in range(2):
                if k < self.tiles and (k < t - 3 or t == self.tiles):
                    moves.append((self.take, k))
                    k += 1
        size = -(-len(moves) // parts)
        return [moves[i : i + size] for i in range(0, len(moves), size)]

    def end(self):
        pltpu.make_async_copy(self.near, self.result, self.e).wait()
        remote(self.part, self.near, self.a, self.b.at[0], head=self.beside).wait_send()

        @pl.when(self.inner)
        def _():
            remote(self.part, self.far, self.c, self.d.at[0], head=self.across).wait_send()


def fold_sems(tiles, streams):
    return [tiles.at[j] for j in range(2)], [streams.at[j] for j in range(3)]


class Relay:
    def __init__(self, seq, blocks, slots, sems, count, way):
        self.seq, self.blocks, self.slots, self.sems = seq, blocks, slots, sems
        self.count, self.way = count, way
        self.place = lax.axis_index("seq")

    def copies(self, d, source):
        to = self.place + self.way * d
        return [
            remote(
                b.at[self.seq], s.at[source, self.seq], self.sems.at[0, j, self.seq, d - 1],
                self.sems.at[1, j, self.seq, d - 1], seq=to,
            )
            for j, (b, s) in enumerate(zip(self.blocks, self.slots))
        ]

    def reaches(self, d):
        return self.place + d < self.count if self.way > 0 else self.place >= d

    def hears(self, d):
        return self.place >= d if self.way > 0 else self.place + d < self.count

    def start(self):
        for d in range(1, self.count):

            @pl.when(self.reaches(d))
            def _():
                for c in self.copies(d, self.place):
                    c.start()

    def gather(self, state, e):
        q = self.seq
        state[q] = jnp.zeros(state.shape[1:], f32)
        for d in range(self.count - 1, 0, -1):

            @pl.when(self.hears(d))
            def _():
                source = self.place - self.way * d
                for c in self.copies(d, source):
                    c.wait_recv()
                decay = mm2(jnp.exp(self.slots[1][source, q]), e[...])[0:1]
                state[q] = state[q] * decay + self.slots[0][source, q].astype(f32)

    def finish(self):
        for d in range(1, self.count):

            @pl.when(self.reaches(d))
            def _():
                for c in self.copies(d, self.place):
                    c.wait_send()


def block(
    dims,
    x_in, cot_in, gain, wg_in, wv_in, spt, stp, wo_in, cs, csb, cv, cvb, sbias, dlog_in, skip, gg,
    outs, dnorm, grads_out, state_result, small_result,
    xb, cot, wg, wv, wst, wo, tapb, taps, cw, hp, sk, xh,
    nt, inv, gate, pad, slope, act, dt, sg, cum, cum_t, dt_t, entry, ys, dy, gn, dg, later,
    dcs, e, st, work, off, tt, stats, stats_t, stats_in,
    fin, tot, slots, slots_t, chained,
    part1, near1, far1, part2, near2, far2, grads, state_out, small_out,
    gr, gr_in, gr_pieces, gr_sum, sg_in, sg_pieces, sg_line, sg_wire, sg_sum, sg_done,
    acc, hsums, sums, nsums, smallz, smallz_in, small, small_two, small_in, nx, edge8,
    load, halo_sem, wt_s, wt_r, f_sem, b_sem, st_s, st_r, nx_s, nx_r,
    z1, y1, z2, y2, ga_s, ga_r, gb_s, gb_r, gc_s, gc_r, gd_s, gd_r,
    out_sem, sa_s, sa_r, sb_s, sb_r, sz_s, sz_r, sc_s, sc_r, sd_s, sd_r, m1_s, m1_r, m2_s, m2_r,
):
    S, L, seqs, lines, tiles = dims
    T, D = xb.shape
    C = wg.shape[1]
    W = C + 2 * Q
    NC = L // Q
    own = spt.shape[0] // 2
    full = C * lines
    ps, pc, ph = lax.axis_index("seq"), lax.axis_index("sample"), lax.axis_index("head")
    other = 1 - pc
    group = 2 * seqs
    DC = D // C
    mine = ps * 2 + pc
    nb = part1

    def peer(i):
        p = lax.rem(mine + i, group)
        return {"seq": p // 2, "sample": lax.rem(p, 2)}

    def line(i):
        return lax.rem(ph + i, lines)

    def ring(i):
        return lax.rem(ps + i, seqs)

    moves = [pltpu.make_async_copy(x_in.at[pl.ds(s * L, L)], xb.at[pl.ds(s * L, L)], load.at[s]) for s in range(S)]
    moves += [
        pltpu.make_async_copy(wg_in, wg, load.at[S]),
        pltpu.make_async_copy(wv_in, wv, load.at[S + 1]),
        pltpu.make_async_copy(
            spt.at[at(pc, own)], wst.at[pl.ds(pl.multiple_of(pc * Q + ph * own, own), own)], load.at[S + 2]
        ),
        pltpu.make_async_copy(wo_in, wo, load.at[S + 3]),
        pltpu.make_async_copy(cot_in, cot, load.at[S + 4]),
    ]
    for m in moves:
        m.start()
    barrier = pltpu.get_barrier_semaphore()
    for i in range(1, group):
        pl.semaphore_signal(barrier, inc=1, device_id=peer(i), device_id_type=MESH)
    for i in range(1, lines):
        pl.semaphore_signal(barrier, inc=1, device_id={"head": line(i)}, device_id_type=MESH)
    heads = stp.shape[0]
    tapb[...] = jnp.zeros_like(tapb)
    hp[...] = jnp.zeros_like(hp)
    for j in range(2):
        tapb[0:4, j * own : (j + 1) * own] = cs[:, j, :]
        tapb[4:5, j * own : (j + 1) * own] = csb[j : j + 1, :]
    taps[ph] = tapb[...]
    hp[0:1, 0:heads] = sbias[...]
    hp[1:2, 0:heads] = -jnp.exp(dlog_in[...])
    hp[2:3, 0:heads] = skip[...]
    wst[2 * Q :, :] = jnp.zeros((Q, D), bf16)
    wst[2 * Q : 2 * Q + heads, :] = stp[...]
    e[...] = lane_heads(C // 64, C)
    sk[...] = mm(hp[...], e[...].astype(f32), precision=HI)[2:3]

    def norm(s):
        moves[s].wait()

        def norm_rows(r):
            rows = at(s * (L // 16) + r, 16)
            v = xb[rows, :].astype(f32)
            i = lax.rsqrt(jnp.mean(v * v, axis=1, keepdims=True) + EPS)
            nb[rows, :] = (v * i * gain[...]).astype(bf16)
            inv[rows, :] = jnp.broadcast_to(i, (16, Q))

        loop(L // 16, norm_rows, 4)

    norm(0)
    pl.semaphore_wait(barrier, group - 1 + lines - 1)

    def halo(s):
        return remote(
            x_in.at[pl.ds(s * L + L - HALO, HALO)], xh.at[pl.ds(s * HALO, HALO)],
            halo_sem.at[0, s], halo_sem.at[1, s], seq=ps + 1,
        )

    @pl.when(ps < seqs - 1)
    def _():
        for s in range(S):
            halo(s).start()

    @pl.when(ps == 0)
    def _():
        xh[...] = jnp.zeros_like(xh)

    def weights(i, source):
        r = pl.ds(pl.multiple_of(pc * Q + source * own, own), own)
        parts = [(spt.at[at(pc, own)], wst.at[r]), (tapb, taps.at[source])]
        return [
            remote(a, b, wt_s.at[j, i - 1], wt_r.at[j, i - 1], head=line(i))
            for j, (a, b) in enumerate(parts)
        ]

    for i in range(1, lines):
        for c in weights(i, ph):
            c.start()

    for s in range(S):
        if s > 0:
            norm(s)
        else:
            moves[S].wait()
            moves[S + 1].wait()
        seq_rows = slice(s * L, (s + 1) * L)
        gate[seq_rows, :] = mm(nb[seq_rows, :], wg[...]).astype(bf16)
        pad[s, HALO:, 0:C] = mm(nb[seq_rows, :], wv[...]).astype(bf16)

    def conv(s, first, end):
        def conv_rows(r):
            for lo in range(first, end, 256):
                lanes = slice(lo, lo + 256)
                w = pad[s, pl.ds(pl.multiple_of(r * TILE, TILE), TILE + HALO), lanes].astype(f32)
                v = cw[4:5, lanes] + cw[0:1, lanes] * w[13 : 13 + TILE]
                for k in range(1, 4):
                    v = v + cw[k : k + 1, lanes] * w[13 + k : 13 + k + TILE]
                g = sigmoid(v)
                rows = at(r + s * (L // TILE), TILE)
                act[rows, lanes] = (v * g).astype(bf16)
                slope[rows, lanes] = g * (1.0 + v * (1.0 - g))

        loop(L // TILE, conv_rows, 2)

    cw[0:4, 0:C] = cv[...]
    cw[4:5, 0:C] = cvb[...]
    edges = []
    for s in range(S):

        @pl.when(ps > 0)
        def _():
            halo(s).wait_recv()

        edges.append(normalize(xh[s * HALO : (s + 1) * HALO, :].astype(f32), gain[...])[0])
        pad[s, 0:HALO, 0:C] = mm(edges[s], wv[...]).astype(bf16)
        conv(s, 0, C)
    moves[S + 3].wait()
    moves[S + 4].wait()
    for s in range(S):
        seq_rows = slice(s * L, (s + 1) * L)
        dy[seq_rows, :] = mm(cot[seq_rows, :], wo[...], NT)

    def share():
        r = at(pc, Q)
        return remote(wst.at[r], wst.at[r], wt_s.at[0, lines - 1], wt_r.at[0, lines - 1], sample=other)

    moves[S + 2].wait()
    for i in range(1, lines):
        for c in weights(i, line(lines - i)):
            c.wait_recv()
    share().start()
    for h in range(lines):
        for j in range(2):
            cw[:, C + j * Q + h * own : C + j * Q + (h + 1) * own] = taps[h, :, j * own : (j + 1) * own]
    r = at(other, Q)
    remote(wst.at[r], wst.at[r], wt_s.at[0, lines - 1], wt_r.at[0, lines - 1], sample=other).wait_recv()

    relays, relays2 = [], []
    for s in range(S):
        seq_rows = slice(s * L, (s + 1) * L)
        both = mm(nb[seq_rows, :], wst[...], NT)
        pad[s, HALO:, C:] = both[:, 0 : 2 * Q].astype(bf16)
        sg[seq_rows, :] = both[:, 2 * Q :]
        pad[s, 0:HALO, C:] = mm(edges[s], wst[0 : 2 * Q, :], NT).astype(bf16)
        conv(s, C, W)

        def steps(k):
            c = s * NC + k
            z = sg[at(c, Q), :] + hp[0:1, :]
            d = jax.nn.softplus(z)
            dt[at(c, Q), :] = d
            sg[at(c, Q), :] = sigmoid(z)
            step = d * hp[1:2, :]
            high, rest = halves(step)
            middle, low = halves(step - high.astype(f32))
            tri = triangle(lambda i, j: i >= j).astype(bf16)
            run = mm(tri, high) + (mm(tri, middle) + mm(tri, low))
            cum[at(c, Q), :] = run
            cum_t[:, at(c, Q)] = run.T[0:8]
            dt_t[:, at(c, Q)] = d.T[0:8]

        loop(NC, steps, 2)
        st[...] = jnp.zeros_like(st)
        tot[s] = jnp.zeros((8, Q), f32)

        def chunk(k):
            c = s * NC + k
            run = cum[at(c, Q), :]
            last = run[Q - 1 : Q, :]
            tail = mm2(jnp.exp(last - run) * dt[at(c, Q), :], e[...])
            xt = act[at(c, Q), 0:C].astype(f32) * tail
            entry[c] = st[...]
            st[...] = st[...] * row_of(jnp.exp(last), e[...]) + mm2(act[at(c, Q), C : C + Q], xt, TN)
            tot[s] += jnp.broadcast_to(last, (8, Q))

        loop(NC, chunk, NC)
        fin[s] = st[...].astype(bf16)
        relays.append(Relay(s, (fin, tot), (slots, slots_t), f_sem, seqs, 1))
        if s == 0:
            relays[s].start()

    def weights_of(h, here, causal):
        gap = cum[here, h : h + 1] - cum_t[h : h + 1, here]
        return jnp.exp(jnp.where(causal, gap, -1e30)) * dt_t[h : h + 1, here]

    def within(c):
        here = at(c, Q)
        scores = mm(act[here, C + Q :], act[here, C : C + Q], NT)
        causal = iota((Q, Q), 0) >= iota((Q, Q), 1)
        upper = iota((Q, Q), 1) >= 64
        for p in range(C // Q):
            xp = act[here, p * Q : (p + 1) * Q]
            y = jnp.zeros((Q, Q), f32)
            for o in range(2):
                m = (scores * weights_of(2 * p + o, here, causal)).astype(bf16)
                y = y + mm(m, jnp.where(upper == bool(o), xp, jnp.zeros_like(xp)))
            ys[here, p * Q : (p + 1) * Q] = y

    loop(NC, within)
    relays[1].start()

    def stat(s, i):
        part = pl.ds(s * L, L)
        return remote(
            stats_t.at[:, part], stats_in.at[i - 1, :, part], st_s.at[s, i - 1], st_r.at[s, i - 1], head=line(i)
        )

    stats_t[...] = jnp.zeros_like(stats_t)

    def cross(s):
        relays[s].gather(chained, e)
        off[...] = jnp.zeros_like(off)

        def across(k, lane=0):
            c = s * NC + k
            here = at(c, Q)
            si = entry[c] + row_of(jnp.exp(off[0:1, :]), e[...]) * chained[s]
            entry[c] = si
            run = cum[here, :]
            work[lane] = mm2(jnp.exp(run), e[...]) * mm2(act[here, C + Q :], si)
            off[...] += jnp.broadcast_to(run[Q - 1 : Q, :], (8, Q))

            def tile(r):
                rows = at(c * (Q // TILE) + r, TILE)
                y = ys[rows, :] + work[lane, at(r, TILE), :]
                ys[rows, :] = y
                m = y + sk[...] * act[rows, 0:C].astype(f32)
                g = gate[rows, :].astype(f32)
                gated = m * (g * sigmoid(g))
                a = gated * gated
                b = dy[rows, :] * gg[...] * gated
                stats[2 * lane, at(r, TILE), :] = sum(a[:, p * Q : (p + 1) * Q] for p in range(C // Q))
                stats[2 * lane + 1, at(r, TILE), :] = sum(b[:, p * Q : (p + 1) * Q] for p in range(C // Q))

            loop(Q // TILE, tile, 4)
            for j in range(2):
                stats_t[j : j + 1, here] = jnp.sum(stats[2 * lane + j].T, axis=0, keepdims=True)

        def pair_of(k):
            across(2 * k, 0)
            across(2 * k + 1, 1)

        loop(NC // 2, pair_of)
        for i in range(1, lines):
            stat(s, i).start()

    cross(0)
    loop(NC, lambda k: within(NC + k))
    sums[...] = jnp.zeros_like(sums)
    fold1 = Fold(part1, near1, far1, outs, fold_sems(z1, y1), tiles)
    fold2 = Fold(part2, near2, far2, dnorm, fold_sems(z2, y2), tiles)

    def spread_dy(c):
        return mm2(jnp.exp(cum[at(c, Q), :]), e[...]) * dy[at(c, Q), :]

    def gating(s):
        for i in range(1, lines):
            stat(s, i).wait_recv()

        def gate_back(k):
            c = s * NC + k
            here = at(c, Q)
            t = stats_t[:, here]
            for i in range(1, lines):
                t = t + stats_in[i - 1, :, here]
            t = t.T
            rms = lax.rsqrt(t[:, 0:1] / full + EPS)
            tt[:, 0:1] = rms
            tt[:, 1:2] = rms * rms * rms * (t[:, 1:2] / full)

            def tile(r):
                rows = at(c * (Q // TILE) + r, TILE)
                near = at(r, TILE)
                rm, co = tt[near, 0:1], tt[near, 1:2]
                x = act[rows, 0:C].astype(f32)
                m = ys[rows, :] + sk[...] * x
                g = gate[rows, :].astype(f32)
                sig = sigmoid(g)
                ga = g * sig
                gated = m * ga
                scaled_rows = gated * rm
                gn[rows, :] = (scaled_rows * gg[...]).astype(bf16)
                d = dy[rows, :]
                dgd = rm * (d * gg[...]) - gated * co
                dmix = dgd * ga
                dg[rows, :] = (dgd * m * (sig * (1.0 + g * (1.0 - sig)))).astype(bf16)
                dy[rows, :] = dmix
                sums[0:8, :] += fold8(d * scaled_rows)
                sums[8:16, :] += fold8(dmix * x)

            loop(Q // TILE, tile, 4)
            part1[here, :] = mm(gn[here, :], wo[...]).astype(bf16)
            few = tiles * Q // T
            if s == 0:

                @pl.when(k == 0)
                def _():
                    fold1.begin(0, few)

            else:
                fold1.begin(c * few, few)
        loop(NC, gate_back)

    def rewind(s):
        st[...] = jnp.zeros_like(st)

        def back(k):
            c = s * NC + NC - 1 - k
            last = cum[pl.ds(pl.multiple_of(c * Q + Q - 8, 8), 8), :][7:8]
            later[c] = st[...]
            st[...] = st[...] * row_of(jnp.exp(last), e[...]) + mm2(act[at(c, Q), C + Q :], spread_dy(c), TN)

        loop(NC, back, NC)
        fin[s] = st[...].astype(bf16)
        relays2.append(Relay(s, (fin, tot), (slots, slots_t), b_sem, seqs, -1))
        relays2[s].start()

    gating(0)
    cross(1)
    fold1.begin(tiles * Q // T, tiles // S - tiles * Q // T)
    for r in relays:
        r.finish()
    rewind(0)
    fold1.step(0)
    gating(1)
    rewind(1)
    fold1.step(1)

    HG = D // 2
    PR = HG // seqs

    def pair(k):
        return remote(gr.at[k, at(other, HG)], gr_in.at[k], ga_s.at[k], ga_r.at[k], sample=other)

    for i in range(D // C):
        gr[0, i * C : (i + 1) * C, :] = mm(gn[...], cot[:, i * C : (i + 1) * C], TN).astype(bf16)
    pair(0).start()

    def turn(i):
        rows = at(i, 256)
        nt[:, rows] = (xb[rows, :].astype(f32) * inv[rows, 0:1] * gain[...]).astype(bf16).T

    loop(T // 256, turn)
    fold1.step(2)

    def outer2(i):
        gr[1, at(i, 512), :] = mm(nt[at(i, 512), :], dg[...]).astype(bf16)

    loop(D // 512, outer2)
    pair(1).start()
    fold1.step(3)

    hsums[...] = jnp.zeros_like(hsums)
    acc[...] = jnp.zeros_like(acc)
    nsums[...] = jnp.zeros_like(nsums)
    LT = L // TILE

    def next_rows(s):
        return remote(edge8.at[s], nx.at[s], nx_s.at[s], nx_r.at[s], seq=ps - 1)

    @pl.when(ps == seqs - 1)
    def _():
        nx[...] = jnp.zeros_like(nx)

    def settle(k):
        pair(k).wait_recv()

        def tile(i):
            r = pl.ds(pl.multiple_of(pc * HG + i * TILE, TILE), TILE)
            v = gr[k, r, :].astype(f32) + gr_in[k, at(i, TILE), :].astype(f32)
            gr[k, r, :] = v.astype(bf16)

        loop(HG // TILE, tile)

    def piece(k, i):
        r = pl.ds(pl.multiple_of(pc * HG + ring(i) * PR, PR), PR)
        return remote(gr.at[k, r], gr_pieces.at[k, i - 1], gb_s.at[k, i - 1], gb_r.at[k, i - 1], seq=ring(i))

    def gather_pieces(k):
        for i in range(1, seqs):
            piece(k, i).wait_recv()

        def tile(j):
            r = at(j, TILE)
            v = gr[k, pl.ds(pl.multiple_of(pc * HG + ps * PR + j * TILE, TILE), TILE), :].astype(f32)
            for i in range(1, seqs):
                v = v + gr_pieces[k, i - 1, r, :].astype(f32)
            gr_sum[k, r, :] = v.astype(bf16)
            grads[k, pl.ds(pl.multiple_of(pc * HG + ps * PR + j * TILE, TILE), TILE), :] = v.astype(bf16)

        loop(PR // TILE, tile)

    def spread(k, i):
        r = pl.ds(pl.multiple_of(pc * HG + ps * PR, PR), PR)
        return remote(gr_sum.at[k], grads.at[k, r], gc_s.at[k, i - 1], gc_r.at[k, i - 1], seq=ring(i))

    def hand(k, i):
        q = lax.rem(ps + seqs - i, seqs)
        r = pl.ds(pl.multiple_of(pc * HG + q * PR, PR), PR)
        src = gr_sum.at[k] if i == 0 else grads.at[k, r]
        return remote(src, grads.at[k, r], gd_s.at[k, i], gd_r.at[k, i], sample=other)

    def send_out(k):
        gather_pieces(k)
        for i in range(1, seqs):
            spread(k, i).start()
        hand(k, 0).start()

    def hand_on(k):
        for i in range(1, seqs):
            q = lax.rem(ps + seqs - i, seqs)
            r = pl.ds(pl.multiple_of(pc * HG + q * PR, PR), PR)
            remote(gr_sum.at[k], grads.at[k, r], gc_s.at[k, i - 1], gc_r.at[k, i - 1], seq=ring(i)).wait_recv()
            hand(k, i).start()

    def result(k):
        return pltpu.make_async_copy(grads.at[k], grads_out.at[k], out_sem.at[k])

    def complete(k):
        for i in range(seqs):
            q = lax.rem(ps + seqs - i, seqs)
            r = pl.ds(pl.multiple_of(other * HG + q * PR, PR), PR)
            remote(gr_sum.at[k], grads.at[k, r], gd_s.at[k, i], gd_r.at[k, i], sample=other).wait()
        result(k).start()

    def send_pieces(k):
        settle(k)
        for i in range(1, seqs):
            piece(k, i).start()

    send_pieces(0)
    send_pieces(1)
    fold1.step(4)
    for s in range(S):
        relays2[s].gather(chained, e)
        off[...] = jnp.zeros_like(off)

        def state_back(k):
            kk = NC - 1 - k
            c = s * NC + kk
            here = at(c, Q)
            run = cum[here, :]
            last = run[Q - 1 : Q, :]
            ds = later[c] + row_of(jnp.exp(off[0:1, :]), e[...]) * chained[s]
            off[...] += jnp.broadcast_to(last, (8, Q))
            upper = iota((Q, Q), 1) >= 64
            causal = iota((Q, Q), 0) >= iota((Q, Q), 1)
            b, r = act[here, C : C + Q], act[here, C + Q :]
            scores = mm(r, b, NT)
            dsc = jnp.zeros((Q, Q), f32)
            for p in range(C // Q):
                lanes = slice(p * Q, (p + 1) * Q)
                xp = act[here, lanes]
                dyp = dy[here, lanes].astype(bf16)
                dyl = (dy[here, lanes] - dyp.astype(f32)).astype(bf16)
                dx = jnp.zeros((Q, Q), f32)
                for o in range(2):
                    keep = upper == bool(o)
                    dym = jnp.where(keep, dyp, jnp.zeros_like(dyp))
                    dyn = jnp.where(keep, dyl, jnp.zeros_like(dyl))
                    w = weights_of(2 * p + o, here, causal)
                    dsc = dsc + (mm(dym, xp, NT) + mm(dyn, xp, NT)) * w
                    dx = dx + mm((scores * w).astype(bf16), dym, TN)
                work[0, :, lanes] = dx
            d = dt[here, :]
            work[2] = mm2(jnp.exp(last - run) * d, e[...])
            work[1] = work[2] * mm2(b, ds)
            d_read = mm2(dsc, b) + mm3(spread_dy(c), entry[c], NT)
            d_in = mm2(dsc, r, TN) + mm3(act[here, 0:C].astype(f32) * work[2], ds, NT)
            slope[here, C : C + Q] = d_in * slope[here, C : C + Q]
            slope[here, C + Q :] = d_read * slope[here, C + Q :]

            def tile(i):
                rows = at(c * (Q // TILE) + i, TILE)
                near = at(i, TILE)
                x = act[rows, 0:C].astype(f32)
                g = dy[rows, :]
                a, o = work[0, near, :], work[1, near, :]
                work[3, near, :] = g.astype(bf16).astype(f32) * ys[rows, :] - x * a
                work[4, near, :] = x * o
                both = a + o
                work[5, near, :] = x * both
                slope[rows, 0:C] = (both + sk[...] * g) * slope[rows, 0:C]

            loop(Q // TILE, tile, 4)
            ha = mm2(work[3], e[...], NT)
            hb = mm2(work[4], e[...], NT)
            hc = mm2(work[5], e[...], NT)
            crossing = mm2(fold8(entry[c] * ds), e[...], NT)
            crossing = jnp.sum(crossing, axis=0, keepdims=True) * jnp.exp(last)
            dlog = (
                mm2(triangle(lambda i, j: i <= j).astype(bf16), ha)
                + mm2(triangle(lambda i, j: i > j).astype(bf16), hb)
                + crossing
            )
            g = sg[here, :]
            ratio = jnp.where(d > 1e-30, g / jnp.maximum(d, 1e-30), 1.0)
            rate = hp[1:2, :]
            draw = rate * dlog * g + hc * ratio
            dcs[here, 2 * Q :] = draw.astype(bf16)
            hsums[0:8, :] += fold8(draw)
            hsums[8:16, :] += fold8(rate * dlog * d)
            fold1.step((5 if s == 0 else 11) + k)

        loop(NC, state_back)
        edge8[s] = slope[s * L : s * L + 8, :]

        @pl.when(ps > 0)
        def _():
            next_rows(s).start()

        def conv_back(r, last):
            for lo in range(0, W, 256):
                lanes = slice(lo, lo + 256)
                if last:
                    w = jnp.concatenate([slope[(s + 1) * L - TILE : (s + 1) * L, lanes], nx[s, :, lanes]], axis=0)
                else:
                    w = slope[pl.ds(pl.multiple_of(s * L + r * TILE, TILE), TILE + 8), lanes]
                u = pad[s, pl.ds(pl.multiple_of(r * TILE, TILE), TILE + HALO), lanes].astype(f32)
                d = w[0:TILE]
                v = cw[3:4, lanes] * d
                for k in range(3):
                    v = v + cw[k : k + 1, lanes] * w[3 - k : 3 - k + TILE]
                rows = at(r + s * LT, TILE)
                if lo < C:
                    gate[rows, lanes] = v.astype(bf16)
                else:
                    dcs[rows, lo - C : lo - C + 256] = v.astype(bf16)
                for k in range(4):
                    acc[8 * k : 8 * k + 8, lanes] += fold8(d * u[13 + k : 13 + k + TILE])
                acc[32:40, lanes] += fold8(d)

        loop(LT - 1, lambda r: conv_back(r, False))
        fold1.step(9 if s == 0 else 15)
        if s > 0:
            fold1.step(16)
            fold2.step(0)

        @pl.when(ps < seqs - 1)
        def _():
            next_rows(s).wait_recv()

        conv_back(LT - 1, True)
        if s > 0:
            fold1.step(17)
            fold2.step(1)

        def into(k):
            i = s * (L // 256) + k
            rows = at(i, 256)
            v = mm(dg[rows, :], wg[...], NT) + mm(gate[rows, :], wv[...], NT) + mm(dcs[rows, :], wst[...])
            part2[rows, :] = v.astype(bf16)
            nsums[...] += fold8(v * xb[rows, :].astype(f32) * inv[rows, 0:1])

        loop(L // 256, into)
        if s == 0:
            fold2.begin(0, tiles // S)
            fold1.step(10)
            send_out(0)

    for k in range(5):
        row = jnp.sum(acc[8 * k : 8 * k + 8, :], axis=0, keepdims=True)
        small[k : k + 1, :] = row[:, 0:C]
        smallz[k : k + 1, 0 : 2 * Q] = row[:, C:]
        smallz[k : k + 1, 2 * Q :] = jnp.zeros((1, C - 2 * Q), f32)
    ngrad = jnp.sum(nsums[...], axis=0, keepdims=True)
    for j in range(D // C):
        smallz[5 + j : 6 + j, :] = ngrad[:, j * C : (j + 1) * C]
    smallz[7:8, :] = jnp.zeros((1, C), f32)

    def to_line(i):
        return remote(smallz, smallz_in.at[i - 1], m1_s.at[i - 1], m1_r.at[i - 1], head=line(i))

    for i in range(1, lines):
        to_line(i).start()
    held = 4
    fold2.begin(tiles // S, tiles - tiles // S - held)
    fold2.step(2)
    fold1.step(18)
    fold1.step(19)

    rest = fold2.last(13, 6)
    for k in range(D // Q):
        t = mm(nt[k * Q : (k + 1) * Q, :], dcs[...])
        for j in range(2):
            turned = t[:, j * Q : (j + 1) * Q].T
            for g in range(own // 8):
                for h in range(lines):
                    later[j * DC + k * Q // C, 8 * (g * lines + h) : 8 * (g * lines + h) + 8, k * Q % C : k * Q % C + Q] = (
                        turned[h * own + 8 * g : h * own + 8 * g + 8]
                    )
        row = 8 + 8 * (k * Q // C)
        small[row : row + 8, k * Q % C : k * Q % C + Q] = t[:, 2 * Q :].T[0:8]

    SR = Q // seqs
    keep_state = at(pc, DC)

    def state_pair():
        return remote(later.at[at(other, DC)], sg_in, sa_s, sa_r, sample=other)

    state_pair().start()
    small[5:6, :] = jnp.sum(sums[0:8, :], axis=0, keepdims=True)
    small[6:7, :] = jnp.sum(sums[8:16, :], axis=0, keepdims=True)
    small[7:8, :] = jnp.zeros((1, C), f32)
    small[7:8, 0:Q] = jnp.sum(hsums[0:8, :], axis=0, keepdims=True)
    small[7:8, Q : 2 * Q] = jnp.sum(hsums[8:16, :], axis=0, keepdims=True)
    fold2.step(3)
    def outer3(i):
        gr[2, at(i, 512), :] = mm(nt[at(i, 512), :], gate[...]).astype(bf16)

    loop(D // 512, outer3)
    pair(2).start()
    fold2.two(4)
    fold2.take(0)
    fold2.closely(4)
    state_pair().wait_recv()
    later[keep_state] = later[keep_state] + sg_in[...]

    def state_piece(i):
        return remote(later.at[keep_state, at(ring(i), SR)], sg_pieces.at[i - 1], sb_s.at[i - 1], sb_r.at[i - 1], seq=ring(i))

    for i in range(1, seqs):
        state_piece(i).start()
    fold2.closely(5)
    send_pieces(2)
    fold2.closely(6)
    hand_on(0)
    fold2.closely(7)
    fold2.closely(8)
    for i in range(1, seqs):
        state_piece(i).wait_recv()
    v = later[keep_state, at(ps, SR), :]
    for i in range(1, seqs):
        v = v + sg_pieces[i - 1]
    sg_sum[...] = v
    blocks = SR // 8

    def block_of(h):
        return lax.rem(h + lines * blocks - lax.rem(ps * blocks, lines), lines)

    for k in range(blocks):
        sg_wire[k] = v[:, 8 * k : 8 * k + 8, :].astype(bf16)
    owns = block_of(ph) < blocks

    def to_owner(i):
        return remote(sg_wire.at[lax.rem(block_of(line(i)), blocks)], sg_line.at[i - 1], sz_s.at[i - 1], sz_r.at[i - 1], head=line(i))

    for i in range(1, lines):

        @pl.when(block_of(line(i)) < blocks)
        def _():
            to_owner(i).start()

    fold2.begin(tiles - held, held)
    fold2.closely(9)
    send_out(1)
    fold2.closely(10)
    total = smallz[...]
    for i in range(1, lines):
        to_line(i).wait_recv()
        total = total + smallz_in[i - 1]
    small[24:32, :] = total

    def to_core():
        return remote(small, small_two.at[0], m2_s.at[seqs - 1], m2_r.at[seqs - 1], sample=other)

    def to_peer(i):
        return remote(small_two.at[1], small_in.at[i - 1], m2_s.at[i - 1], m2_r.at[i - 1], seq=ring(i))

    to_core().start()
    fold2.closely(11)
    send_out(2)
    fold2.closely(12)
    to_core().wait_recv()
    small_two[1] = small[...] + small_two[0]
    for i in range(1, seqs):
        to_peer(i).start()
    fold2.closely(13)
    span = own // 8

    def place_row(g, core):
        return pl.ds(pl.multiple_of(core * own + g * 8, 8), 8)

    my_row = lax.div(ps * blocks, lines)

    def state_out_to(i):
        return remote(sg_done, state_out.at[:, place_row(my_row, pc)], sc_s.at[i - 1], sc_r.at[i - 1], seq=ring(i))

    def holder(g):
        return lax.div(g * lines + ph, blocks)

    def state_hand(g, src):
        return remote(src, state_out.at[:, place_row(g, pc)], sd_s.at[g], sd_r.at[g], sample=other)

    @pl.when(owns)
    def _():
        t = sg_sum[:, pl.ds(pl.multiple_of(8 * block_of(ph), 8), 8), :]
        for i in range(1, lines):
            to_owner(i).wait_recv()
            t = t + sg_line[i - 1].astype(f32)
        sg_done[...] = t
        state_out[:, place_row(my_row, pc), :] = t
        for i in range(1, seqs):
            state_out_to(i).start()

    for move, i in rest[0]:
        move(i)
    hand_on(1)
    complete(0)
    for move, i in rest[1]:
        move(i)
    for move, i in rest[2]:
        move(i)
    hand_on(2)
    complete(1)
    for move, i in rest[3]:
        move(i)
    total = small_two[1]
    for i in range(1, seqs):
        to_peer(i).wait_recv()
        total = total + small_in[i - 1]
    small_out[...] = total
    small_copy = pltpu.make_async_copy(small_out, small_result, out_sem.at[3])
    small_copy.start()
    for move, i in rest[4]:
        move(i)
    for move, i in rest[5]:
        move(i)
    for g in range(span):

        @pl.when(holder(g) == ps)
        def _():
            state_hand(g, sg_done).start()

        for i in range(1, seqs):

            @pl.when(ring(seqs - i) == holder(g))
            def _():
                remote(
                    sg_done, state_out.at[:, place_row(g, pc)], sc_s.at[i - 1], sc_r.at[i - 1], seq=ring(i)
                ).wait_recv()
                state_hand(g, state_out.at[:, place_row(g, pc)]).start()

    for g in range(span):
        remote(sg_done, state_out.at[:, place_row(g, other)], sd_s.at[g], sd_r.at[g], sample=other).wait()
    state_copy = pltpu.make_async_copy(state_out, state_result, out_sem.at[4])
    state_copy.start()
    complete(2)
    fold1.end()
    fold2.end()
    for r in relays2:
        r.finish()
    for i in range(1, lines):
        for c in weights(i, ph):
            c.wait_send()
        for s in range(S):
            stat(s, i).wait_send()
        to_line(i).wait_send()

        @pl.when(block_of(line(i)) < blocks)
        def _():
            to_owner(i).wait_send()

    @pl.when(ps < seqs - 1)
    def _():
        for s in range(S):
            halo(s).wait_send()

    @pl.when(ps > 0)
    def _():
        for s in range(S):
            next_rows(s).wait_send()

    for k in range(3):
        pair(k).wait_send()
        for i in range(1, seqs):
            piece(k, i).wait_send()
            spread(k, i).wait_send()
        result(k).wait()
    small_copy.wait()
    state_copy.wait()
    state_pair().wait_send()
    share().wait_send()
    for i in range(1, seqs):
        state_piece(i).wait_send()

        @pl.when(owns)
        def _():
            state_out_to(i).wait_send()

    to_core().wait_send()
    for i in range(1, seqs):
        to_peer(i).wait_send()


def finish(
    lines, x, cot, gain, dn, outs, g_out, g_gate, g_value, state, small,
    block_out, input_grad, gate_grad, value_grad, out_grad,
    state_grad, norm_grad, step_grad, cv, cs, cvb, csb, sbias, dlog, skip, gated_gain,
):
    rows, width = x.shape
    for j in range(rows // 16):
        r = slice(j * 16, (j + 1) * 16)
        v = x[r, :].astype(f32)
        block_out[r, :] = (v + outs[r, :].astype(f32)).astype(bf16)
        s = dn[r, :].astype(f32) * gain[...]
        i1 = lax.rsqrt(jnp.mean(v * v, axis=1, keepdims=True) + EPS)
        m = jnp.mean(s * v, axis=1, keepdims=True)
        input_grad[r, :] = cot[r, :].astype(f32) + i1 * s - v * (i1 * i1 * i1 * m)
    half = g_gate.shape[1]
    for j in range(width // half):
        out_grad[:, j * half : (j + 1) * half] = g_out[j].astype(f32)
    gate_grad[...] = g_gate[...].astype(f32)
    value_grad[...] = g_value[...].astype(f32)

    @pl.when(pl.program_id(0) == 0)
    def _():
        heads, own = sbias.shape[1], csb.shape[1]
        for j in range(width // half):
            lanes = slice(j * half, (j + 1) * half)
            state_grad[:, lanes] = state[j]
            norm_grad[:, lanes] = small[29 + j : 30 + j, :]
            step_grad[:, lanes] = small[8 + 8 * j : 16 + 8 * j, :]
        cv[...] = small[0:4, :]
        cvb[...] = small[4:5, :]
        gated_gain[...] = small[5:6, :]
        e = lane_heads(half // 64, half)
        skip[...] = mm(jnp.broadcast_to(small[6:7, :], (8, half)), e.astype(f32), NT, HI)[0:1, 0:heads]
        sbias[...] = small[7:8, 0:heads]
        dlog[...] = small[7:8, Q : Q + heads]
        for h in range(lines):

            @pl.when(lax.axis_index("head") == h)
            def _():
                for j in range(2):
                    lanes = slice(j * Q + h * own, j * Q + (h + 1) * own)
                    cs[:, j, :] = small[24:28, lanes]
                    csb[j : j + 1, :] = small[28:29, lanes]


def per_device(
    block_in, out_cotangent, norm_gain, gate_proj, value_proj, state_proj, step_proj,
    conv_value, conv_state, conv_value_bias, conv_state_bias, step_bias, decay_log,
    skip_gain, gated_gain, out_proj,
):
    S, L, D = block_in.shape
    T = S * L
    heads = step_proj.shape[1]
    C = gate_proj.shape[1]
    own = state_proj.shape[2]
    W = C + 2 * Q
    NCH = T // Q
    seqs, lines = lax.axis_size("seq"), lax.axis_size("head")
    tiles = 32
    H = D // 2
    PR = H // seqs
    SR = Q // seqs
    x = block_in.reshape(T, D)
    cot = out_cotangent.reshape(T, D)
    spt = state_proj.transpose(0, 2, 1).reshape(2 * own, D)
    gain = norm_gain[None]
    vm = pl.BlockSpec(memory_space=pltpu.VMEM)
    hbm = pl.BlockSpec(memory_space=pl.ANY)
    dma = pltpu.SemaphoreType.DMA
    n1, l1 = seqs - 1, lines - 1
    V = pltpu.VMEM
    scratch = [
        V((T, D), bf16), V((T, D), bf16), V((D, C), bf16), V((D, C), bf16), V((3 * Q, D), bf16),
        V((C, D), bf16), V((8, Q), f32), V((lines, 8, Q), f32), V((8, W), f32), V((8, Q), f32), V((1, C), f32),
        V((S * HALO, D), bf16),
        V((D, T), bf16), V((T, Q), f32), V((T, C), bf16), V((S, HALO + L, W), bf16), V((T, W), f32),
        V((T, W), bf16), V((T, Q), f32), V((T, Q), f32), V((T, Q), f32), V((8, T), f32), V((8, T), f32),
        V((NCH, Q, C), f32), V((T, C), f32), V((T, C), f32), V((T, C), bf16), V((T, C), bf16),
        V((NCH, Q, C), f32),
        V((T, 3 * Q), bf16), V((Q, C), bf16), V((Q, C), f32), V((6, Q, C), f32),
        V((8, Q), f32), V((Q, Q), f32), V((4, Q, Q), f32), V((8, T), f32), V((l1, 8, T), f32),
        V((S, Q, C), bf16), V((S, 8, Q), f32), V((seqs, S, Q, C), bf16), V((seqs, S, 8, Q), f32),
        V((S, Q, C), f32),
        V((T, D), bf16), V((T, D), bf16), V((T, D), bf16), V((T, D), bf16), V((T, D), bf16), V((T, D), bf16),
        V((3, D, C), bf16), V((D // C, 2 * own, C), f32), V((32, C), f32), V((3, D, C), bf16), V((3, H, C), bf16), V((3, n1, PR, C), bf16), V((3, PR, C), bf16),
        V((D // C, Q, C), f32), V((n1, D // C, SR, C), f32), V((l1, D // C, 8, C), bf16),
        V((SR // 8, D // C, 8, C), bf16), V((D // C, SR, C), f32), V((D // C, 8, C), f32),
        V((40, W), f32), V((16, Q), f32), V((16, C), f32), V((8, D), f32), V((8, C), f32),
        V((l1, 8, C), f32), V((32, C), f32), V((2, 32, C), f32), V((n1, 32, C), f32), V((S, 8, W), f32), V((S, 8, W), f32),
        dma((S + 5,)), dma((2, S)), dma((2, lines)), dma((2, lines)), dma((2, 2, S, n1)), dma((2, 2, S, n1)),
        dma((S, l1)), dma((S, l1)), dma((S,)), dma((S,)),
        dma((2, tiles)), dma((3,)), dma((2, tiles)), dma((3,)), dma((3,)), dma((3,)), dma((3, n1)), dma((3, n1)),
        dma((3, n1)), dma((3, n1)), dma((3, seqs)), dma((3, seqs)),
        dma((5,)), dma, dma, dma((n1,)), dma((n1,)), dma((l1,)), dma((l1,)), dma((n1,)), dma((n1,)),
        dma((own // 8,)), dma((own // 8,)), dma((l1,)), dma((l1,)), dma((seqs,)), dma((seqs,)),
    ]
    outs, dnorm, grads, state_out, small = pl.pallas_call(
        functools.partial(block, (S, L, seqs, lines, tiles)),
        out_shape=[
            jax.ShapeDtypeStruct((T, D), bf16), jax.ShapeDtypeStruct((T, D), bf16),
            jax.ShapeDtypeStruct((3, D, C), bf16), jax.ShapeDtypeStruct((D // C, 2 * own, C), f32),
            jax.ShapeDtypeStruct((32, C), f32),
        ],
        in_specs=[hbm, hbm, vm, hbm, hbm, hbm, vm, hbm] + [vm] * 8,
        out_specs=[hbm] * 5,
        scratch_shapes=scratch,
        name="block",
        compiler_params=pltpu.CompilerParams(
            collective_id=0, has_side_effects=True, vmem_limit_bytes=67043328
        ),
    )(
        x, cot, gain, gate_proj, value_proj, spt, step_proj.T, out_proj, conv_state, conv_state_bias,
        conv_value, conv_value_bias[None], step_bias[None], decay_log[None], skip_gain[None], gated_gain[None],
    )
    steps = 2

    def whole(*shape):
        return pl.BlockSpec(shape, lambda i: (0,) * len(shape))

    by_rows = pl.BlockSpec((T // steps, D), lambda i: (i, 0))
    by_grad = pl.BlockSpec((D // steps, C), lambda i: (i, 0))
    shape = jax.ShapeDtypeStruct
    (block_out, input_grad, gate_grad, value_grad, out_grad, state_grad, norm_grad, step_grad, cv, cs, cvb, csb,
     sbias, dlog, skip, gated) = pl.pallas_call(
        functools.partial(finish, lines),
        grid=(steps,),
        out_shape=[
            shape((T, D), bf16), shape((T, D), f32), shape((D, C), f32), shape((D, C), f32), shape((C, D), f32),
            shape((2 * own, D), f32), shape((1, D), f32), shape((heads, D), f32), shape((4, C), f32),
            shape((4, 2, own), f32), shape((1, C), f32), shape((2, own), f32), shape((1, heads), f32),
            shape((1, heads), f32), shape((1, heads), f32), shape((1, C), f32),
        ],
        in_specs=[
            by_rows, by_rows, whole(1, D), by_rows, by_rows,
            pl.BlockSpec((None, D // C, C // steps, C), lambda i: (0, 0, i, 0)),
            pl.BlockSpec((None, D // steps, C), lambda i: (1, i, 0)),
            pl.BlockSpec((None, D // steps, C), lambda i: (2, i, 0)),
            whole(D // C, 2 * own, C), whole(32, C),
        ],
        out_specs=[
            by_rows, by_rows, by_grad, by_grad, pl.BlockSpec((C // steps, D), lambda i: (i, 0)),
            whole(2 * own, D), whole(1, D), whole(heads, D), whole(4, C), whole(4, 2, own), whole(1, C),
            whole(2, own), whole(1, heads), whole(1, heads), whole(1, heads), whole(1, C),
        ],
        name="finish",
        compiler_params=pltpu.CompilerParams(vmem_limit_bytes=60 * 2**20),
    )(x, cot, gain, dnorm, outs, grads.reshape(3, D // C, C, C), grads, grads, state_out, small)
    return (
        block_out.reshape(S, L, D), input_grad.reshape(S, L, D), norm_grad[0], gate_grad, value_grad,
        state_grad.reshape(2, own, D).transpose(0, 2, 1), step_grad.T, cv, cs, cvb[0], csb, sbias[0], dlog[0],
        skip[0], gated[0], out_grad,
    )


def solution(mesh):
    tokens = P("sample", "seq", None)
    params = (
        P(), P(None, "head"), P(None, "head"), P(None, None, "head"), P(None, "head"),
        P(None, "head"), P(None, None, "head"), P("head"), P(None, "head"), P("head"),
        P("head"), P("head"), P("head"), P("head", None),
    )
    return jax.shard_map(
        per_device,
        mesh=mesh,
        in_specs=(tokens, tokens) + params,
        out_specs=(tokens, tokens) + params,
        check_vma=False,
    )
```
